256 devices in a mesh: ta: 128 (over x, y, z), row: 2 (over core).
Axes of the slice: x: 4, y: 4, z: 8, core: 2. Of those that a mesh axis runs over, the one named last changes fastest.
Arguments:
- movie: bfloat16 [2, 1024, 128, 512], P('row', 'ta'), may hold values from -384 to 384
- shifts: int32 [2, 1024, 4, 2], P('row', 'ta'), may hold values from -8 to 8
- footprint: bfloat16 [2, 128, 8, 512], P('row', 'ta'), may hold values from 0.25 to 1
- support: int32 [2, 128, 8, 512], P('row', 'ta'), may hold values 0 or 1
- neuron_ids: int32 [2, 128, 8], P('row', 'ta'), may hold values from 0 to 255, as said below
- owner_order: int32 [256], replicated, may hold values from 0 to 255, each once
- start_traces: float32 [256, 1024], P(('ta', 'row')), may hold values from 0 to 2
Outputs:
- tile_movie: bfloat16 [2, 128, 1024, 512], P('row', 'ta')
- traces: float32 [256, 1024], P(('ta', 'row'))
The draws below stay inside these ranges and needn't reach their ends.
Inputs may be any that keep to these rules, and one draw needn't show every extreme that they name: `neuron_ids`: the neurons named by one tile's slots are distinct. Slot 0 of tile t of slab s names neuron s * 128 + t, and every slot of that tile names a neuron within 12 of it, counted modulo 256. `owner_order`: A permutation of all neurons.
All inputs are finite; a program needn't handle non-finite values. No bound on the sum of `support` on one device may be relied on, other than what follows from the above.
Results may differ from the reference program's by a relative error of at most 0.004.
Values may be sent and summed in bfloat16 or wider, within the bound.
No kernel may reach another device: no remote copies, remote signals or barrier semaphores. Data moves between devices by JAX's collectives and lax.ppermute only.
A program may use at most 64 MiB of HBM per device.

```python
import jax
import jax.numpy as jnp
from jax import lax

H = 128
W = 512
TH = 16
TW = 32
PW = 128
MAXS = 8
SLOTS = 8
REACH = 12
ITERS = 2
FRAMES = 1024
SLABS = 2
PATCHES = 4
TILES = 128
TPIX = 512
NEURONS = 256


def draw_neuron_ids(key, part):
    tile_total = SLABS * TILES
    tile_keys = jax.random.split(jax.random.fold_in(key, 17), tile_total)

    def offsets(tile_key):
        order = jax.random.permutation(tile_key, 2 * REACH)
        picked = order[:SLOTS - 1].astype(jnp.int32)
        signed = jnp.where(picked < REACH, picked - REACH, picked - REACH + 1)
        return jnp.concatenate([jnp.zeros((1,), jnp.int32), signed])
    moves = jax.vmap(offsets)(tile_keys)
    home = jnp.arange(tile_total, dtype=jnp.int32) * (NEURONS // tile_total)
    return ((home[:, None] + moves) % NEURONS).reshape(SLABS, TILES, SLOTS).astype(jnp.int32)


def with_ends(entries, rng, least, high):
    longest = entries.shape.index(max(entries.shape))
    spots = []
    for shift in (0, 1):
        where = [jax.random.randint(jax.random.fold_in(rng, axis), (), 0, length) for axis, length in enumerate(entries.shape)]
        where[longest] = (where[longest] + shift) % entries.shape[longest]
        spots.append(tuple(where))
    return entries.at[spots[0]].set(least).at[spots[1]].set(high)


def levels(own_key, dims, pieces, least, high):
    def one(axis_at, blocks):
        steps = jax.random.uniform(jax.random.fold_in(jax.random.fold_in(own_key, 6), axis_at), (blocks,), jnp.float32, least / len(pieces), high / len(pieces))
        return jnp.repeat(jnp.exp(steps), dims[axis_at] // blocks).reshape((-1,) + (1,) * (len(dims) - axis_at - 1))

    gain = one(*pieces[0])
    for cut in pieces[1:]:
        gain = gain * one(*cut)
    return gain


def centred(own_key, dims, width, limit, cuts=(), kind=jnp.bfloat16):
    drawn = jax.random.normal(own_key, dims, jnp.float32) * width
    if len(cuts) > 0:
        drawn = levels(own_key, dims, cuts, -0.22, 0.18) * drawn
    return jnp.clip(drawn, min=-limit, max=limit).astype(kind)


def setup_inputs(seed: int = 0) -> dict:
    key_list = jax.random.split(jax.random.key(seed), 8)
    movie = centred(key_list[0], (SLABS, FRAMES, H, W), 64.0, 384.0, ((0, 2), (1, 128)))
    shifts = with_ends(jax.random.randint(key_list[1], (SLABS, FRAMES, PATCHES, 2), 0 - MAXS, MAXS + 1), jax.random.fold_in(key_list[1], 1), 0 - MAXS, MAXS).astype(jnp.int32)
    footprint = jnp.clip(0.25 + 0.75 * jax.random.uniform(key_list[2], (SLABS, TILES, SLOTS, TPIX), jnp.float32) ** levels(key_list[2], (SLABS, TILES, SLOTS, TPIX), ((0, 2), (1, 128)), -0.2, 0.2), 0.25, 1.0).astype(jnp.bfloat16)
    support = with_ends((jax.random.randint(key_list[3], (SLABS, TILES, SLOTS, TPIX), 0, 2) < 1).astype(jnp.int32), jax.random.fold_in(key_list[3], 1), 0, 1)
    neuron_ids = draw_neuron_ids(jax.random.fold_in(key_list[7], 71), 0)
    owner_order = jax.random.permutation(key_list[5], NEURONS).astype(jnp.int32)
    start_traces = jnp.clip(2.0 * jax.random.uniform(key_list[6], (NEURONS, FRAMES), jnp.float32) ** levels(key_list[6], (NEURONS, FRAMES), ((0, 256),), -0.2, 0.2), 0.0, 2.0)
    return dict(movie=movie, shifts=shifts, footprint=footprint, support=support, neuron_ids=neuron_ids, owner_order=owner_order, start_traces=start_traces)


def smoothing_table(length):
    places = jnp.arange(length, dtype=jnp.float32)
    spread = places[:, None] - places[None, :]
    kernel = jnp.exp(-spread * spread / 32.0)
    return (kernel / jnp.sum(kernel, axis=0, keepdims=True)).astype(jnp.bfloat16)


def register_frame(frame_image, frame_moves):
    padded = jnp.pad(frame_image, MAXS)
    strips = []
    for patch_index in range(PATCHES):
        row_anchor = (MAXS + frame_moves[patch_index, 0]).astype(jnp.int32)
        col_anchor = (MAXS + patch_index * PW + frame_moves[patch_index, 1]).astype(jnp.int32)
        strips.append(lax.dynamic_slice(padded, (row_anchor, col_anchor), (H, PW)))
    return jnp.concatenate(strips, axis=1)


def reference(movie, shifts, footprint, support, neuron_ids, owner_order, start_traces):
    table_wide = smoothing_table(W)
    table_tall = smoothing_table(H)

    def filter_frame(frame_pair):
        registered = register_frame(frame_pair[0], frame_pair[1])
        wide = jnp.dot(registered, table_wide, preferred_element_type=jnp.float32).astype(jnp.bfloat16)
        wide = lax.optimization_barrier(wide)
        smooth = jnp.dot(table_tall.T, wide, preferred_element_type=jnp.float32)
        return (registered.astype(jnp.float32) - smooth).astype(jnp.bfloat16)

    slab_tiles = []
    for slab_index in range(SLABS):
        filtered = lax.map(filter_frame, (movie[slab_index], shifts[slab_index]))
        tiled = filtered.reshape(FRAMES, H // TH, TH, W // TW, TW).transpose(1, 3, 0, 2, 4)
        slab_tiles.append(tiled.reshape(TILES, FRAMES, TPIX))
    tile_movie = jnp.stack(slab_tiles, axis=0)

    footprints = footprint * support.astype(jnp.bfloat16)
    flat_prints = footprints.reshape(SLABS * TILES, SLOTS, TPIX)
    flat_movie = tile_movie.reshape(SLABS * TILES, FRAMES, TPIX)

    def project_tile(tile_pair):
        return jnp.dot(tile_pair[0], tile_pair[1].T, preferred_element_type=jnp.float32)

    projected = lax.map(project_tile, (flat_prints, flat_movie))
    prints_wide = flat_prints.astype(jnp.float32)
    gram = jnp.einsum("tip,tjp->tij", prints_wide, prints_wide, precision=lax.Precision.HIGHEST)
    flat_ids = neuron_ids.reshape(SLABS * TILES, SLOTS).astype(jnp.int32)
    coupling = jnp.zeros((NEURONS, NEURONS), jnp.float32).at[flat_ids[:, :, None], flat_ids[:, None, :]].add(gram)
    drive = jnp.zeros((NEURONS, FRAMES), jnp.float32).at[flat_ids].add(projected)
    bound = 1.0 + jnp.sum(coupling, axis=1)
    current = start_traces[owner_order]
    for iteration in range(ITERS):
        gradient = jnp.dot(coupling, current, precision=lax.Precision.HIGHEST) - drive
        current = jnp.maximum(current - gradient / bound[:, None], 0.0)
    traces = jnp.zeros((NEURONS, FRAMES), jnp.float32).at[owner_order].set(current)
    return tile_movie, traces
```

```python
import jax
import jax.numpy as jnp
import numpy as np
from jax import lax
from jax.experimental import pallas as pl
from jax.experimental.pallas import tpu as pltpu
from jax.sharding import Mesh
from jax.sharding import PartitionSpec as P

TH = 16
TW = 32
MAXS = 8
ITERS = 2
TA = ("ta_0", "ta_1", "ta_2")
TA_ROW = ("ta_0", "ta_1", "ta_2", "row")

FRAMES = 8
H = 128
W = 512
LANES = 128
BLOCKS = W // LANES
SLOTS = 8
NEURONS = 256
SPAN = 4
GRAM_AT = SPAN * SLOTS
IDS_AT = GRAM_AT + SLOTS * SLOTS
START_AT = IDS_AT + SLOTS
WIDE = NEURONS + LANES
HIGHEST = lax.Precision.HIGHEST
VMEM = pl.BlockSpec(memory_space=pltpu.VMEM)
SMEM = pl.BlockSpec(memory_space=pltpu.SMEM)


def smoothing_table(length):
    places = np.arange(length, dtype=np.float32)
    spread = places[:, None] - places[None, :]
    kernel = np.exp(-spread * spread / np.float32(32.0)).astype(np.float32)
    return (kernel / np.sum(kernel, axis=0, keepdims=True, dtype=np.float32)).astype(jnp.bfloat16)


def iota(shape, dim):
    return lax.broadcasted_iota(jnp.int32, shape, dim)


def split3(value):
    high = value.astype(jnp.bfloat16)
    rest = value - high.astype(jnp.float32)
    mid = rest.astype(jnp.bfloat16)
    low = (rest - mid.astype(jnp.float32)).astype(jnp.bfloat16)
    return high, mid, low


def dot32(left, right):
    return jnp.dot(left, right, preferred_element_type=jnp.float32)


def pick(exact, value):
    high, mid, low = split3(value)
    return dot32(exact, high) + (dot32(exact, mid) + dot32(exact, low))


def place(value, exact):
    high, mid, low = split3(value)
    return dot32(high, exact) + (dot32(mid, exact) + dot32(low, exact))


def filter_kernel(
    shifts_ref, ids_ref, order_ref, movie_ref, wide_ref, tall_ref, start_ref,
    out_ref, base_ref, padded_ref, registered_ref, filtered_ref,
):
    lane = iota((H, LANES), 1)
    padded_ref[:, pl.ds(0, MAXS), :] = jnp.zeros((BLOCKS, MAXS, LANES), jnp.float32)
    padded_ref[:, pl.ds(MAXS + H, MAXS), :] = jnp.zeros((BLOCKS, MAXS, LANES), jnp.float32)

    def block(f, p):
        if p < 0 or p >= BLOCKS:
            return None
        return movie_ref[f, :, p * LANES : (p + 1) * LANES].astype(jnp.float32)

    def frame(f, carry):
        for p in range(BLOCKS):
            dy = shifts_ref[f, p, 0]
            dx = shifts_ref[f, p, 1]
            amount = jnp.where(dx > 0, LANES - dx, -dx)
            source = lane + dx

            def rolled(value):
                if value is None:
                    return jnp.zeros((H, LANES), jnp.float32)
                return pltpu.roll(value, amount, 1)

            inner = jnp.where(source >= LANES, rolled(block(f, p + 1)), rolled(block(f, p)))
            moved = jnp.where(source < 0, rolled(block(f, p - 1)), inner)
            padded_ref[p, pl.ds(MAXS, H), :] = moved
            registered_ref[:, p * LANES : (p + 1) * LANES] = padded_ref[p, pl.ds(MAXS + dy, H), :]
        registered = registered_ref[...]
        wide = dot32(registered.astype(jnp.bfloat16), wide_ref[...]).astype(jnp.bfloat16)
        filtered = registered - dot32(tall_ref[...], wide)
        for p in range(BLOCKS):
            filtered_ref[p, pl.ds(f, H, stride=FRAMES), :] = filtered[:, p * LANES : (p + 1) * LANES]
        return carry

    lax.fori_loop(0, FRAMES, frame, 0)
    lanes8 = iota((FRAMES, LANES), 1)
    near = lanes8 < 2 * TW
    even = lax.rem(lanes8 // TW, 2) == 0

    def tile_row(ty, carry):
        for q in range(4):
            for p in range(BLOCKS):
                v = []
                for r in range(4):
                    at = pl.multiple_of((ty * TH + 4 * q + r) * FRAMES, FRAMES)
                    v.append(filtered_ref[p, pl.ds(at, FRAMES), :])
                a0 = jnp.where(near, v[0], pltpu.roll(v[2], 64, 1))
                a2 = jnp.where(near, pltpu.roll(v[0], 64, 1), v[2])
                a1 = jnp.where(near, v[1], pltpu.roll(v[3], 64, 1))
                a3 = jnp.where(near, pltpu.roll(v[1], 64, 1), v[3])
                tiles = (
                    jnp.where(even, a0, pltpu.roll(a1, 32, 1)),
                    jnp.where(even, pltpu.roll(a0, 96, 1), a1),
                    jnp.where(even, a2, pltpu.roll(a3, 32, 1)),
                    jnp.where(even, pltpu.roll(a2, 96, 1), a3),
                )
                for m in range(4):
                    out_ref[ty * 16 + 4 * p + m, :, q * LANES : (q + 1) * LANES] = tiles[m].astype(jnp.bfloat16)
        return carry

    lax.fori_loop(0, H // TH, tile_row, 0)

    row_lane = iota((1, LANES), 1)
    owners = jnp.zeros((1, LANES), jnp.float32)
    for i in range(SLOTS):
        owner = order_ref[ids_ref[0, i]].astype(jnp.float32)
        owners = jnp.where(row_lane == IDS_AT + i, owner, owners)
    inside = iota((32, LANES), 1) // SPAN == iota((32, LANES), 0)
    fold = jnp.where(
        lax.rem(iota((LANES, LANES), 0), SPAN) == iota((LANES, LANES), 1) - START_AT, 1.0, 0.0
    ).astype(jnp.bfloat16)
    for b in range(NEURONS // 32):
        row = start_ref[:, b * LANES : (b + 1) * LANES]
        spread = jnp.where(inside, jnp.broadcast_to(row, (32, LANES)), 0.0)
        base_ref[pl.ds(b * 32, 32), :] = place(spread, fold) + owners


def filter_tiles(movie, shifts, ids, order, start):
    return pl.pallas_call(
        filter_kernel,
        out_shape=(
            jax.ShapeDtypeStruct((128, FRAMES, TH * TW), jnp.bfloat16),
            jax.ShapeDtypeStruct((NEURONS, LANES), jnp.float32),
        ),
        in_specs=[SMEM, SMEM, SMEM, VMEM, VMEM, VMEM, VMEM],
        out_specs=(VMEM, VMEM),
        scratch_shapes=[
            pltpu.VMEM((BLOCKS, H + 2 * MAXS, LANES), jnp.float32),
            pltpu.VMEM((H, W), jnp.float32),
            pltpu.VMEM((BLOCKS, H * FRAMES, LANES), jnp.float32),
        ],
        name="filter",
    )(shifts, ids, order, movie, smoothing_table(W), smoothing_table(H).T, start)


def project_kernel(movie_ref, footprint_ref, support_ref, base_ref, out_ref, full_ref):
    footprints = footprint_ref[...] * support_ref[...].astype(jnp.bfloat16)
    copies = jnp.concatenate([footprints] * (LANES // SLOTS), axis=0)
    contract = (((1,), (1,)), ((), ()))
    full_ref[...] = lax.dot_general(
        movie_ref[...], copies, contract, preferred_element_type=jnp.float32
    )
    gram = lax.dot_general(footprints, copies, contract, preferred_element_type=jnp.float32)
    own = iota((SLOTS, LANES), 1) // SLOTS - SPAN == iota((SLOTS, LANES), 0)
    common = jnp.sum(jnp.where(own, gram, 0.0), axis=0, keepdims=True)
    total = base_ref[...] + common
    group = iota((NEURONS, LANES), 1) // SLOTS
    for j in range(SPAN):
        total = jnp.where(group == j, full_ref[pl.ds(j, NEURONS, stride=SPAN), :], total)
    out_ref[...] = total


def project(tile_movie, footprint, support, base):
    return pl.pallas_call(
        project_kernel,
        out_shape=jax.ShapeDtypeStruct((NEURONS, LANES), jnp.float32),
        in_specs=[VMEM] * 4,
        out_specs=VMEM,
        scratch_shapes=[pltpu.VMEM((SPAN * NEURONS, LANES), jnp.float32)],
        name="project",
    )(tile_movie, footprint, support, base)


def solve_kernel(mail_ref, out_ref, select_ref, high_ref, mid_ref, low_ref):
    mail_t = mail_ref[...].T
    neuron = iota((NEURONS, NEURONS), 0)
    for i in range(SLOTS):
        ids = mail_t[IDS_AT + i : IDS_AT + i + 1, :].astype(jnp.int32)
        select_ref[:, i * NEURONS : (i + 1) * NEURONS] = jnp.where(neuron == ids, 1.0, 0.0).astype(jnp.bfloat16)

    step = 32
    lane = iota((step, LANES), 1)
    place_of = iota((step, NEURONS), 1)

    def rows(b, carry):
        at = pl.multiple_of(b * step, step)
        mail = mail_ref[pl.ds(at, step), :]
        same = [place_of == mail[:, IDS_AT + i : IDS_AT + i + 1].astype(jnp.int32) for i in range(SLOTS)]
        for i in range(SLOTS):
            line = jnp.zeros((step, NEURONS), jnp.float32)
            for k in range(SLOTS):
                column = GRAM_AT + i * SLOTS + k
                line = jnp.where(same[k], mail[:, column : column + 1], line)
            mine = jnp.where((lax.rem(lane, SLOTS) == i) & (lane < GRAM_AT), mail, 0.0)
            to = pl.ds(pl.multiple_of(i * NEURONS + at, step), step)
            for start, value in ((0, line), (NEURONS, mine)):
                end = start + value.shape[1]
                high, mid, low = split3(value)
                high_ref[to, start:end] = high
                mid_ref[to, start:end] = mid
                low_ref[to, start:end] = low
        return carry

    lax.fori_loop(0, NEURONS // step, rows, 0)
    select = select_ref[...]
    sums = dot32(select, high_ref[...]) + (dot32(select, mid_ref[...]) + dot32(select, low_ref[...]))
    coupling = sums[:, :NEURONS]
    source = iota((LANES, LANES), 0)
    target = lax.rem(iota((LANES, LANES), 1), SPAN)
    fold = jnp.where((source // SLOTS == target) & (source < GRAM_AT), 1.0, 0.0).astype(jnp.bfloat16)
    drive = place(sums[:, NEURONS:], fold)
    copy = jnp.where(source - START_AT == target, 1.0, 0.0).astype(jnp.bfloat16)
    current = place(mail_ref[...], copy)
    bound = 1.0 + jnp.sum(coupling, axis=1, keepdims=True)
    for _ in range(ITERS):
        product = jnp.dot(coupling, current, preferred_element_type=jnp.float32, precision=HIGHEST)
        current = jnp.maximum(current - (product - drive) / bound, 0.0)
    out_ref[...] = current


def solve(mail):
    return pl.pallas_call(
        solve_kernel,
        out_shape=jax.ShapeDtypeStruct((NEURONS, LANES), jnp.float32),
        in_specs=[VMEM],
        out_specs=VMEM,
        scratch_shapes=[pltpu.VMEM((NEURONS, SLOTS * NEURONS), jnp.bfloat16)]
        + [pltpu.VMEM((SLOTS * NEURONS, WIDE), jnp.bfloat16)] * 3,
        name="solve",
    )(mail)


def join_kernel(pieces_ref, out_ref):
    inside = iota((32, LANES), 1) // SPAN == iota((32, LANES), 0)
    for b in range(NEURONS // 32):
        piece = jnp.where(inside, pieces_ref[pl.ds(b * 32, 32), :], 0.0)
        out_ref[:, b * LANES : (b + 1) * LANES] = jnp.sum(piece, axis=0, keepdims=True)


def join(pieces):
    return pl.pallas_call(
        join_kernel,
        out_shape=jax.ShapeDtypeStruct((1, SPAN * NEURONS), jnp.float32),
        in_specs=[VMEM],
        out_specs=VMEM,
        name="join",
    )(pieces)


def local(movie, shifts, footprint, support, neuron_ids, owner_order, start_traces):
    tiled, base = filter_tiles(movie[0], shifts[0], neuron_ids[0], owner_order, start_traces)
    tile_movie = lax.all_to_all(tiled, TA, split_axis=0, concat_axis=0, tiled=True)
    tile_movie = tile_movie.reshape(-1, TH * TW)
    mail = project(tile_movie, footprint[0, 0], support[0, 0], base)
    mail = lax.all_to_all(mail.reshape(NEURONS, 1, LANES), TA_ROW, 0, 0, tiled=True)
    pieces = solve(mail.reshape(NEURONS, LANES))
    pieces = lax.all_to_all(pieces.reshape(NEURONS, 1, LANES), TA_ROW, 0, 0, tiled=True)
    return (tile_movie[None, None], join(pieces.reshape(NEURONS, LANES)))


def solution(mesh):
    finer = Mesh(mesh.devices.reshape(4, 4, 8, mesh.shape["row"]), ("ta_0", "ta_1", "ta_2", "row"))
    return jax.shard_map(
        local,
        mesh=finer,
        in_specs=(
            P("row", TA, None, None),
            P("row", TA, None, None),
            P("row", TA, None, None),
            P("row", TA, None, None),
            P("row", TA, None),
            P(),
            P(TA_ROW, None),
        ),
        out_specs=(P("row", TA, None, None), P(TA_ROW, None)),
        check_vma=False,
    )
```

```python
import jax
import jax.numpy as jnp
import numpy as np
from jax import lax
from jax.experimental import pallas as pl
from jax.experimental.pallas import tpu as pltpu
from jax.sharding import Mesh
from jax.sharding import PartitionSpec as P

TH = 16
TW = 32
MAXS = 8
ITERS = 2
TA = ("ta_0", "ta_1", "ta_2")
TA_ROW = ("ta_0", "ta_1", "ta_2", "row")

FRAMES = 8
H = 128
W = 512
LANES = 128
BLOCKS = W // LANES
SLOTS = 8
NEURONS = 256
TILES = 128
PIXELS = TH * TW
LINE = 8
MESSAGE = PIXELS + LANES
ID_LANE = 64
HIGHEST = lax.Precision.HIGHEST
VMEM = pl.BlockSpec(memory_space=pltpu.VMEM)
SMEM = pl.BlockSpec(memory_space=pltpu.SMEM)


def smoothing_table(length):
    places = np.arange(length, dtype=np.float32)
    spread = places[:, None] - places[None, :]
    kernel = np.exp(-spread * spread / np.float32(32.0)).astype(np.float32)
    return (kernel / np.sum(kernel, axis=0, keepdims=True, dtype=np.float32)).astype(jnp.bfloat16)


def iota(shape, dim):
    return lax.broadcasted_iota(jnp.int32, shape, dim)


def split3(value):
    high = value.astype(jnp.bfloat16)
    rest = value - high.astype(jnp.float32)
    mid = rest.astype(jnp.bfloat16)
    low = (rest - mid.astype(jnp.float32)).astype(jnp.bfloat16)
    return high, mid, low


def dot32(left, right):
    return jnp.dot(left, right, preferred_element_type=jnp.float32)


def place(value, exact):
    high, mid, low = split3(value)
    return dot32(high, exact) + (dot32(mid, exact) + dot32(low, exact))


def filter_kernel(
    shifts_ref, movie_ref, wide_ref, tall_ref, out_ref, padded_ref, registered_ref, filtered_ref,
):
    lane = iota((H, LANES), 1)
    padded_ref[:, pl.ds(0, MAXS), :] = jnp.zeros((BLOCKS, MAXS, LANES), jnp.float32)
    padded_ref[:, pl.ds(MAXS + H, MAXS), :] = jnp.zeros((BLOCKS, MAXS, LANES), jnp.float32)

    def block(f, p):
        if p < 0 or p >= BLOCKS:
            return None
        return movie_ref[f, :, p * LANES : (p + 1) * LANES].astype(jnp.float32)

    def frame(f, carry):
        for p in range(BLOCKS):
            dy = shifts_ref[f, p, 0]
            dx = shifts_ref[f, p, 1]
            amount = jnp.where(dx > 0, LANES - dx, -dx)
            source = lane + dx

            def rolled(value):
                if value is None:
                    return jnp.zeros((H, LANES), jnp.float32)
                return pltpu.roll(value, amount, 1)

            inner = jnp.where(source >= LANES, rolled(block(f, p + 1)), rolled(block(f, p)))
            moved = jnp.where(source < 0, rolled(block(f, p - 1)), inner)
            padded_ref[p, pl.ds(MAXS, H), :] = moved
            registered_ref[:, p * LANES : (p + 1) * LANES] = padded_ref[p, pl.ds(MAXS + dy, H), :]
        registered = registered_ref[...]
        wide = dot32(registered.astype(jnp.bfloat16), wide_ref[...]).astype(jnp.bfloat16)
        filtered = registered - dot32(tall_ref[...], wide)
        for p in range(BLOCKS):
            filtered_ref[p, pl.ds(f, H, stride=FRAMES), :] = filtered[:, p * LANES : (p + 1) * LANES]
        return carry

    lax.fori_loop(0, FRAMES, frame, 0)
    lanes8 = iota((FRAMES, LANES), 1)
    near = lanes8 < 2 * TW
    even = lax.rem(lanes8 // TW, 2) == 0

    def tile_row(ty, carry):
        for q in range(4):
            for p in range(BLOCKS):
                v = []
                for r in range(4):
                    at = pl.multiple_of((ty * TH + 4 * q + r) * FRAMES, FRAMES)
                    v.append(filtered_ref[p, pl.ds(at, FRAMES), :])
                a0 = jnp.where(near, v[0], pltpu.roll(v[2], 64, 1))
                a2 = jnp.where(near, pltpu.roll(v[0], 64, 1), v[2])
                a1 = jnp.where(near, v[1], pltpu.roll(v[3], 64, 1))
                a3 = jnp.where(near, pltpu.roll(v[1], 64, 1), v[3])
                tiles = (
                    jnp.where(even, a0, pltpu.roll(a1, 32, 1)),
                    jnp.where(even, pltpu.roll(a0, 96, 1), a1),
                    jnp.where(even, a2, pltpu.roll(a3, 32, 1)),
                    jnp.where(even, pltpu.roll(a2, 96, 1), a3),
                )
                for m in range(4):
                    out_ref[ty * 16 + 4 * p + m, :, q * LANES : (q + 1) * LANES] = tiles[m].astype(jnp.bfloat16)
        return carry

    lax.fori_loop(0, H // TH, tile_row, 0)


def filter_tiles(movie, shifts):
    return pl.pallas_call(
        filter_kernel,
        out_shape=jax.ShapeDtypeStruct((TILES, FRAMES, PIXELS), jnp.bfloat16),
        in_specs=[SMEM, VMEM, VMEM, VMEM],
        out_specs=VMEM,
        scratch_shapes=[
            pltpu.VMEM((BLOCKS, H + 2 * MAXS, LANES), jnp.float32),
            pltpu.VMEM((H, W), jnp.float32),
            pltpu.VMEM((BLOCKS, H * FRAMES, LANES), jnp.float32),
        ],
        cost_estimate=pl.CostEstimate(flops=4_000_000_000, bytes_accessed=3_000_000, transcendentals=0),
        name="filter",
    )(shifts, movie, smoothing_table(W), smoothing_table(H).T)


def pack_kernel(ids_ref, order_ref, footprint_ref, support_ref, start_ref, out_ref):
    footprints = footprint_ref[...] * support_ref[...].astype(jnp.bfloat16)
    parts = jnp.concatenate(split3(start_ref[...]), axis=1)
    source = iota((3 * LANES, LINE * LANES), 0)
    target = iota((3 * LANES, LINE * LANES), 1)
    part, lane = source // LANES, lax.rem(source, LANES)
    half, z, frame = lane // 64, lax.rem(lane, 64) // FRAMES, lax.rem(lane, FRAMES)
    exact = jnp.where(target == z * LANES + part * 16 + half * FRAMES + frame, 1.0, 0.0).astype(jnp.bfloat16)
    pieces = dot32(parts, exact)
    row = iota((SLOTS, LANES), 0)
    lanes8 = iota((SLOTS, LANES), 1)
    owners = jnp.zeros((SLOTS, LANES), jnp.float32)
    for i in range(SLOTS):
        owner = order_ref[ids_ref[0, i]].astype(jnp.float32)
        owners = jnp.where((row == i) & (lanes8 == ID_LANE), owner, owners)
    for z in range(LINE):
        out_ref[z, :, :PIXELS] = footprints
        out_ref[z, :, PIXELS:] = (pieces[:, z * LANES : (z + 1) * LANES] + owners).astype(jnp.bfloat16)


def pack(ids, order, footprint, support, start):
    return pl.pallas_call(
        pack_kernel,
        out_shape=jax.ShapeDtypeStruct((LINE, SLOTS, MESSAGE), jnp.bfloat16),
        in_specs=[SMEM, SMEM, VMEM, VMEM, VMEM],
        out_specs=VMEM,
        cost_estimate=pl.CostEstimate(flops=200_000_000, bytes_accessed=200_000, transcendentals=0),
        name="pack",
    )(ids, order, footprint, support, start)


def project_kernel(
    where_ref, tiled_ref, here_ref, left_ref, right_ref, far_ref, far2_ref,
    out_ref, select_ref, high_ref, mid_ref, low_ref,
):
    x, y = where_ref[0], where_ref[1]
    rows = LINE * SLOTS
    same = iota((rows, LANES), 0) // SLOTS == lax.rem(iota((rows, LANES), 1), rows) // SLOTS
    mine = 4 * x + y
    own_row = iota((LINE, SLOTS, LANES), 1) == mine // 2
    back = lax.rem(LANES - FRAMES * lax.rem(mine, 2), LANES)
    contract = (((1,), (1,)), ((), ()))
    neuron = iota((rows, NEURONS), 1)
    out_ref[:, NEURONS + LANES :] = jnp.zeros((NEURONS, LANES), jnp.float32)
    blocks = []
    for ky in range(4):
        blocks.append((here_ref, ky, 0, ky))
        blocks.append((left_ref, ky, 1, ky))
        blocks.append((right_ref, ky, 3, ky))
        blocks.append((far_ref, ky, 2, ky) if ky < 2 else (far2_ref, ky - 2, 2, ky))
    for at, (ref, index, kx, ky) in enumerate(blocks):
        message = ref[index]
        tile = pl.multiple_of(LINE * (4 * lax.rem(x + 4 - kx, 4) + lax.rem(y + 4 - ky, 4)), LINE)
        frames = tiled_ref[pl.ds(tile, LINE)].reshape(LINE * FRAMES, PIXELS)
        prints = message[:, :, :PIXELS].reshape(rows, PIXELS)
        extra = message[:, :, PIXELS:].astype(jnp.float32)
        both = jnp.concatenate([frames, prints], axis=0)
        found = lax.dot_general(prints, both, contract, preferred_element_type=jnp.float32)
        found = jnp.where(same, found, 0.0)
        ids = extra.reshape(rows, LANES)[:, ID_LANE : ID_LANE + 1].astype(jnp.int32)
        select = jnp.where(neuron == ids, 1.0, 0.0).astype(jnp.bfloat16)
        spread = place(found[:, rows:], select)
        span = pl.ds(at * rows, rows)
        select_ref[span, :] = select
        for start, value in ((0, spread), (NEURONS, found)):
            end = start + value.shape[1]
            high, mid, low = split3(value)
            high_ref[span, start:end] = high
            mid_ref[span, start:end] = mid
            low_ref[span, start:end] = low
        piece = jnp.sum(jnp.where(own_row, extra, 0.0), axis=1)
        piece = pltpu.roll(piece, back, 1)
        piece = piece + (pltpu.roll(piece, LANES - 16, 1) + pltpu.roll(piece, LANES - 32, 1))
        out_ref[pl.ds(tile, LINE), NEURONS + LANES :] = piece
    select = select_ref[...]
    turn = (((0,), (0,)), ((), ()))

    def add(ref):
        return lax.dot_general(select, ref[...], turn, preferred_element_type=jnp.float32)

    out_ref[:, : NEURONS + LANES] = add(high_ref) + (add(mid_ref) + add(low_ref))


def project(where, tiled, here, left, right, far, far2):
    rows = TILES * SLOTS
    return pl.pallas_call(
        project_kernel,
        out_shape=jax.ShapeDtypeStruct((NEURONS, NEURONS + 2 * LANES), jnp.float32),
        in_specs=[SMEM] + [VMEM] * 6,
        out_specs=VMEM,
        scratch_shapes=[pltpu.VMEM((rows, NEURONS), jnp.bfloat16)]
        + [pltpu.VMEM((rows, NEURONS + LANES), jnp.bfloat16)] * 3,
        cost_estimate=pl.CostEstimate(flops=2_000_000_000, bytes_accessed=3_000_000, transcendentals=0),
        name="project",
    )(where, tiled, here, left, right, far, far2)


def solve_kernel(where_ref, mine_ref, other_ref, out_ref, current_ref):
    core = where_ref[2]
    sums = mine_ref[:, : NEURONS + LANES] + other_ref[:, : NEURONS + LANES]
    coupling = sums[:, :NEURONS]
    source = iota((LANES, LANES), 0)
    target = lax.rem(iota((LANES, LANES), 1), FRAMES)
    fold = jnp.where((lax.rem(source, FRAMES) == target) & (source < LINE * FRAMES), 1.0, 0.0)
    drive = place(sums[:, NEURONS:], fold.astype(jnp.bfloat16))
    copy = jnp.where(source == target, 1.0, 0.0).astype(jnp.bfloat16)
    here = mine_ref[:TILES, NEURONS + LANES :]
    there = other_ref[:TILES, NEURONS + LANES :]
    current_ref[pl.ds(0, TILES, stride=2), :] = place(jnp.where(core == 0, here, there), copy)
    current_ref[pl.ds(1, TILES, stride=2), :] = place(jnp.where(core == 0, there, here), copy)
    current = current_ref[...]
    bound = 1.0 + jnp.sum(coupling, axis=1, keepdims=True)
    for _ in range(ITERS):
        product = jnp.dot(coupling, current, preferred_element_type=jnp.float32, precision=HIGHEST)
        current = jnp.maximum(current - (product - drive) / bound, 0.0)
    current_ref[...] = current
    even = current_ref[pl.ds(0, TILES, stride=2), :]
    odd = current_ref[pl.ds(1, TILES, stride=2), :]
    out_ref[...] = jnp.where(core == 0, even, odd)


def solve(where, mine, other):
    return pl.pallas_call(
        solve_kernel,
        out_shape=jax.ShapeDtypeStruct((TILES, LANES), jnp.float32),
        in_specs=[SMEM, VMEM, VMEM],
        out_specs=VMEM,
        scratch_shapes=[pltpu.VMEM((NEURONS, LANES), jnp.float32)],
        cost_estimate=pl.CostEstimate(flops=2_000_000_000, bytes_accessed=1_000_000, transcendentals=0),
        name="solve",
    )(where, mine, other)


def join_kernel(pieces_ref, out_ref):
    near = LANES // FRAMES
    inside = iota((near, LANES), 1) // FRAMES == iota((near, LANES), 0)
    for b in range(TILES // near):
        piece = jnp.where(inside, pieces_ref[pl.ds(b * near, near), :], 0.0)
        out_ref[:, b * LANES : (b + 1) * LANES] = jnp.sum(piece, axis=0, keepdims=True)


def join(pieces):
    return pl.pallas_call(
        join_kernel,
        out_shape=jax.ShapeDtypeStruct((1, TILES * FRAMES), jnp.float32),
        in_specs=[VMEM],
        out_specs=VMEM,
        name="join",
    )(pieces)


def moved(array, axis, by):
    count = lax.axis_size(axis)
    return lax.ppermute(array, axis, [(i, (i + by) % count) for i in range(count)])


def local(movie, shifts, footprint, support, neuron_ids, owner_order, start_traces):
    where = jnp.stack([lax.axis_index(axis) for axis in ("ta_0", "ta_1", "row")]).astype(jnp.int32)
    packed = pack(neuron_ids[0], owner_order, footprint[0, 0], support[0, 0], start_traces.reshape(8, LANES))
    line = lax.all_to_all(packed, "ta_2", 0, 0, tiled=True)
    tiled = filter_tiles(movie[0], shifts[0])
    tile_movie = lax.all_to_all(tiled, TA, split_axis=0, concat_axis=0, tiled=True)
    here = jnp.stack([line] + [moved(line, "ta_1", by) for by in range(1, 4)])
    left = moved(here, "ta_0", 1)
    right = moved(here, "ta_0", 3)
    far = moved(left[:2], "ta_0", 1)
    far2 = moved(right[2:], "ta_0", 3)
    mine = project(where, tiled, here, left, right, far, far2)
    other = moved(mine, "row", 1)
    pieces = solve(where, mine, other)
    pieces = lax.all_to_all(pieces.reshape(TILES, 1, LANES), TA, 0, 0, tiled=True)
    traces = join(pieces.reshape(TILES, LANES))
    return (tile_movie.reshape(1, 1, -1, PIXELS), traces)


def solution(mesh):
    finer = Mesh(mesh.devices.reshape(4, 4, 8, mesh.shape["row"]), TA_ROW)
    return jax.shard_map(
        local,
        mesh=finer,
        in_specs=(
            P("row", TA, None, None),
            P("row", TA, None, None),
            P("row", TA, None, None),
            P("row", TA, None, None),
            P("row", TA, None),
            P(),
            P(TA_ROW, None),
        ),
        out_specs=(P("row", TA, None, None), P(TA_ROW, None)),
        check_vma=False,
    )
```

```python
import jax
import jax.numpy as jnp
import numpy as np
from jax import lax
from jax.experimental import pallas as pl
from jax.experimental.pallas import tpu as pltpu
from jax.sharding import Mesh
from jax.sharding import PartitionSpec as P

TH = 16
TW = 32
MAXS = 8
ITERS = 2
TA = ("ta_0", "ta_1", "ta_2")
TA_ROW = ("ta_0", "ta_1", "ta_2", "row")

FRAMES = 8
H = 128
W = 512
LANES = 128
BLOCKS = W // LANES
SLOTS = 8
NEURONS = 256
TILES = 128
PIXELS = TH * TW
LINE = 8
MESSAGE = PIXELS + LANES
ID_LANE = 64
HIGHEST = lax.Precision.HIGHEST
VMEM = pl.BlockSpec(memory_space=pltpu.VMEM)
SMEM = pl.BlockSpec(memory_space=pltpu.SMEM)


def smoothing_table(length):
    places = np.arange(length, dtype=np.float32)
    spread = places[:, None] - places[None, :]
    kernel = np.exp(-spread * spread / np.float32(32.0)).astype(np.float32)
    return (kernel / np.sum(kernel, axis=0, keepdims=True, dtype=np.float32)).astype(jnp.bfloat16)


def iota(shape, dim):
    return lax.broadcasted_iota(jnp.int32, shape, dim)


def split3(value):
    high = value.astype(jnp.bfloat16)
    rest = value - high.astype(jnp.float32)
    mid = rest.astype(jnp.bfloat16)
    low = (rest - mid.astype(jnp.float32)).astype(jnp.bfloat16)
    return high, mid, low


def dot32(left, right):
    return jnp.dot(left, right, preferred_element_type=jnp.float32)


def place(value, exact):
    high, mid, low = split3(value)
    return dot32(high, exact) + (dot32(mid, exact) + dot32(low, exact))


def filter_kernel(
    shifts_ref, movie_ref, wide_ref, tall_ref, out_ref, padded_ref, registered_ref, filtered_ref,
):
    lane = iota((H, LANES), 1)
    padded_ref[:, pl.ds(0, MAXS), :] = jnp.zeros((BLOCKS, MAXS, LANES), jnp.float32)
    padded_ref[:, pl.ds(MAXS + H, MAXS), :] = jnp.zeros((BLOCKS, MAXS, LANES), jnp.float32)

    def block(f, p):
        if p < 0 or p >= BLOCKS:
            return None
        return movie_ref[f, :, p * LANES : (p + 1) * LANES].astype(jnp.float32)

    def frame(f, carry):
        for p in range(BLOCKS):
            dy = shifts_ref[f, p, 0]
            dx = shifts_ref[f, p, 1]
            amount = jnp.where(dx > 0, LANES - dx, -dx)
            source = lane + dx

            def rolled(value):
                if value is None:
                    return jnp.zeros((H, LANES), jnp.float32)
                return pltpu.roll(value, amount, 1)

            inner = jnp.where(source >= LANES, rolled(block(f, p + 1)), rolled(block(f, p)))
            moved = jnp.where(source < 0, rolled(block(f, p - 1)), inner)
            padded_ref[p, pl.ds(MAXS, H), :] = moved
            registered_ref[:, p * LANES : (p + 1) * LANES] = padded_ref[p, pl.ds(MAXS + dy, H), :]
        registered = registered_ref[...]
        wide = dot32(registered.astype(jnp.bfloat16), wide_ref[...]).astype(jnp.bfloat16)
        filtered = registered - dot32(tall_ref[...], wide)
        for p in range(BLOCKS):
            filtered_ref[p, pl.ds(f, H, stride=FRAMES), :] = filtered[:, p * LANES : (p + 1) * LANES]
        return carry

    lax.fori_loop(0, FRAMES, frame, 0)
    lanes8 = iota((FRAMES, LANES), 1)
    near = lanes8 < 2 * TW
    even = lax.rem(lanes8 // TW, 2) == 0

    def tile_row(ty, carry):
        for q in range(4):
            for p in range(BLOCKS):
                v = []
                for r in range(4):
                    at = pl.multiple_of((ty * TH + 4 * q + r) * FRAMES, FRAMES)
                    v.append(filtered_ref[p, pl.ds(at, FRAMES), :])
                a0 = jnp.where(near, v[0], pltpu.roll(v[2], 64, 1))
                a2 = jnp.where(near, pltpu.roll(v[0], 64, 1), v[2])
                a1 = jnp.where(near, v[1], pltpu.roll(v[3], 64, 1))
                a3 = jnp.where(near, pltpu.roll(v[1], 64, 1), v[3])
                tiles = (
                    jnp.where(even, a0, pltpu.roll(a1, 32, 1)),
                    jnp.where(even, pltpu.roll(a0, 96, 1), a1),
                    jnp.where(even, a2, pltpu.roll(a3, 32, 1)),
                    jnp.where(even, pltpu.roll(a2, 96, 1), a3),
                )
                for m in range(4):
                    out_ref[ty * 16 + 4 * p + m, :, q * LANES : (q + 1) * LANES] = tiles[m].astype(jnp.bfloat16)
        return carry

    lax.fori_loop(0, H // TH, tile_row, 0)


def filter_tiles(movie, shifts):
    return pl.pallas_call(
        filter_kernel,
        out_shape=jax.ShapeDtypeStruct((TILES, FRAMES, PIXELS), jnp.bfloat16),
        in_specs=[SMEM, VMEM, VMEM, VMEM],
        out_specs=VMEM,
        scratch_shapes=[
            pltpu.VMEM((BLOCKS, H + 2 * MAXS, LANES), jnp.float32),
            pltpu.VMEM((H, W), jnp.float32),
            pltpu.VMEM((BLOCKS, H * FRAMES, LANES), jnp.float32),
        ],
        cost_estimate=pl.CostEstimate(flops=4_000_000_000, bytes_accessed=3_000_000, transcendentals=0),
        compiler_params=pltpu.CompilerParams(vmem_limit_bytes=16 << 20),
        name="filter",
    )(shifts, movie, smoothing_table(W), smoothing_table(H).T)


def pack_kernel(ids_ref, order_ref, footprint_ref, support_ref, start_ref, out_ref):
    footprints = footprint_ref[...] * support_ref[...].astype(jnp.bfloat16)
    parts = jnp.concatenate(split3(start_ref[...]), axis=1)
    source = iota((3 * LANES, LINE * LANES), 0)
    target = iota((3 * LANES, LINE * LANES), 1)
    part, lane = source // LANES, lax.rem(source, LANES)
    half, z, frame = lane // 64, lax.rem(lane, 64) // FRAMES, lax.rem(lane, FRAMES)
    exact = jnp.where(target == z * LANES + part * 16 + half * FRAMES + frame, 1.0, 0.0).astype(jnp.bfloat16)
    pieces = dot32(parts, exact)
    row = iota((SLOTS, LANES), 0)
    lanes8 = iota((SLOTS, LANES), 1)
    owners = jnp.zeros((SLOTS, LANES), jnp.float32)
    for i in range(SLOTS):
        owner = order_ref[ids_ref[0, i]].astype(jnp.float32)
        owners = jnp.where((row == i) & (lanes8 == ID_LANE), owner, owners)
    for z in range(LINE):
        out_ref[z, :, :PIXELS] = footprints
        out_ref[z, :, PIXELS:] = (pieces[:, z * LANES : (z + 1) * LANES] + owners).astype(jnp.bfloat16)


def pack(ids, order, footprint, support, start):
    return pl.pallas_call(
        pack_kernel,
        out_shape=jax.ShapeDtypeStruct((LINE, SLOTS, MESSAGE), jnp.bfloat16),
        in_specs=[SMEM, SMEM, VMEM, VMEM, VMEM],
        out_specs=VMEM,
        cost_estimate=pl.CostEstimate(flops=200_000_000, bytes_accessed=200_000, transcendentals=0),
        compiler_params=pltpu.CompilerParams(vmem_limit_bytes=4 << 20),
        name="pack",
    )(ids, order, footprint, support, start)


def project_kernel(
    where_ref, tiled_ref, here_ref, left_ref, far_ref, right_ref, out_ref, select_ref, terms_ref
):
    x, y = where_ref[0], where_ref[1]
    rows = 2 * LINE * SLOTS
    width = NEURONS + LANES
    same = iota((rows, 2 * rows), 0) // SLOTS == lax.rem(iota((rows, 2 * rows), 1), rows) // SLOTS
    mine = 4 * x + y
    own_row = iota((2 * LINE, SLOTS, LANES), 1) == mine // 2
    back = lax.rem(LANES - FRAMES * lax.rem(mine, 2), LANES)
    contract = (((1,), (1,)), ((), ()))
    neuron = iota((rows, NEURONS), 1)
    neuron_t = iota((NEURONS, rows), 0)
    diagonal = iota((rows, rows), 0) == iota((rows, rows), 1)
    out_ref[:, width:] = jnp.zeros((NEURONS, LANES), jnp.float32)
    for at in range(8):
        kx, first = at // 2, 2 * (at % 2)
        ref = (here_ref, left_ref, far_ref, right_ref)[kx]
        tiles = [
            pl.multiple_of(LINE * (4 * lax.rem(x + 4 - kx, 4) + lax.rem(y + 4 - ky, 4)), LINE)
            for ky in (first, first + 1)
        ]
        message = ref[first : first + 2]
        frames = [tiled_ref[pl.ds(tile, LINE)].reshape(rows // 2, PIXELS) for tile in tiles]
        prints = message[:, :, :, :PIXELS].reshape(rows, PIXELS)
        extra = message[:, :, :, PIXELS:].astype(jnp.float32).reshape(rows, LANES)
        found = lax.dot_general(
            prints, jnp.concatenate(frames + [prints], axis=0), contract, preferred_element_type=jnp.float32
        )
        found = jnp.where(same, found, 0.0)
        ids = extra[:, ID_LANE : ID_LANE + 1]
        select = jnp.where(neuron == ids.astype(jnp.int32), 1.0, 0.0).astype(jnp.bfloat16)
        ids_row = jnp.sum(jnp.where(diagonal, ids, 0.0), axis=0, keepdims=True).astype(jnp.int32)
        span = slice(at * rows, (at + 1) * rows)
        select_ref[:, span] = jnp.where(neuron_t == ids_row, 1.0, 0.0).astype(jnp.bfloat16)
        spread = place(found[:, rows:], select)
        for k, (one, two) in enumerate(zip(split3(spread), split3(found[:, :rows]), strict=True)):
            terms_ref[span, k * width : k * width + NEURONS] = one
            terms_ref[span, k * width + NEURONS : (k + 1) * width] = two
        piece = jnp.sum(jnp.where(own_row, extra.reshape(2 * LINE, SLOTS, LANES), 0.0), axis=1)
        piece = pltpu.roll(piece, back, 1)
        piece = piece + (pltpu.roll(piece, LANES - 16, 1) + pltpu.roll(piece, LANES - 32, 1))
        for k in range(2):
            out_ref[pl.ds(tiles[k], LINE), width:] = piece[k * LINE : (k + 1) * LINE]
    sums = dot32(select_ref[...], terms_ref[...])
    out_ref[:, :width] = sums[:, :width] + (sums[:, width : 2 * width] + sums[:, 2 * width :])


def project(where, tiled, here, left, far, right):
    rows = TILES * SLOTS
    return pl.pallas_call(
        project_kernel,
        out_shape=jax.ShapeDtypeStruct((NEURONS, NEURONS + 2 * LANES), jnp.float32),
        in_specs=[SMEM] + [VMEM] * 5,
        out_specs=VMEM,
        scratch_shapes=[
            pltpu.VMEM((NEURONS, rows), jnp.bfloat16),
            pltpu.VMEM((rows, 3 * (NEURONS + LANES)), jnp.bfloat16),
        ],
        cost_estimate=pl.CostEstimate(flops=2_000_000_000, bytes_accessed=3_000_000, transcendentals=0),
        compiler_params=pltpu.CompilerParams(vmem_limit_bytes=16 << 20),
        name="project",
    )(where, tiled, here, left, far, right)


def solve_kernel(where_ref, mine_ref, other_ref, out_ref, current_ref):
    core = where_ref[2]
    sums = mine_ref[:, : NEURONS + LANES] + other_ref[:, : NEURONS + LANES]
    coupling = sums[:, :NEURONS]
    source = iota((LANES, LANES), 0)
    target = lax.rem(iota((LANES, LANES), 1), FRAMES)
    fold = jnp.where(lax.rem(source, FRAMES) == target, 1.0, 0.0)
    drive = place(sums[:, NEURONS:], fold.astype(jnp.bfloat16))
    copy = jnp.where(source == target, 1.0, 0.0).astype(jnp.bfloat16)
    here = mine_ref[:TILES, NEURONS + LANES :]
    there = other_ref[:TILES, NEURONS + LANES :]
    current_ref[pl.ds(0, TILES, stride=2), :] = place(jnp.where(core == 0, here, there), copy)
    current_ref[pl.ds(1, TILES, stride=2), :] = place(jnp.where(core == 0, there, here), copy)
    current = current_ref[...]
    bound = 1.0 + jnp.sum(coupling, axis=1, keepdims=True)
    for _ in range(ITERS):
        product = jnp.dot(coupling, current, preferred_element_type=jnp.float32, precision=HIGHEST)
        current = jnp.maximum(current - (product - drive) / bound, 0.0)
    current_ref[...] = current
    even = current_ref[pl.ds(0, TILES, stride=2), :]
    odd = current_ref[pl.ds(1, TILES, stride=2), :]
    out_ref[...] = jnp.where(core == 0, even, odd)


def solve(where, mine, other):
    return pl.pallas_call(
        solve_kernel,
        out_shape=jax.ShapeDtypeStruct((TILES, LANES), jnp.float32),
        in_specs=[SMEM, VMEM, VMEM],
        out_specs=VMEM,
        scratch_shapes=[pltpu.VMEM((NEURONS, LANES), jnp.float32)],
        cost_estimate=pl.CostEstimate(flops=2_000_000_000, bytes_accessed=1_000_000, transcendentals=0),
        compiler_params=pltpu.CompilerParams(vmem_limit_bytes=8 << 20),
        name="solve",
    )(where, mine, other)


def join_kernel(pieces_ref, out_ref):
    near = LANES // FRAMES
    inside = iota((near, LANES), 1) // FRAMES == iota((near, LANES), 0)
    for b in range(TILES // near):
        piece = jnp.where(inside, pieces_ref[pl.ds(b * near, near), :], 0.0)
        out_ref[:, b * LANES : (b + 1) * LANES] = jnp.sum(piece, axis=0, keepdims=True)


def join(pieces):
    return pl.pallas_call(
        join_kernel,
        out_shape=jax.ShapeDtypeStruct((1, TILES * FRAMES), jnp.float32),
        in_specs=[VMEM],
        out_specs=VMEM,
        compiler_params=pltpu.CompilerParams(vmem_limit_bytes=2 << 20),
        name="join",
    )(pieces)


def moved(array, axis, by):
    count = lax.axis_size(axis)
    return lax.ppermute(array, axis, [(i, (i + by) % count) for i in range(count)])


def local(movie, shifts, footprint, support, neuron_ids, owner_order, start_traces):
    where = jnp.stack([lax.axis_index(axis) for axis in ("ta_0", "ta_1", "row")]).astype(jnp.int32)
    packed = pack(neuron_ids[0], owner_order, footprint[0, 0], support[0, 0], start_traces.reshape(8, LANES))
    line = lax.all_to_all(packed, "ta_2", 0, 0, tiled=True)
    tiled = filter_tiles(movie[0], shifts[0])
    tile_movie = lax.all_to_all(tiled, TA, split_axis=0, concat_axis=0, tiled=True)
    here = jnp.stack([line] + [moved(line, "ta_1", by) for by in range(1, 4)])
    left, far, right = [moved(here, "ta_0", by) for by in range(1, 4)]
    mine = project(where, tiled, here, left, far, right)
    other = moved(mine, "row", 1)
    pieces = solve(where, mine, other)
    pieces = lax.all_to_all(pieces.reshape(TILES, 1, LANES), TA, 0, 0, tiled=True)
    traces = join(pieces.reshape(TILES, LANES))
    return (tile_movie.reshape(1, 1, -1, PIXELS), traces)


def solution(mesh):
    finer = Mesh(mesh.devices.reshape(4, 4, 8, mesh.shape["row"]), TA_ROW)
    return jax.shard_map(
        local,
        mesh=finer,
        in_specs=(
            P("row", TA, None, None),
            P("row", TA, None, None),
            P("row", TA, None, None),
            P("row", TA, None, None),
            P("row", TA, None),
            P(),
            P(TA_ROW, None),
        ),
        out_specs=(P("row", TA, None, None), P(TA_ROW, None)),
        check_vma=False,
    )
```

```python
import jax
import jax.numpy as jnp
import numpy as np
from jax import lax
from jax.experimental import pallas as pl
from jax.experimental.pallas import tpu as pltpu
from jax.sharding import Mesh
from jax.sharding import PartitionSpec as P

TH = 16
TW = 32
MAXS = 8
ITERS = 2
TA = ("ta_0", "ta_1", "ta_2")
YZ = ("ta_1", "ta_2")
TA_ROW = ("ta_0", "ta_1", "ta_2", "row")

FRAMES = 8
H = 128
W = 512
LANES = 128
BLOCKS = W // LANES
SLOTS = 8
NEURONS = 256
TILES = 128
PIXELS = TH * TW
PLANE = 32
PLANES = 4
MESSAGE = PIXELS + LANES
ID_LANE = 64
HIGHEST = lax.Precision.HIGHEST
VMEM = pl.BlockSpec(memory_space=pltpu.VMEM)
SMEM = pl.BlockSpec(memory_space=pltpu.SMEM)


def smoothing_table(length):
    places = np.arange(length, dtype=np.float32)
    spread = places[:, None] - places[None, :]
    kernel = np.exp(-spread * spread / np.float32(32.0)).astype(np.float32)
    return (kernel / np.sum(kernel, axis=0, keepdims=True, dtype=np.float32)).astype(jnp.bfloat16)


def iota(shape, dim):
    return lax.broadcasted_iota(jnp.int32, shape, dim)


def split3(value):
    high = value.astype(jnp.bfloat16)
    rest = value - high.astype(jnp.float32)
    mid = rest.astype(jnp.bfloat16)
    low = (rest - mid.astype(jnp.float32)).astype(jnp.bfloat16)
    return high, mid, low


def dot32(left, right):
    return jnp.dot(left, right, preferred_element_type=jnp.float32)


def place(value, exact):
    high, mid, low = split3(value)
    return dot32(high, exact) + (dot32(mid, exact) + dot32(low, exact))


def filter_kernel(
    shifts_ref, movie_ref, wide_ref, tall_ref, out_ref, padded_ref, registered_ref, filtered_ref,
):
    lane = iota((H, LANES), 1)
    padded_ref[:, pl.ds(0, MAXS), :] = jnp.zeros((BLOCKS, MAXS, LANES), jnp.float32)
    padded_ref[:, pl.ds(MAXS + H, MAXS), :] = jnp.zeros((BLOCKS, MAXS, LANES), jnp.float32)

    def block(f, p):
        if p < 0 or p >= BLOCKS:
            return None
        return movie_ref[f, :, p * LANES : (p + 1) * LANES].astype(jnp.float32)

    def frame(f, carry):
        for p in range(BLOCKS):
            dy = shifts_ref[f, p, 0]
            dx = shifts_ref[f, p, 1]
            amount = jnp.where(dx > 0, LANES - dx, -dx)
            source = lane + dx

            def rolled(value):
                if value is None:
                    return jnp.zeros((H, LANES), jnp.float32)
                return pltpu.roll(value, amount, 1)

            inner = jnp.where(source >= LANES, rolled(block(f, p + 1)), rolled(block(f, p)))
            moved = jnp.where(source < 0, rolled(block(f, p - 1)), inner)
            padded_ref[p, pl.ds(MAXS, H), :] = moved
            registered_ref[:, p * LANES : (p + 1) * LANES] = padded_ref[p, pl.ds(MAXS + dy, H), :]
        registered = registered_ref[...]
        wide = dot32(registered.astype(jnp.bfloat16), wide_ref[...]).astype(jnp.bfloat16)
        filtered = registered - dot32(tall_ref[...], wide)
        for p in range(BLOCKS):
            filtered_ref[p, pl.ds(f, H, stride=FRAMES), :] = filtered[:, p * LANES : (p + 1) * LANES]
        return carry

    lax.fori_loop(0, FRAMES, frame, 0)
    lanes8 = iota((FRAMES, LANES), 1)
    near = lanes8 < 2 * TW
    even = lax.rem(lanes8 // TW, 2) == 0

    def tile_row(ty, carry):
        for q in range(4):
            for p in range(BLOCKS):
                v = []
                for r in range(4):
                    at = pl.multiple_of((ty * TH + 4 * q + r) * FRAMES, FRAMES)
                    v.append(filtered_ref[p, pl.ds(at, FRAMES), :])
                a0 = jnp.where(near, v[0], pltpu.roll(v[2], 64, 1))
                a2 = jnp.where(near, pltpu.roll(v[0], 64, 1), v[2])
                a1 = jnp.where(near, v[1], pltpu.roll(v[3], 64, 1))
                a3 = jnp.where(near, pltpu.roll(v[1], 64, 1), v[3])
                tiles = (
                    jnp.where(even, a0, pltpu.roll(a1, 32, 1)),
                    jnp.where(even, pltpu.roll(a0, 96, 1), a1),
                    jnp.where(even, a2, pltpu.roll(a3, 32, 1)),
                    jnp.where(even, pltpu.roll(a2, 96, 1), a3),
                )
                for m in range(4):
                    out_ref[ty * 16 + 4 * p + m, :, q * LANES : (q + 1) * LANES] = tiles[m].astype(jnp.bfloat16)
        return carry

    lax.fori_loop(0, H // TH, tile_row, 0)


def filter_tiles(movie, shifts):
    return pl.pallas_call(
        filter_kernel,
        out_shape=jax.ShapeDtypeStruct((TILES, FRAMES, PIXELS), jnp.bfloat16),
        in_specs=[SMEM, VMEM, VMEM, VMEM],
        out_specs=VMEM,
        scratch_shapes=[
            pltpu.VMEM((BLOCKS, H + 2 * MAXS, LANES), jnp.float32),
            pltpu.VMEM((H, W), jnp.float32),
            pltpu.VMEM((BLOCKS, H * FRAMES, LANES), jnp.float32),
        ],
        cost_estimate=pl.CostEstimate(flops=4_000_000_000, bytes_accessed=3_000_000, transcendentals=0),
        compiler_params=pltpu.CompilerParams(vmem_limit_bytes=16 << 20),
        name="filter",
    )(shifts, movie, smoothing_table(W), smoothing_table(H).T)


def pack_kernel(ids_ref, order_ref, footprint_ref, support_ref, start_ref, out_ref):
    footprints = footprint_ref[...] * support_ref[...].astype(jnp.bfloat16)
    parts = [part.astype(jnp.float32) for part in split3(start_ref[...])]
    row = iota((SLOTS, LANES), 0)
    lane = iota((SLOTS, LANES), 1)
    owners = jnp.zeros((SLOTS, LANES), jnp.float32)
    for i in range(SLOTS):
        owner = order_ref[ids_ref[0, i]].astype(jnp.float32)
        owners = jnp.where((row == i) & (lane == ID_LANE), owner, owners)
    for w in range(PLANE // 2):
        extra = owners
        for k, part in enumerate(parts):
            extra = jnp.where(lane // FRAMES == k, pltpu.roll(part, (FRAMES * (k - w)) % LANES, 1), extra)
        for to in (w, w + PLANE // 2):
            out_ref[to, :, :PIXELS] = footprints
            out_ref[to, :, PIXELS:] = extra.astype(jnp.bfloat16)


def pack(ids, order, footprint, support, start):
    return pl.pallas_call(
        pack_kernel,
        out_shape=jax.ShapeDtypeStruct((PLANE, SLOTS, MESSAGE), jnp.bfloat16),
        in_specs=[SMEM, SMEM, VMEM, VMEM, VMEM],
        out_specs=VMEM,
        cost_estimate=pl.CostEstimate(flops=200_000_000, bytes_accessed=200_000, transcendentals=0),
        name="pack",
    )(ids, order, footprint, support, start)


def project_kernel(
    where_ref, tiled_ref, here_ref, left_ref, far_ref, right_ref, out_ref, select_ref, terms_ref
):
    x, y = where_ref[0], where_ref[1]
    many = PLANE // 2
    rows = many * SLOTS
    width = NEURONS + LANES
    same = iota((rows, 2 * rows), 0) // SLOTS == lax.rem(iota((rows, 2 * rows), 1), rows) // SLOTS
    own_row = iota((many, SLOTS, LANES), 1) == 2 * x + y // 2
    contract = (((1,), (1,)), ((), ()))
    neuron = iota((rows, NEURONS), 1)
    neuron_t = iota((NEURONS, rows), 0)
    diagonal = iota((rows, rows), 0) == iota((rows, rows), 1)
    out_ref[:, width:] = jnp.zeros((NEURONS, LANES), jnp.float32)
    for at in range(2 * PLANES):
        kx, first = at // 2, many * (at % 2)
        message = (here_ref, left_ref, far_ref, right_ref)[kx][first : first + many]
        tile = pl.multiple_of(PLANE * lax.rem(x + PLANES - kx, PLANES) + first, many)
        frames = tiled_ref[pl.ds(tile, many)].reshape(rows, PIXELS)
        prints = message[:, :, :PIXELS].reshape(rows, PIXELS)
        extra = message[:, :, PIXELS:].astype(jnp.float32).reshape(rows, LANES)
        found = lax.dot_general(
            prints, jnp.concatenate([frames, prints], axis=0), contract, preferred_element_type=jnp.float32
        )
        found = jnp.where(same, found, 0.0)
        ids = extra[:, ID_LANE : ID_LANE + 1]
        select = jnp.where(neuron == ids.astype(jnp.int32), 1.0, 0.0).astype(jnp.bfloat16)
        ids_row = jnp.sum(jnp.where(diagonal, ids, 0.0), axis=0, keepdims=True).astype(jnp.int32)
        span = slice(at * rows, (at + 1) * rows)
        select_ref[:, span] = jnp.where(neuron_t == ids_row, 1.0, 0.0).astype(jnp.bfloat16)
        spread = place(found[:, rows:], select)
        for k, (one, two) in enumerate(zip(split3(spread), split3(found[:, :rows]), strict=True)):
            terms_ref[span, k * width : k * width + NEURONS] = one
            terms_ref[span, k * width + NEURONS : (k + 1) * width] = two
        piece = jnp.sum(jnp.where(own_row, extra.reshape(many, SLOTS, LANES), 0.0), axis=1)
        piece = piece + (pltpu.roll(piece, LANES - FRAMES, 1) + pltpu.roll(piece, LANES - 2 * FRAMES, 1))
        out_ref[pl.ds(tile, many), width:] = piece
    sums = dot32(select_ref[...], terms_ref[...])
    out_ref[:, :width] = sums[:, :width] + (sums[:, width : 2 * width] + sums[:, 2 * width :])


def project(where, tiled, here, left, far, right):
    rows = TILES * SLOTS
    return pl.pallas_call(
        project_kernel,
        out_shape=jax.ShapeDtypeStruct((NEURONS, NEURONS + 2 * LANES), jnp.float32),
        in_specs=[SMEM] + [VMEM] * 5,
        out_specs=VMEM,
        scratch_shapes=[
            pltpu.VMEM((NEURONS, rows), jnp.bfloat16),
            pltpu.VMEM((rows, 3 * (NEURONS + LANES)), jnp.bfloat16),
        ],
        cost_estimate=pl.CostEstimate(flops=2_000_000_000, bytes_accessed=3_000_000, transcendentals=0),
        compiler_params=pltpu.CompilerParams(vmem_limit_bytes=16 << 20),
        name="project",
    )(where, tiled, here, left, far, right)


def solve_kernel(where_ref, mine_ref, other_ref, *refs):
    out_refs, current_ref, own_ref = refs[:PLANES], refs[PLANES], refs[PLANES + 1]
    x, core = where_ref[0], where_ref[2]
    sums = mine_ref[:, : NEURONS + LANES] + other_ref[:, : NEURONS + LANES]
    coupling = sums[:, :NEURONS]
    source = iota((LANES, LANES), 0)
    target = lax.rem(iota((LANES, LANES), 1), FRAMES)
    fold = jnp.where(lax.rem(source, FRAMES) == target, 1.0, 0.0)
    drive = place(sums[:, NEURONS:], fold.astype(jnp.bfloat16))
    copy = jnp.where(source == target, 1.0, 0.0).astype(jnp.bfloat16)
    here = mine_ref[:TILES, NEURONS + LANES :]
    there = other_ref[:TILES, NEURONS + LANES :]
    current_ref[pl.ds(0, TILES, stride=2), :] = place(jnp.where(core == 0, here, there), copy)
    current_ref[pl.ds(1, TILES, stride=2), :] = place(jnp.where(core == 0, there, here), copy)
    current = current_ref[...]
    bound = 1.0 + jnp.sum(coupling, axis=1, keepdims=True)
    for _ in range(ITERS):
        product = jnp.dot(coupling, current, preferred_element_type=jnp.float32, precision=HIGHEST)
        current = jnp.maximum(current - (product - drive) / bound, 0.0)
    current_ref[...] = current
    even = current_ref[pl.ds(0, TILES, stride=2), :]
    odd = current_ref[pl.ds(1, TILES, stride=2), :]
    own_ref[...] = jnp.where(core == 0, even, odd)
    for k in range(PLANES):
        at = pl.multiple_of(PLANE * lax.rem(x + k, PLANES), PLANE)
        out_refs[k][...] = own_ref[pl.ds(at, PLANE), :]


def solve(where, mine, other):
    return pl.pallas_call(
        solve_kernel,
        out_shape=[jax.ShapeDtypeStruct((PLANE, LANES), jnp.float32)] * PLANES,
        in_specs=[SMEM, VMEM, VMEM],
        out_specs=[VMEM] * PLANES,
        scratch_shapes=[pltpu.VMEM((NEURONS, LANES), jnp.float32), pltpu.VMEM((TILES, LANES), jnp.float32)],
        cost_estimate=pl.CostEstimate(flops=2_000_000_000, bytes_accessed=1_000_000, transcendentals=0),
        compiler_params=pltpu.CompilerParams(vmem_limit_bytes=8 << 20),
        name="solve",
    )(where, mine, other)


def merge_kernel(where_ref, *refs):
    group = lax.rem(iota((PLANE, LANES), 1) // FRAMES, PLANES)
    merged = refs[0][...]
    for k in range(1, PLANES):
        merged = jnp.where(group == lax.rem(where_ref[0] + PLANES - k, PLANES), refs[k][...], merged)
    refs[PLANES][...] = merged


def merge(where, pieces):
    return pl.pallas_call(
        merge_kernel,
        out_shape=jax.ShapeDtypeStruct((PLANE, LANES), jnp.float32),
        in_specs=[SMEM] + [VMEM] * PLANES,
        out_specs=VMEM,
        cost_estimate=pl.CostEstimate(flops=100_000_000, bytes_accessed=100_000, transcendentals=0),
        compiler_params=pltpu.CompilerParams(vmem_limit_bytes=2 << 20),
        name="merge",
    )(where, *pieces)


def join_kernel(pieces_ref, out_ref):
    near = LANES // FRAMES
    pieces = pieces_ref[...]
    rolled = [pieces] + [pltpu.roll(pieces, FRAMES * j, 1) for j in range(1, PLANES)]
    group = iota((near, LANES), 1) // FRAMES
    inside = group == iota((near, LANES), 0)
    for b in range(TILES // near):
        xs, first = b // 2, near * (b % 2)
        total = jnp.zeros((near, LANES), jnp.float32)
        for j in range(PLANES):
            hit = inside & (lax.rem(group + PLANES - j, PLANES) == xs)
            total = jnp.where(hit, rolled[j][first : first + near], total)
        out_ref[:, b * LANES : (b + 1) * LANES] = jnp.sum(total, axis=0, keepdims=True)


def join(pieces):
    return pl.pallas_call(
        join_kernel,
        out_shape=jax.ShapeDtypeStruct((1, TILES * FRAMES), jnp.float32),
        in_specs=[VMEM],
        out_specs=VMEM,
        compiler_params=pltpu.CompilerParams(vmem_limit_bytes=2 << 20),
        name="join",
    )(pieces)


def moved(array, axis, by):
    count = lax.axis_size(axis)
    return lax.ppermute(array, axis, [(i, (i + by) % count) for i in range(count)])


def local(movie, shifts, footprint, support, neuron_ids, owner_order, start_traces):
    where = jnp.stack([lax.axis_index(axis) for axis in ("ta_0", "ta_1", "row")]).astype(jnp.int32)
    packed = pack(neuron_ids[0], owner_order, footprint[0, 0], support[0, 0], start_traces.reshape(8, LANES))
    here = lax.all_to_all(packed, YZ, 0, 0, tiled=True)
    tiled = filter_tiles(movie[0], shifts[0])
    tile_movie = lax.all_to_all(tiled, TA, split_axis=0, concat_axis=0, tiled=True)
    left, far, right = [moved(here, "ta_0", by) for by in range(1, PLANES)]
    mine = project(where, tiled, here, left, far, right)
    other = moved(mine, "row", 1)
    pieces = solve(where, mine, other)
    pieces = [pieces[0]] + [moved(pieces[k], "ta_0", k) for k in range(1, PLANES)]
    pieces = merge(where, pieces)
    pieces = lax.all_to_all(pieces.reshape(PLANE, 1, LANES), YZ, 0, 0, tiled=True)
    traces = join(pieces.reshape(PLANE, LANES))
    return (tile_movie.reshape(1, 1, -1, PIXELS), traces)


def solution(mesh):
    finer = Mesh(mesh.devices.reshape(4, 4, 8, mesh.shape["row"]), TA_ROW)
    return jax.shard_map(
        local,
        mesh=finer,
        in_specs=(
            P("row", TA, None, None),
            P("row", TA, None, None),
            P("row", TA, None, None),
            P("row", TA, None, None),
            P("row", TA, None),
            P(),
            P(TA_ROW, None),
        ),
        out_specs=(P("row", TA, None, None), P(TA_ROW, None)),
        check_vma=False,
    )
```

```python
import jax
import jax.numpy as jnp
import numpy as np
from jax import lax
from jax.experimental import pallas as pl
from jax.experimental.pallas import tpu as pltpu
from jax.sharding import Mesh
from jax.sharding import PartitionSpec as P

TH = 16
TW = 32
MAXS = 8
ITERS = 2
TA = ("ta_0", "ta_1", "ta_2")
YZ = ("ta_1", "ta_2")
TA_ROW = ("ta_0", "ta_1", "ta_2", "row")

FRAMES = 8
H = 128
W = 512
LANES = 128
BLOCKS = W // LANES
SLOTS = 8
NEURONS = 256
TILES = 128
PIXELS = TH * TW
PLANE = 32
PLANES = 4
MESSAGE = PIXELS + LANES
ID_LANE = 64
HIGHEST = lax.Precision.HIGHEST
VMEM = pl.BlockSpec(memory_space=pltpu.VMEM)
SMEM = pl.BlockSpec(memory_space=pltpu.SMEM)


def smoothing_table(length):
    places = np.arange(length, dtype=np.float32)
    spread = places[:, None] - places[None, :]
    kernel = np.exp(-spread * spread / np.float32(32.0)).astype(np.float32)
    return (kernel / np.sum(kernel, axis=0, keepdims=True, dtype=np.float32)).astype(jnp.bfloat16)


def iota(shape, dim):
    return lax.broadcasted_iota(jnp.int32, shape, dim)


def split3(value):
    high = value.astype(jnp.bfloat16)
    rest = value - high.astype(jnp.float32)
    mid = rest.astype(jnp.bfloat16)
    low = (rest - mid.astype(jnp.float32)).astype(jnp.bfloat16)
    return high, mid, low


def dot32(left, right):
    return jnp.dot(left, right, preferred_element_type=jnp.float32)


def place(value, exact):
    high, mid, low = split3(value)
    return dot32(high, exact) + (dot32(mid, exact) + dot32(low, exact))


def register_kernel(shifts_ref, movie_ref, out_ref, padded_ref):
    lane = iota((H, LANES), 1)
    for s in range(2 * BLOCKS):
        padded_ref[s, pl.ds(0, MAXS), :] = jnp.zeros((MAXS, LANES), jnp.float32)
        padded_ref[s, pl.ds(MAXS + H, MAXS), :] = jnp.zeros((MAXS, LANES), jnp.float32)

    def block(f, p):
        if p < 0 or p >= BLOCKS:
            return None
        return movie_ref[f, :, p * LANES : (p + 1) * LANES].astype(jnp.float32)

    def shift(f, p, s):
        dy = shifts_ref[f, p, 0]
        dx = shifts_ref[f, p, 1]
        amount = jnp.where(dx > 0, LANES - dx, -dx)
        source = lane + dx

        def rolled(value):
            if value is None:
                return jnp.zeros((H, LANES), jnp.float32)
            return pltpu.roll(value, amount, 1)

        inner = jnp.where(source >= LANES, rolled(block(f, p + 1)), rolled(block(f, p)))
        padded_ref[s, pl.ds(MAXS, H), :] = jnp.where(source < 0, rolled(block(f, p - 1)), inner)
        out_ref[f, :, p * LANES : (p + 1) * LANES] = padded_ref[s, pl.ds(MAXS + dy, H), :].astype(jnp.bfloat16)

    def frames(g, carry):
        for h in range(2):
            for p in range(BLOCKS):
                shift(2 * g + h, p, h * BLOCKS + p)
        return carry

    lax.fori_loop(0, FRAMES // 2, frames, 0)


def register(movie, shifts):
    return pl.pallas_call(
        register_kernel,
        out_shape=jax.ShapeDtypeStruct((FRAMES, H, W), jnp.bfloat16),
        in_specs=[SMEM, VMEM],
        out_specs=VMEM,
        scratch_shapes=[pltpu.VMEM((2 * BLOCKS, H + 2 * MAXS, LANES), jnp.float32)],
        cost_estimate=pl.CostEstimate(flops=2_000_000_000, bytes_accessed=2_000_000, transcendentals=0),
        compiler_params=pltpu.CompilerParams(vmem_limit_bytes=8 << 20),
        name="register",
    )(shifts, movie)


def smooth_kernel(registered_ref, wide_ref, tall_ref, out_ref, filtered_ref, soft_ref):
    step = 2

    def chunk(c, carry):
        registered = registered_ref[pl.ds(c * step, step)].reshape(step * H, W)
        soft_ref[...] = dot32(registered, wide_ref[...]).astype(jnp.bfloat16)
        for k in range(step):
            low = dot32(tall_ref[...], soft_ref[k * H : (k + 1) * H, :])
            filtered = registered[k * H : (k + 1) * H].astype(jnp.float32) - low
            for p in range(BLOCKS):
                span = pl.ds(c * step + k, H, stride=FRAMES)
                filtered_ref[p, span, :] = filtered[:, p * LANES : (p + 1) * LANES]
        return carry

    lax.fori_loop(0, FRAMES // step, chunk, 0)
    lanes8 = iota((FRAMES, LANES), 1)
    near = lanes8 < 2 * TW
    even = lax.rem(lanes8 // TW, 2) == 0

    def tile_row(ty, carry):
        for q in range(4):
            for p in range(BLOCKS):
                v = []
                for r in range(4):
                    at = pl.multiple_of((ty * TH + 4 * q + r) * FRAMES, FRAMES)
                    v.append(filtered_ref[p, pl.ds(at, FRAMES), :])
                a0 = jnp.where(near, v[0], pltpu.roll(v[2], 64, 1))
                a2 = jnp.where(near, pltpu.roll(v[0], 64, 1), v[2])
                a1 = jnp.where(near, v[1], pltpu.roll(v[3], 64, 1))
                a3 = jnp.where(near, pltpu.roll(v[1], 64, 1), v[3])
                tiles = (
                    jnp.where(even, a0, pltpu.roll(a1, 32, 1)),
                    jnp.where(even, pltpu.roll(a0, 96, 1), a1),
                    jnp.where(even, a2, pltpu.roll(a3, 32, 1)),
                    jnp.where(even, pltpu.roll(a2, 96, 1), a3),
                )
                for m in range(4):
                    out_ref[ty * 16 + 4 * p + m, :, q * LANES : (q + 1) * LANES] = tiles[m].astype(jnp.bfloat16)
        return carry

    lax.fori_loop(0, H // TH, tile_row, 0)
    out_ref[:, :, PIXELS:] = jnp.zeros((TILES, FRAMES, LANES), jnp.bfloat16)


def smooth(registered):
    return pl.pallas_call(
        smooth_kernel,
        out_shape=jax.ShapeDtypeStruct((TILES, FRAMES, MESSAGE), jnp.bfloat16),
        in_specs=[VMEM] * 3,
        out_specs=VMEM,
        scratch_shapes=[
            pltpu.VMEM((BLOCKS, H * FRAMES, LANES), jnp.float32),
            pltpu.VMEM((2 * H, W), jnp.bfloat16),
        ],
        cost_estimate=pl.CostEstimate(flops=4_000_000_000, bytes_accessed=3_000_000, transcendentals=0),
        compiler_params=pltpu.CompilerParams(vmem_limit_bytes=16 << 20),
        name="smooth",
    )(registered, smoothing_table(W), smoothing_table(H).T)


def pack_kernel(ids_ref, order_ref, footprint_ref, support_ref, start_ref, out_ref):
    footprints = footprint_ref[...] * support_ref[...].astype(jnp.bfloat16)
    parts = [part.astype(jnp.float32) for part in split3(start_ref[...])]
    row = iota((SLOTS, LANES), 0)
    lane = iota((SLOTS, LANES), 1)
    owners = jnp.zeros((SLOTS, LANES), jnp.float32)
    for i in range(SLOTS):
        owner = order_ref[ids_ref[0, i]].astype(jnp.float32)
        owners = jnp.where((row == i) & (lane == ID_LANE), owner, owners)
    for w in range(PLANE // 2):
        extra = owners
        for k, part in enumerate(parts):
            extra = jnp.where(lane // FRAMES == k, pltpu.roll(part, (FRAMES * (k - w)) % LANES, 1), extra)
        for to in (w, w + PLANE // 2):
            out_ref[to, :, :PIXELS] = footprints
            out_ref[to, :, PIXELS:] = extra.astype(jnp.bfloat16)


def pack(ids, order, footprint, support, start):
    return pl.pallas_call(
        pack_kernel,
        out_shape=jax.ShapeDtypeStruct((PLANE, SLOTS, MESSAGE), jnp.bfloat16),
        in_specs=[SMEM, SMEM, VMEM, VMEM, VMEM],
        out_specs=VMEM,
        cost_estimate=pl.CostEstimate(flops=200_000_000, bytes_accessed=200_000, transcendentals=0),
        name="pack",
    )(ids, order, footprint, support, start)


def project_kernel(
    where_ref, tiled_ref, here_ref, left_ref, far_ref, right_ref, out_ref, select_ref, terms_ref
):
    x, y = where_ref[0], where_ref[1]
    many = PLANE // 2
    rows = many * SLOTS
    width = NEURONS + LANES
    same = iota((rows, 2 * rows), 0) // SLOTS == lax.rem(iota((rows, 2 * rows), 1), rows) // SLOTS
    own_row = iota((many, SLOTS, LANES), 1) == 2 * x + y // 2
    contract = (((1,), (1,)), ((), ()))
    neuron = iota((rows, NEURONS), 1)
    neuron_t = iota((NEURONS, rows), 0)
    diagonal = iota((rows, rows), 0) == iota((rows, rows), 1)
    out_ref[:, width:] = jnp.zeros((NEURONS, LANES), jnp.float32)
    for at in range(2 * PLANES):
        kx, first = at // 2, many * (at % 2)
        message = (here_ref, left_ref, far_ref, right_ref)[kx][first : first + many]
        tile = pl.multiple_of(PLANE * lax.rem(x + PLANES - kx, PLANES) + first, many)
        frames = tiled_ref[pl.ds(tile, many), :, :PIXELS].reshape(rows, PIXELS)
        prints = message[:, :, :PIXELS].reshape(rows, PIXELS)
        extra = message[:, :, PIXELS:].astype(jnp.float32).reshape(rows, LANES)
        found = lax.dot_general(
            prints, jnp.concatenate([frames, prints], axis=0), contract, preferred_element_type=jnp.float32
        )
        found = jnp.where(same, found, 0.0)
        ids = extra[:, ID_LANE : ID_LANE + 1]
        select = jnp.where(neuron == ids.astype(jnp.int32), 1.0, 0.0).astype(jnp.bfloat16)
        ids_row = jnp.sum(jnp.where(diagonal, ids, 0.0), axis=0, keepdims=True).astype(jnp.int32)
        span = slice(at * rows, (at + 1) * rows)
        select_ref[:, span] = jnp.where(neuron_t == ids_row, 1.0, 0.0).astype(jnp.bfloat16)
        spread = place(found[:, rows:], select)
        for k, (one, two) in enumerate(zip(split3(spread), split3(found[:, :rows]), strict=True)):
            terms_ref[span, k * width : k * width + NEURONS] = one
            terms_ref[span, k * width + NEURONS : (k + 1) * width] = two
        piece = jnp.sum(jnp.where(own_row, extra.reshape(many, SLOTS, LANES), 0.0), axis=1)
        piece = piece + (pltpu.roll(piece, LANES - FRAMES, 1) + pltpu.roll(piece, LANES - 2 * FRAMES, 1))
        out_ref[pl.ds(tile, many), width:] = piece
    sums = dot32(select_ref[...], terms_ref[...])
    out_ref[:, :width] = sums[:, :width] + (sums[:, width : 2 * width] + sums[:, 2 * width :])


def project(where, tiled, here, left, far, right):
    rows = TILES * SLOTS
    return pl.pallas_call(
        project_kernel,
        out_shape=jax.ShapeDtypeStruct((NEURONS, NEURONS + 2 * LANES), jnp.float32),
        in_specs=[SMEM] + [VMEM] * 5,
        out_specs=VMEM,
        scratch_shapes=[
            pltpu.VMEM((NEURONS, rows), jnp.bfloat16),
            pltpu.VMEM((rows, 3 * (NEURONS + LANES)), jnp.bfloat16),
        ],
        cost_estimate=pl.CostEstimate(flops=2_000_000_000, bytes_accessed=3_000_000, transcendentals=0),
        compiler_params=pltpu.CompilerParams(vmem_limit_bytes=16 << 20),
        name="project",
    )(where, tiled, here, left, far, right)


def solve_kernel(where_ref, mine_ref, other_ref, tiled_ref, out_ref, current_ref, parts_ref, sem):
    core = where_ref[2]
    sums = mine_ref[:, : NEURONS + LANES] + other_ref[:, : NEURONS + LANES]
    coupling = sums[:, :NEURONS]
    source = iota((LANES, LANES), 0)
    target = lax.rem(iota((LANES, LANES), 1), FRAMES)
    fold = jnp.where(lax.rem(source, FRAMES) == target, 1.0, 0.0)
    drive = place(sums[:, NEURONS:], fold.astype(jnp.bfloat16))
    copy = jnp.where(source == target, 1.0, 0.0).astype(jnp.bfloat16)
    here = mine_ref[:TILES, NEURONS + LANES :]
    there = other_ref[:TILES, NEURONS + LANES :]
    current_ref[pl.ds(0, TILES, stride=2), :] = place(jnp.where(core == 0, here, there), copy)
    current_ref[pl.ds(1, TILES, stride=2), :] = place(jnp.where(core == 0, there, here), copy)
    current = current_ref[...]
    bound = 1.0 + jnp.sum(coupling, axis=1, keepdims=True)
    for _ in range(ITERS):
        product = jnp.dot(coupling, current, preferred_element_type=jnp.float32, precision=HIGHEST)
        current = jnp.maximum(current - (product - drive) / bound, 0.0)
    current_ref[...] = current
    even = current_ref[pl.ds(0, TILES, stride=2), :]
    odd = current_ref[pl.ds(1, TILES, stride=2), :]
    high, mid, low = [part.astype(jnp.float32) for part in split3(jnp.where(core == 0, even, odd))]
    row = iota((SLOTS, LANES), 0)
    for t in range(TILES):
        lower = jnp.where(row == 1, mid[t : t + 1], jnp.where(row == 2, low[t : t + 1], 0.0))
        parts_ref[t] = jnp.where(row == 0, high[t : t + 1], lower).astype(jnp.bfloat16)
    store = pltpu.make_async_copy(parts_ref, out_ref.at[:, :, pl.ds(PIXELS, LANES)], sem)
    store.start()
    store.wait()


def solve(where, mine, other, tiled):
    return pl.pallas_call(
        solve_kernel,
        out_shape=jax.ShapeDtypeStruct(tiled.shape, tiled.dtype),
        in_specs=[SMEM, VMEM, VMEM, pl.BlockSpec(memory_space=pl.ANY)],
        out_specs=pl.BlockSpec(memory_space=pl.ANY),
        scratch_shapes=[
            pltpu.VMEM((NEURONS, LANES), jnp.float32),
            pltpu.VMEM((TILES, SLOTS, LANES), jnp.bfloat16),
            pltpu.SemaphoreType.DMA,
        ],
        input_output_aliases={3: 0},
        cost_estimate=pl.CostEstimate(flops=2_000_000_000, bytes_accessed=1_000_000, transcendentals=0),
        compiler_params=pltpu.CompilerParams(vmem_limit_bytes=8 << 20),
        name="solve",
    )(where, mine, other, tiled)


def unpack_kernel(arrived_ref, movie_ref, traces_ref):
    movie_ref[...] = arrived_ref[:, :, :PIXELS].reshape(TILES * FRAMES, PIXELS)
    near = LANES // FRAMES
    group = iota((SLOTS, LANES), 1) // FRAMES
    for b in range(TILES // near):
        total = jnp.zeros((SLOTS, LANES), jnp.float32)
        for t in range(near):
            total = jnp.where(group == t, arrived_ref[b * near + t, :, PIXELS:].astype(jnp.float32), total)
        traces_ref[:, b * LANES : (b + 1) * LANES] = jnp.sum(total, axis=0, keepdims=True)


def unpack(arrived):
    return pl.pallas_call(
        unpack_kernel,
        out_shape=(
            jax.ShapeDtypeStruct((TILES * FRAMES, PIXELS), jnp.bfloat16),
            jax.ShapeDtypeStruct((1, TILES * FRAMES), jnp.float32),
        ),
        in_specs=[VMEM],
        out_specs=(VMEM, VMEM),
        compiler_params=pltpu.CompilerParams(vmem_limit_bytes=8 << 20),
        name="unpack",
    )(arrived)


def moved(array, axis, by):
    count = lax.axis_size(axis)
    return lax.ppermute(array, axis, [(i, (i + by) % count) for i in range(count)])


def local(movie, shifts, footprint, support, neuron_ids, owner_order, start_traces):
    where = jnp.stack([lax.axis_index(axis) for axis in ("ta_0", "ta_1", "row")]).astype(jnp.int32)
    packed = pack(neuron_ids[0], owner_order, footprint[0, 0], support[0, 0], start_traces.reshape(8, LANES))
    here = lax.all_to_all(packed, YZ, 0, 0, tiled=True)
    registered = register(movie[0], shifts[0])
    left, far, right = [moved(here, "ta_0", by) for by in range(1, PLANES)]
    tiled = smooth(registered)
    mine = project(where, tiled, here, left, far, right)
    other = moved(mine, "row", 1)
    tiled = solve(where, mine, other, tiled)
    arrived = lax.all_to_all(tiled, TA, split_axis=0, concat_axis=0, tiled=True)
    tile_movie, traces = unpack(arrived)
    return (tile_movie.reshape(1, 1, -1, PIXELS), traces)


def solution(mesh):
    finer = Mesh(mesh.devices.reshape(4, 4, 8, mesh.shape["row"]), TA_ROW)
    return jax.shard_map(
        local,
        mesh=finer,
        in_specs=(
            P("row", TA, None, None),
            P("row", TA, None, None),
            P("row", TA, None, None),
            P("row", TA, None, None),
            P("row", TA, None),
            P(),
            P(TA_ROW, None),
        ),
        out_specs=(P("row", TA, None, None), P(TA_ROW, None)),
        check_vma=False,
    )
```

```python
import jax
import jax.numpy as jnp
import numpy as np
from jax import lax
from jax.experimental import pallas as pl
from jax.experimental.pallas import tpu as pltpu
from jax.sharding import Mesh
from jax.sharding import PartitionSpec as P

TH = 16
TW = 32
MAXS = 8
ITERS = 2
TA = ("ta_0", "ta_1", "ta_2")
YZ = ("ta_1", "ta_2")
ZYX = ("ta_2", "ta_1", "ta_0")
TA_ROW = ("ta_0", "ta_1", "ta_2", "row")

FRAMES = 8
H = 128
W = 512
LANES = 128
BLOCKS = W // LANES
SLOTS = 8
NEURONS = 256
TILES = 128
PIXELS = TH * TW
PLANE = 32
PLANES = 4
MESSAGE = PIXELS + LANES
ID_LANE = 64
HIGHEST = lax.Precision.HIGHEST
VMEM = pl.BlockSpec(memory_space=pltpu.VMEM)
SMEM = pl.BlockSpec(memory_space=pltpu.SMEM)


def smoothing_table(length):
    places = np.arange(length, dtype=np.float32)
    spread = places[:, None] - places[None, :]
    kernel = np.exp(-spread * spread / np.float32(32.0)).astype(np.float32)
    return (kernel / np.sum(kernel, axis=0, keepdims=True, dtype=np.float32)).astype(jnp.bfloat16)


def iota(shape, dim):
    return lax.broadcasted_iota(jnp.int32, shape, dim)


def split3(value):
    high = value.astype(jnp.bfloat16)
    rest = value - high.astype(jnp.float32)
    mid = rest.astype(jnp.bfloat16)
    low = (rest - mid.astype(jnp.float32)).astype(jnp.bfloat16)
    return high, mid, low


def dot32(left, right):
    return jnp.dot(left, right, preferred_element_type=jnp.float32)


def place(value, exact):
    high, mid, low = split3(value)
    return dot32(high, exact) + (dot32(mid, exact) + dot32(low, exact))


def register_kernel(shifts_ref, movie_ref, out_ref, padded_ref):
    lane = iota((H, LANES), 1)
    for s in range(2 * BLOCKS):
        padded_ref[s, pl.ds(0, MAXS), :] = jnp.zeros((MAXS, LANES), jnp.float32)
        padded_ref[s, pl.ds(MAXS + H, MAXS), :] = jnp.zeros((MAXS, LANES), jnp.float32)

    def block(f, p):
        if p < 0 or p >= BLOCKS:
            return None
        return movie_ref[f, :, p * LANES : (p + 1) * LANES].astype(jnp.float32)

    def shift(f, p, s):
        dy = shifts_ref[f, p, 0]
        dx = shifts_ref[f, p, 1]
        amount = jnp.where(dx > 0, LANES - dx, -dx)
        source = lane + dx

        def rolled(value):
            if value is None:
                return jnp.zeros((H, LANES), jnp.float32)
            return pltpu.roll(value, amount, 1)

        inner = jnp.where(source >= LANES, rolled(block(f, p + 1)), rolled(block(f, p)))
        padded_ref[s, pl.ds(MAXS, H), :] = jnp.where(source < 0, rolled(block(f, p - 1)), inner)
        out_ref[f, :, p * LANES : (p + 1) * LANES] = padded_ref[s, pl.ds(MAXS + dy, H), :].astype(jnp.bfloat16)

    def frames(g, carry):
        for h in range(2):
            for p in range(BLOCKS):
                shift(2 * g + h, p, h * BLOCKS + p)
        return carry

    lax.fori_loop(0, FRAMES // 2, frames, 0)


def register(movie, shifts):
    return pl.pallas_call(
        register_kernel,
        out_shape=jax.ShapeDtypeStruct((FRAMES, H, W), jnp.bfloat16),
        in_specs=[SMEM, VMEM],
        out_specs=VMEM,
        scratch_shapes=[pltpu.VMEM((2 * BLOCKS, H + 2 * MAXS, LANES), jnp.float32)],
        cost_estimate=pl.CostEstimate(flops=2_000_000_000, bytes_accessed=2_000_000, transcendentals=0),
        compiler_params=pltpu.CompilerParams(vmem_limit_bytes=8 << 20),
        name="register",
    )(shifts, movie)


def smooth_kernel(registered_ref, wide_ref, tall_ref, out_ref, filtered_ref, soft_ref):
    step = 2

    def chunk(c, carry):
        registered = registered_ref[pl.ds(c * step, step)].reshape(step * H, W)
        soft_ref[...] = dot32(registered, wide_ref[...]).astype(jnp.bfloat16)
        for k in range(step):
            low = dot32(tall_ref[...], soft_ref[k * H : (k + 1) * H, :])
            filtered = registered[k * H : (k + 1) * H].astype(jnp.float32) - low
            for p in range(BLOCKS):
                span = pl.ds(c * step + k, H, stride=FRAMES)
                filtered_ref[p, span, :] = filtered[:, p * LANES : (p + 1) * LANES]
        return carry

    lax.fori_loop(0, FRAMES // step, chunk, 0)
    lanes8 = iota((FRAMES, LANES), 1)
    near = lanes8 < 2 * TW
    even = lax.rem(lanes8 // TW, 2) == 0

    def tile_row(ty, carry):
        for q in range(4):
            for p in range(BLOCKS):
                v = []
                for r in range(4):
                    at = pl.multiple_of((ty * TH + 4 * q + r) * FRAMES, FRAMES)
                    v.append(filtered_ref[p, pl.ds(at, FRAMES), :])
                a0 = jnp.where(near, v[0], pltpu.roll(v[2], 64, 1))
                a2 = jnp.where(near, pltpu.roll(v[0], 64, 1), v[2])
                a1 = jnp.where(near, v[1], pltpu.roll(v[3], 64, 1))
                a3 = jnp.where(near, pltpu.roll(v[1], 64, 1), v[3])
                tiles = (
                    jnp.where(even, a0, pltpu.roll(a1, 32, 1)),
                    jnp.where(even, pltpu.roll(a0, 96, 1), a1),
                    jnp.where(even, a2, pltpu.roll(a3, 32, 1)),
                    jnp.where(even, pltpu.roll(a2, 96, 1), a3),
                )
                for m in range(4):
                    column = 4 * p + m
                    at = (column % 8) * 16 + (2 * lax.rem(ty, 2) + column // 8) * 4 + ty // 2
                    out_ref[at, :, q * LANES : (q + 1) * LANES] = tiles[m].astype(jnp.bfloat16)
        return carry

    lax.fori_loop(0, H // TH, tile_row, 0)


def smooth(registered):
    return pl.pallas_call(
        smooth_kernel,
        out_shape=jax.ShapeDtypeStruct((TILES, FRAMES, PIXELS), jnp.bfloat16),
        in_specs=[VMEM] * 3,
        out_specs=VMEM,
        scratch_shapes=[
            pltpu.VMEM((BLOCKS, H * FRAMES, LANES), jnp.float32),
            pltpu.VMEM((2 * H, W), jnp.bfloat16),
        ],
        cost_estimate=pl.CostEstimate(flops=4_000_000_000, bytes_accessed=3_000_000, transcendentals=0),
        compiler_params=pltpu.CompilerParams(vmem_limit_bytes=16 << 20),
        name="smooth",
    )(registered, smoothing_table(W), smoothing_table(H).T)


def pack_kernel(ids_ref, order_ref, footprint_ref, support_ref, start_ref, out_ref):
    footprints = footprint_ref[...] * support_ref[...].astype(jnp.bfloat16)
    parts = [part.astype(jnp.float32) for part in split3(start_ref[...])]
    row = iota((SLOTS, LANES), 0)
    lane = iota((SLOTS, LANES), 1)
    owners = jnp.zeros((SLOTS, LANES), jnp.float32)
    for i in range(SLOTS):
        owner = order_ref[ids_ref[0, i]].astype(jnp.float32)
        owners = jnp.where((row == i) & (lane == ID_LANE), owner, owners)
    for w in range(PLANE // 2):
        extra = owners
        for k, part in enumerate(parts):
            extra = jnp.where(lane // FRAMES == k, pltpu.roll(part, (FRAMES * (k - w)) % LANES, 1), extra)
        for to in (w, w + PLANE // 2):
            out_ref[to, :, :PIXELS] = footprints
            out_ref[to, :, PIXELS:] = extra.astype(jnp.bfloat16)


def pack(ids, order, footprint, support, start):
    return pl.pallas_call(
        pack_kernel,
        out_shape=jax.ShapeDtypeStruct((PLANE, SLOTS, MESSAGE), jnp.bfloat16),
        in_specs=[SMEM, SMEM, VMEM, VMEM, VMEM],
        out_specs=VMEM,
        cost_estimate=pl.CostEstimate(flops=200_000_000, bytes_accessed=200_000, transcendentals=0),
        name="pack",
    )(ids, order, footprint, support, start)


def project_kernel(
    where_ref, tiled_ref, here_ref, left_ref, far_ref, right_ref, out_ref, select_ref, terms_ref
):
    x, y = where_ref[0], where_ref[1]
    many = PLANE // 2
    rows = many * SLOTS
    width = NEURONS + LANES
    same = iota((rows, 2 * rows), 0) // SLOTS == lax.rem(iota((rows, 2 * rows), 1), rows) // SLOTS
    own_row = iota((many, SLOTS, LANES), 1) == 2 * x + y // 2
    contract = (((1,), (1,)), ((), ()))
    neuron = iota((rows, NEURONS), 1)
    neuron_t = iota((NEURONS, rows), 0)
    diagonal = iota((rows, rows), 0) == iota((rows, rows), 1)
    out_ref[:, width:] = jnp.zeros((NEURONS, LANES), jnp.float32)
    for at in range(2 * PLANES):
        kx, first = at // 2, many * (at % 2)
        message = (here_ref, left_ref, far_ref, right_ref)[kx][first : first + many]
        source = lax.rem(x + PLANES - kx, PLANES)
        tile = pl.multiple_of(PLANE * source + first, many)
        frames = [tiled_ref[(k % 8) * 16 + (first // 8 + k // 8) * 4 + source] for k in range(many)]
        prints = message[:, :, :PIXELS].reshape(rows, PIXELS)
        extra = message[:, :, PIXELS:].astype(jnp.float32).reshape(rows, LANES)
        found = lax.dot_general(
            prints, jnp.concatenate(frames + [prints], axis=0), contract, preferred_element_type=jnp.float32
        )
        found = jnp.where(same, found, 0.0)
        ids = extra[:, ID_LANE : ID_LANE + 1]
        select = jnp.where(neuron == ids.astype(jnp.int32), 1.0, 0.0).astype(jnp.bfloat16)
        ids_row = jnp.sum(jnp.where(diagonal, ids, 0.0), axis=0, keepdims=True).astype(jnp.int32)
        span = slice(at * rows, (at + 1) * rows)
        select_ref[:, span] = jnp.where(neuron_t == ids_row, 1.0, 0.0).astype(jnp.bfloat16)
        spread = place(found[:, rows:], select)
        for k, (one, two) in enumerate(zip(split3(spread), split3(found[:, :rows]), strict=True)):
            terms_ref[span, k * width : k * width + NEURONS] = one
            terms_ref[span, k * width + NEURONS : (k + 1) * width] = two
        piece = jnp.sum(jnp.where(own_row, extra.reshape(many, SLOTS, LANES), 0.0), axis=1)
        piece = piece + (pltpu.roll(piece, LANES - FRAMES, 1) + pltpu.roll(piece, LANES - 2 * FRAMES, 1))
        out_ref[pl.ds(tile, many), width:] = piece
    sums = dot32(select_ref[...], terms_ref[...])
    out_ref[:, :width] = sums[:, :width] + (sums[:, width : 2 * width] + sums[:, 2 * width :])


def project(where, tiled, here, left, far, right):
    rows = TILES * SLOTS
    return pl.pallas_call(
        project_kernel,
        out_shape=jax.ShapeDtypeStruct((NEURONS, NEURONS + 2 * LANES), jnp.float32),
        in_specs=[SMEM] + [VMEM] * 5,
        out_specs=VMEM,
        scratch_shapes=[
            pltpu.VMEM((NEURONS, rows), jnp.bfloat16),
            pltpu.VMEM((rows, 3 * (NEURONS + LANES)), jnp.bfloat16),
        ],
        cost_estimate=pl.CostEstimate(flops=2_000_000_000, bytes_accessed=3_000_000, transcendentals=0),
        compiler_params=pltpu.CompilerParams(vmem_limit_bytes=16 << 20),
        name="project",
    )(where, tiled, here, left, far, right)


def solve_kernel(where_ref, mine_ref, other_ref, *refs):
    out_refs, current_ref, own_ref = refs[:PLANES], refs[PLANES], refs[PLANES + 1]
    x, core = where_ref[0], where_ref[2]
    sums = mine_ref[:, : NEURONS + LANES] + other_ref[:, : NEURONS + LANES]
    coupling = sums[:, :NEURONS]
    source = iota((LANES, LANES), 0)
    target = lax.rem(iota((LANES, LANES), 1), FRAMES)
    fold = jnp.where(lax.rem(source, FRAMES) == target, 1.0, 0.0)
    drive = place(sums[:, NEURONS:], fold.astype(jnp.bfloat16))
    copy = jnp.where(source == target, 1.0, 0.0).astype(jnp.bfloat16)
    here = mine_ref[:TILES, NEURONS + LANES :]
    there = other_ref[:TILES, NEURONS + LANES :]
    current_ref[pl.ds(0, TILES, stride=2), :] = place(jnp.where(core == 0, here, there), copy)
    current_ref[pl.ds(1, TILES, stride=2), :] = place(jnp.where(core == 0, there, here), copy)
    current = current_ref[...]
    bound = 1.0 + jnp.sum(coupling, axis=1, keepdims=True)
    for _ in range(ITERS):
        product = jnp.dot(coupling, current, preferred_element_type=jnp.float32, precision=HIGHEST)
        current = jnp.maximum(current - (product - drive) / bound, 0.0)
    current_ref[...] = current
    even = current_ref[pl.ds(0, TILES, stride=2), :]
    odd = current_ref[pl.ds(1, TILES, stride=2), :]
    own_ref[...] = jnp.where(core == 0, even, odd)
    for k in range(PLANES):
        at = pl.multiple_of(PLANE * lax.rem(x + k, PLANES), PLANE)
        out_refs[k][...] = own_ref[pl.ds(at, PLANE), :]


def solve(where, mine, other):
    return pl.pallas_call(
        solve_kernel,
        out_shape=[jax.ShapeDtypeStruct((PLANE, LANES), jnp.float32)] * PLANES,
        in_specs=[SMEM, VMEM, VMEM],
        out_specs=[VMEM] * PLANES,
        scratch_shapes=[pltpu.VMEM((NEURONS, LANES), jnp.float32), pltpu.VMEM((TILES, LANES), jnp.float32)],
        cost_estimate=pl.CostEstimate(flops=2_000_000_000, bytes_accessed=1_000_000, transcendentals=0),
        compiler_params=pltpu.CompilerParams(vmem_limit_bytes=8 << 20),
        name="solve",
    )(where, mine, other)


def merge_kernel(where_ref, *refs):
    group = lax.rem(iota((PLANE, LANES), 1) // FRAMES, PLANES)
    merged = refs[0][...]
    for k in range(1, PLANES):
        merged = jnp.where(group == lax.rem(where_ref[0] + PLANES - k, PLANES), refs[k][...], merged)
    refs[PLANES][...] = merged


def merge(where, pieces):
    return pl.pallas_call(
        merge_kernel,
        out_shape=jax.ShapeDtypeStruct((PLANE, LANES), jnp.float32),
        in_specs=[SMEM] + [VMEM] * PLANES,
        out_specs=VMEM,
        cost_estimate=pl.CostEstimate(flops=100_000_000, bytes_accessed=100_000, transcendentals=0),
        compiler_params=pltpu.CompilerParams(vmem_limit_bytes=2 << 20),
        name="merge",
    )(where, *pieces)


def join_kernel(pieces_ref, out_ref):
    near = LANES // FRAMES
    pieces = pieces_ref[...]
    rolled = [pieces] + [pltpu.roll(pieces, FRAMES * j, 1) for j in range(1, PLANES)]
    group = iota((near, LANES), 1) // FRAMES
    inside = group == iota((near, LANES), 0)
    for b in range(TILES // near):
        xs, first = b // 2, near * (b % 2)
        total = jnp.zeros((near, LANES), jnp.float32)
        for j in range(PLANES):
            hit = inside & (lax.rem(group + PLANES - j, PLANES) == xs)
            total = jnp.where(hit, rolled[j][first : first + near], total)
        out_ref[:, b * LANES : (b + 1) * LANES] = jnp.sum(total, axis=0, keepdims=True)


def join(pieces):
    return pl.pallas_call(
        join_kernel,
        out_shape=jax.ShapeDtypeStruct((1, TILES * FRAMES), jnp.float32),
        in_specs=[VMEM],
        out_specs=VMEM,
        compiler_params=pltpu.CompilerParams(vmem_limit_bytes=2 << 20),
        name="join",
    )(pieces)


def store_kernel(arrived_ref, out_ref, sems):
    copies = []
    for x in range(4):
        for y in range(4):
            copies.append(pltpu.make_async_copy(arrived_ref.at[:, y, x], out_ref.at[x, y], sems.at[4 * x + y]))
    for copy in copies:
        copy.start()
    for copy in copies:
        copy.wait()


def store(arrived):
    return pl.pallas_call(
        store_kernel,
        out_shape=jax.ShapeDtypeStruct((4, 4, 8, FRAMES, PIXELS), jnp.bfloat16),
        in_specs=[VMEM],
        out_specs=pl.BlockSpec(memory_space=pl.ANY),
        scratch_shapes=[pltpu.SemaphoreType.DMA((16,))],
        cost_estimate=pl.CostEstimate(flops=500_000_000, bytes_accessed=2_000_000, transcendentals=0),
        compiler_params=pltpu.CompilerParams(vmem_limit_bytes=4 << 20),
        name="store",
    )(arrived.reshape(8, 4, 4, FRAMES, PIXELS))


def moved(array, axis, by):
    count = lax.axis_size(axis)
    return lax.ppermute(array, axis, [(i, (i + by) % count) for i in range(count)])


def local(movie, shifts, footprint, support, neuron_ids, owner_order, start_traces):
    where = jnp.stack([lax.axis_index(axis) for axis in ("ta_0", "ta_1", "row")]).astype(jnp.int32)
    packed = pack(neuron_ids[0], owner_order, footprint[0, 0], support[0, 0], start_traces.reshape(8, LANES))
    here = lax.all_to_all(packed, YZ, 0, 0, tiled=True)
    registered = register(movie[0], shifts[0])
    tiled = smooth(registered)
    arrived = lax.all_to_all(tiled, ZYX, split_axis=0, concat_axis=0, tiled=True)
    left, far, right = [moved(here, "ta_0", by) for by in range(1, PLANES)]
    mine = project(where, tiled, here, left, far, right)
    other = moved(mine, "row", 1)
    pieces = solve(where, mine, other)
    pieces = [pieces[0]] + [moved(pieces[k], "ta_0", k) for k in range(1, PLANES)]
    pieces = merge(where, pieces)
    pieces = lax.all_to_all(pieces.reshape(PLANE, 1, LANES), YZ, 0, 0, tiled=True)
    tile_movie = store(arrived)
    traces = join(pieces.reshape(PLANE, LANES))
    return (tile_movie.reshape(1, 1, -1, PIXELS), traces)


def solution(mesh):
    finer = Mesh(mesh.devices.reshape(4, 4, 8, mesh.shape["row"]), TA_ROW)
    return jax.shard_map(
        local,
        mesh=finer,
        in_specs=(
            P("row", TA, None, None),
            P("row", TA, None, None),
            P("row", TA, None, None),
            P("row", TA, None, None),
            P("row", TA, None),
            P(),
            P(TA_ROW, None),
        ),
        out_specs=(P("row", TA, None, None), P(TA_ROW, None)),
        check_vma=False,
    )
```

```python
import jax
import jax.numpy as jnp
import numpy as np
from jax import lax
from jax.experimental import pallas as pl
from jax.experimental.pallas import tpu as pltpu
from jax.sharding import Mesh
from jax.sharding import PartitionSpec as P

TH = 16
TW = 32
MAXS = 8
ITERS = 2
TA = ("ta_0", "ta_1", "ta_2")
YZ = ("ta_1", "ta_2")
YZX = ("ta_1", "ta_2", "ta_0")
TA_ROW = ("ta_0", "ta_1", "ta_2", "row")

FRAMES = 8
H = 128
W = 512
LANES = 128
BLOCKS = W // LANES
SLOTS = 8
NEURONS = 256
TILES = 128
PIXELS = TH * TW
PLANE = 32
PLANES = 4
MESSAGE = PIXELS + LANES
ID_LANE = 64
HIGHEST = lax.Precision.HIGHEST
VMEM = pl.BlockSpec(memory_space=pltpu.VMEM)
SMEM = pl.BlockSpec(memory_space=pltpu.SMEM)


def smoothing_table(length):
    places = np.arange(length, dtype=np.float32)
    spread = places[:, None] - places[None, :]
    kernel = np.exp(-spread * spread / np.float32(32.0)).astype(np.float32)
    return (kernel / np.sum(kernel, axis=0, keepdims=True, dtype=np.float32)).astype(jnp.bfloat16)


def iota(shape, dim):
    return lax.broadcasted_iota(jnp.int32, shape, dim)


def split3(value):
    high = value.astype(jnp.bfloat16)
    rest = value - high.astype(jnp.float32)
    mid = rest.astype(jnp.bfloat16)
    low = (rest - mid.astype(jnp.float32)).astype(jnp.bfloat16)
    return high, mid, low


def dot32(left, right):
    return jnp.dot(left, right, preferred_element_type=jnp.float32)


def place(value, exact):
    high, mid, low = split3(value)
    return dot32(high, exact) + (dot32(mid, exact) + dot32(low, exact))


def register_kernel(shifts_ref, movie_ref, out_ref, padded_ref):
    lane = iota((H, LANES), 1)
    for s in range(2 * BLOCKS):
        padded_ref[s, pl.ds(0, MAXS), :] = jnp.zeros((MAXS, LANES), jnp.float32)
        padded_ref[s, pl.ds(MAXS + H, MAXS), :] = jnp.zeros((MAXS, LANES), jnp.float32)

    def block(f, p):
        if p < 0 or p >= BLOCKS:
            return None
        return movie_ref[f, :, p * LANES : (p + 1) * LANES].astype(jnp.float32)

    def shift(f, p, s):
        dy = shifts_ref[f, p, 0]
        dx = shifts_ref[f, p, 1]
        amount = jnp.where(dx > 0, LANES - dx, -dx)
        source = lane + dx

        def rolled(value):
            if value is None:
                return jnp.zeros((H, LANES), jnp.float32)
            return pltpu.roll(value, amount, 1)

        inner = jnp.where(source >= LANES, rolled(block(f, p + 1)), rolled(block(f, p)))
        padded_ref[s, pl.ds(MAXS, H), :] = jnp.where(source < 0, rolled(block(f, p - 1)), inner)
        out_ref[f, :, p * LANES : (p + 1) * LANES] = padded_ref[s, pl.ds(MAXS + dy, H), :].astype(jnp.bfloat16)

    def frames(g, carry):
        for h in range(2):
            for p in range(BLOCKS):
                shift(2 * g + h, p, h * BLOCKS + p)
        return carry

    lax.fori_loop(0, FRAMES // 2, frames, 0)


def register(movie, shifts):
    return pl.pallas_call(
        register_kernel,
        out_shape=jax.ShapeDtypeStruct((FRAMES, H, W), jnp.bfloat16),
        in_specs=[SMEM, VMEM],
        out_specs=VMEM,
        scratch_shapes=[pltpu.VMEM((2 * BLOCKS, H + 2 * MAXS, LANES), jnp.float32)],
        cost_estimate=pl.CostEstimate(flops=2_000_000_000, bytes_accessed=2_000_000, transcendentals=0),
        compiler_params=pltpu.CompilerParams(vmem_limit_bytes=8 << 20),
        name="register",
    )(shifts, movie)


def smooth_kernel(registered_ref, wide_ref, tall_ref, out_ref, filtered_ref, soft_ref):
    step = 2

    def chunk(c, carry):
        registered = registered_ref[pl.ds(c * step, step)].reshape(step * H, W)
        soft_ref[...] = dot32(registered, wide_ref[...]).astype(jnp.bfloat16)
        for k in range(step):
            low = dot32(tall_ref[...], soft_ref[k * H : (k + 1) * H, :])
            filtered = registered[k * H : (k + 1) * H].astype(jnp.float32) - low
            for p in range(BLOCKS):
                span = pl.ds(c * step + k, H, stride=FRAMES)
                filtered_ref[p, span, :] = filtered[:, p * LANES : (p + 1) * LANES]
        return carry

    lax.fori_loop(0, FRAMES // step, chunk, 0)
    lanes8 = iota((FRAMES, LANES), 1)
    near = lanes8 < 2 * TW
    even = lax.rem(lanes8 // TW, 2) == 0

    def tile_row(ty, carry):
        for q in range(4):
            for p in range(BLOCKS):
                v = []
                for r in range(4):
                    at = pl.multiple_of((ty * TH + 4 * q + r) * FRAMES, FRAMES)
                    v.append(filtered_ref[p, pl.ds(at, FRAMES), :])
                a0 = jnp.where(near, v[0], pltpu.roll(v[2], 64, 1))
                a2 = jnp.where(near, pltpu.roll(v[0], 64, 1), v[2])
                a1 = jnp.where(near, v[1], pltpu.roll(v[3], 64, 1))
                a3 = jnp.where(near, pltpu.roll(v[1], 64, 1), v[3])
                tiles = (
                    jnp.where(even, a0, pltpu.roll(a1, 32, 1)),
                    jnp.where(even, pltpu.roll(a0, 96, 1), a1),
                    jnp.where(even, a2, pltpu.roll(a3, 32, 1)),
                    jnp.where(even, pltpu.roll(a2, 96, 1), a3),
                )
                for m in range(4):
                    column = 4 * p + m
                    at = (16 * lax.rem(ty, 2) + column) * 4 + ty // 2
                    out_ref[at, :, q * LANES : (q + 1) * LANES] = tiles[m].astype(jnp.bfloat16)
        return carry

    lax.fori_loop(0, H // TH, tile_row, 0)


def smooth(registered):
    return pl.pallas_call(
        smooth_kernel,
        out_shape=jax.ShapeDtypeStruct((TILES, FRAMES, PIXELS), jnp.bfloat16),
        in_specs=[VMEM] * 3,
        out_specs=VMEM,
        scratch_shapes=[
            pltpu.VMEM((BLOCKS, H * FRAMES, LANES), jnp.float32),
            pltpu.VMEM((2 * H, W), jnp.bfloat16),
        ],
        cost_estimate=pl.CostEstimate(flops=4_000_000_000, bytes_accessed=3_000_000, transcendentals=0),
        compiler_params=pltpu.CompilerParams(vmem_limit_bytes=16 << 20),
        name="smooth",
    )(registered, smoothing_table(W), smoothing_table(H).T)


def pack_kernel(ids_ref, order_ref, footprint_ref, support_ref, start_ref, out_ref):
    footprints = footprint_ref[...] * support_ref[...].astype(jnp.bfloat16)
    parts = [part.astype(jnp.float32) for part in split3(start_ref[...])]
    row = iota((SLOTS, LANES), 0)
    lane = iota((SLOTS, LANES), 1)
    owners = jnp.zeros((SLOTS, LANES), jnp.float32)
    for i in range(SLOTS):
        owner = order_ref[ids_ref[0, i]].astype(jnp.float32)
        owners = jnp.where((row == i) & (lane == ID_LANE), owner, owners)
    for w in range(PLANE // 2):
        extra = owners
        for k, part in enumerate(parts):
            extra = jnp.where(lane // FRAMES == k, pltpu.roll(part, (FRAMES * (k - w)) % LANES, 1), extra)
        for to in (w, w + PLANE // 2):
            out_ref[to, :, :PIXELS] = footprints
            out_ref[to, :, PIXELS:] = extra.astype(jnp.bfloat16)


def pack(ids, order, footprint, support, start):
    return pl.pallas_call(
        pack_kernel,
        out_shape=jax.ShapeDtypeStruct((PLANE, SLOTS, MESSAGE), jnp.bfloat16),
        in_specs=[SMEM, SMEM, VMEM, VMEM, VMEM],
        out_specs=VMEM,
        cost_estimate=pl.CostEstimate(flops=200_000_000, bytes_accessed=200_000, transcendentals=0),
        name="pack",
    )(ids, order, footprint, support, start)


def project_kernel(
    where_ref, tiled_ref, here_ref, left_ref, far_ref, right_ref, out_ref, select_ref, terms_ref
):
    x, y = where_ref[0], where_ref[1]
    many = PLANE // 2
    rows = many * SLOTS
    width = NEURONS + LANES
    same = iota((rows, 2 * rows), 0) // SLOTS == lax.rem(iota((rows, 2 * rows), 1), rows) // SLOTS
    own_row = iota((many, SLOTS, LANES), 1) == 2 * x + y // 2
    contract = (((1,), (1,)), ((), ()))
    neuron = iota((rows, NEURONS), 1)
    neuron_t = iota((NEURONS, rows), 0)
    diagonal = iota((rows, rows), 0) == iota((rows, rows), 1)
    out_ref[:, width:] = jnp.zeros((NEURONS, LANES), jnp.float32)
    for at in range(2 * PLANES):
        kx, first = at // 2, many * (at % 2)
        message = (here_ref, left_ref, far_ref, right_ref)[kx][first : first + many]
        source = lax.rem(x + PLANES - kx, PLANES)
        tile = pl.multiple_of(PLANE * source + first, many)
        frames = [tiled_ref[PLANES * (first + k) + source] for k in range(many)]
        prints = message[:, :, :PIXELS].reshape(rows, PIXELS)
        extra = message[:, :, PIXELS:].astype(jnp.float32).reshape(rows, LANES)
        found = lax.dot_general(
            prints, jnp.concatenate(frames + [prints], axis=0), contract, preferred_element_type=jnp.float32
        )
        found = jnp.where(same, found, 0.0)
        ids = extra[:, ID_LANE : ID_LANE + 1]
        select = jnp.where(neuron == ids.astype(jnp.int32), 1.0, 0.0).astype(jnp.bfloat16)
        ids_row = jnp.sum(jnp.where(diagonal, ids, 0.0), axis=0, keepdims=True).astype(jnp.int32)
        span = slice(at * rows, (at + 1) * rows)
        select_ref[:, span] = jnp.where(neuron_t == ids_row, 1.0, 0.0).astype(jnp.bfloat16)
        spread = place(found[:, rows:], select)
        for k, (one, two) in enumerate(zip(split3(spread), split3(found[:, :rows]), strict=True)):
            terms_ref[span, k * width : k * width + NEURONS] = one
            terms_ref[span, k * width + NEURONS : (k + 1) * width] = two
        piece = jnp.sum(jnp.where(own_row, extra.reshape(many, SLOTS, LANES), 0.0), axis=1)
        piece = piece + (pltpu.roll(piece, LANES - FRAMES, 1) + pltpu.roll(piece, LANES - 2 * FRAMES, 1))
        out_ref[pl.ds(tile, many), width:] = piece
    sums = dot32(select_ref[...], terms_ref[...])
    out_ref[:, :width] = sums[:, :width] + (sums[:, width : 2 * width] + sums[:, 2 * width :])


def project(where, tiled, here, left, far, right):
    rows = TILES * SLOTS
    return pl.pallas_call(
        project_kernel,
        out_shape=jax.ShapeDtypeStruct((NEURONS, NEURONS + 2 * LANES), jnp.float32),
        in_specs=[SMEM] + [VMEM] * 5,
        out_specs=VMEM,
        scratch_shapes=[
            pltpu.VMEM((NEURONS, rows), jnp.bfloat16),
            pltpu.VMEM((rows, 3 * (NEURONS + LANES)), jnp.bfloat16),
        ],
        cost_estimate=pl.CostEstimate(flops=2_000_000_000, bytes_accessed=3_000_000, transcendentals=0),
        compiler_params=pltpu.CompilerParams(vmem_limit_bytes=16 << 20),
        name="project",
    )(where, tiled, here, left, far, right)


def solve_kernel(where_ref, mine_ref, other_ref, *refs):
    out_refs, current_ref, own_ref = refs[:PLANES], refs[PLANES], refs[PLANES + 1]
    x, core = where_ref[0], where_ref[2]
    sums = mine_ref[:, : NEURONS + LANES] + other_ref[:, : NEURONS + LANES]
    coupling = sums[:, :NEURONS]
    source = iota((LANES, LANES), 0)
    target = lax.rem(iota((LANES, LANES), 1), FRAMES)
    fold = jnp.where(lax.rem(source, FRAMES) == target, 1.0, 0.0)
    drive = place(sums[:, NEURONS:], fold.astype(jnp.bfloat16))
    copy = jnp.where(source == target, 1.0, 0.0).astype(jnp.bfloat16)
    here = mine_ref[:TILES, NEURONS + LANES :]
    there = other_ref[:TILES, NEURONS + LANES :]
    current_ref[pl.ds(0, TILES, stride=2), :] = place(jnp.where(core == 0, here, there), copy)
    current_ref[pl.ds(1, TILES, stride=2), :] = place(jnp.where(core == 0, there, here), copy)
    current = current_ref[...]
    bound = 1.0 + jnp.sum(coupling, axis=1, keepdims=True)
    for _ in range(ITERS):
        product = jnp.dot(coupling, current, preferred_element_type=jnp.float32, precision=HIGHEST)
        current = jnp.maximum(current - (product - drive) / bound, 0.0)
    current_ref[...] = current
    even = current_ref[pl.ds(0, TILES, stride=2), :]
    odd = current_ref[pl.ds(1, TILES, stride=2), :]
    own_ref[...] = jnp.where(core == 0, even, odd)
    for k in range(PLANES):
        at = pl.multiple_of(PLANE * lax.rem(x + k, PLANES), PLANE)
        out_refs[k][...] = own_ref[pl.ds(at, PLANE), :]


def solve(where, mine, other):
    return pl.pallas_call(
        solve_kernel,
        out_shape=[jax.ShapeDtypeStruct((PLANE, LANES), jnp.float32)] * PLANES,
        in_specs=[SMEM, VMEM, VMEM],
        out_specs=[VMEM] * PLANES,
        scratch_shapes=[pltpu.VMEM((NEURONS, LANES), jnp.float32), pltpu.VMEM((TILES, LANES), jnp.float32)],
        cost_estimate=pl.CostEstimate(flops=2_000_000_000, bytes_accessed=1_000_000, transcendentals=0),
        compiler_params=pltpu.CompilerParams(vmem_limit_bytes=8 << 20),
        name="solve",
    )(where, mine, other)


def merge_kernel(where_ref, *refs):
    group = lax.rem(iota((PLANE, LANES), 1) // FRAMES, PLANES)
    merged = refs[0][...]
    for k in range(1, PLANES):
        merged = jnp.where(group == lax.rem(where_ref[0] + PLANES - k, PLANES), refs[k][...], merged)
    refs[PLANES][...] = merged


def merge(where, pieces):
    return pl.pallas_call(
        merge_kernel,
        out_shape=jax.ShapeDtypeStruct((PLANE, LANES), jnp.float32),
        in_specs=[SMEM] + [VMEM] * PLANES,
        out_specs=VMEM,
        cost_estimate=pl.CostEstimate(flops=100_000_000, bytes_accessed=100_000, transcendentals=0),
        compiler_params=pltpu.CompilerParams(vmem_limit_bytes=2 << 20),
        name="merge",
    )(where, *pieces)


def join_kernel(pieces_ref, out_ref):
    near = LANES // FRAMES
    pieces = pieces_ref[...]
    rolled = [pieces] + [pltpu.roll(pieces, FRAMES * j, 1) for j in range(1, PLANES)]
    group = iota((near, LANES), 1) // FRAMES
    inside = group == iota((near, LANES), 0)
    for b in range(TILES // near):
        xs, first = b // 2, near * (b % 2)
        total = jnp.zeros((near, LANES), jnp.float32)
        for j in range(PLANES):
            hit = inside & (lax.rem(group + PLANES - j, PLANES) == xs)
            total = jnp.where(hit, rolled[j][first : first + near], total)
        out_ref[:, b * LANES : (b + 1) * LANES] = jnp.sum(total, axis=0, keepdims=True)


def join(pieces):
    return pl.pallas_call(
        join_kernel,
        out_shape=jax.ShapeDtypeStruct((1, TILES * FRAMES), jnp.float32),
        in_specs=[VMEM],
        out_specs=VMEM,
        compiler_params=pltpu.CompilerParams(vmem_limit_bytes=2 << 20),
        name="join",
    )(pieces)


def store_kernel(arrived_ref, out_ref, sems):
    copies = [pltpu.make_async_copy(arrived_ref.at[:, x], out_ref.at[x], sems.at[x]) for x in range(PLANES)]
    for copy in copies:
        copy.start()
    for copy in copies:
        copy.wait()


def store(arrived):
    return pl.pallas_call(
        store_kernel,
        out_shape=jax.ShapeDtypeStruct((PLANES, PLANE, FRAMES, PIXELS), jnp.bfloat16),
        in_specs=[VMEM],
        out_specs=pl.BlockSpec(memory_space=pl.ANY),
        scratch_shapes=[pltpu.SemaphoreType.DMA((PLANES,))],
        cost_estimate=pl.CostEstimate(flops=500_000_000, bytes_accessed=2_000_000, transcendentals=0),
        compiler_params=pltpu.CompilerParams(vmem_limit_bytes=4 << 20),
        name="store",
    )(arrived.reshape(PLANE, PLANES, FRAMES, PIXELS))


def moved(array, axis, by):
    count = lax.axis_size(axis)
    return lax.ppermute(array, axis, [(i, (i + by) % count) for i in range(count)])


def local(movie, shifts, footprint, support, neuron_ids, owner_order, start_traces):
    where = jnp.stack([lax.axis_index(axis) for axis in ("ta_0", "ta_1", "row")]).astype(jnp.int32)
    packed = pack(neuron_ids[0], owner_order, footprint[0, 0], support[0, 0], start_traces.reshape(8, LANES))
    here = lax.all_to_all(packed, YZ, 0, 0, tiled=True)
    registered = register(movie[0], shifts[0])
    tiled = smooth(registered)
    arrived = lax.all_to_all(tiled, YZX, split_axis=0, concat_axis=0, tiled=True)
    left, far, right = [moved(here, "ta_0", by) for by in range(1, PLANES)]
    mine = project(where, tiled, here, left, far, right)
    other = moved(mine, "row", 1)
    pieces = solve(where, mine, other)
    pieces = [pieces[0]] + [moved(pieces[k], "ta_0", k) for k in range(1, PLANES)]
    pieces = merge(where, pieces)
    pieces = lax.all_to_all(pieces.reshape(PLANE, 1, LANES), YZ, 0, 0, tiled=True)
    tile_movie = store(arrived)
    traces = join(pieces.reshape(PLANE, LANES))
    return (tile_movie.reshape(1, 1, -1, PIXELS), traces)


def solution(mesh):
    finer = Mesh(mesh.devices.reshape(4, 4, 8, mesh.shape["row"]), TA_ROW)
    return jax.shard_map(
        local,
        mesh=finer,
        in_specs=(
            P("row", TA, None, None),
            P("row", TA, None, None),
            P("row", TA, None, None),
            P("row", TA, None, None),
            P("row", TA, None),
            P(),
            P(TA_ROW, None),
        ),
        out_specs=(P("row", TA, None, None), P(TA_ROW, None)),
        check_vma=False,
    )
```

```python
import jax
import jax.numpy as jnp
import numpy as np
from jax import lax
from jax.experimental import pallas as pl
from jax.experimental.pallas import tpu as pltpu
from jax.sharding import Mesh
from jax.sharding import PartitionSpec as P

TH = 16
TW = 32
MAXS = 8
ITERS = 2
TA = ("ta_0", "ta_1", "ta_2")
XZ = ("ta_0", "ta_2")
YZX = ("ta_1", "ta_2", "ta_0")
TA_ROW = ("ta_0", "ta_1", "ta_2", "row")

FRAMES = 8
H = 128
W = 512
LANES = 128
BLOCKS = W // LANES
SLOTS = 8
NEURONS = 256
TILES = 128
PIXELS = TH * TW
PLANE = 32
PLANES = 4
LINE = 8
MESSAGE = PIXELS + LANES
ID_LANE = 64
HIGHEST = lax.Precision.HIGHEST
VMEM = pl.BlockSpec(memory_space=pltpu.VMEM)
SMEM = pl.BlockSpec(memory_space=pltpu.SMEM)


def smoothing_table(length):
    places = np.arange(length, dtype=np.float32)
    spread = places[:, None] - places[None, :]
    kernel = np.exp(-spread * spread / np.float32(32.0)).astype(np.float32)
    return (kernel / np.sum(kernel, axis=0, keepdims=True, dtype=np.float32)).astype(jnp.bfloat16)


def iota(shape, dim):
    return lax.broadcasted_iota(jnp.int32, shape, dim)


def split3(value):
    high = value.astype(jnp.bfloat16)
    rest = value - high.astype(jnp.float32)
    mid = rest.astype(jnp.bfloat16)
    low = (rest - mid.astype(jnp.float32)).astype(jnp.bfloat16)
    return high, mid, low


def dot32(left, right):
    return jnp.dot(left, right, preferred_element_type=jnp.float32)


def place(value, exact):
    high, mid, low = split3(value)
    return dot32(high, exact) + (dot32(mid, exact) + dot32(low, exact))


def register_kernel(shifts_ref, movie_ref, out_ref, padded_ref):
    lane = iota((H, LANES), 1)
    for s in range(2 * BLOCKS):
        padded_ref[s, pl.ds(0, MAXS), :] = jnp.zeros((MAXS, LANES), jnp.float32)
        padded_ref[s, pl.ds(MAXS + H, MAXS), :] = jnp.zeros((MAXS, LANES), jnp.float32)

    def block(f, p):
        if p < 0 or p >= BLOCKS:
            return None
        return movie_ref[f, :, p * LANES : (p + 1) * LANES].astype(jnp.float32)

    def shift(f, p, s):
        dy = shifts_ref[f, p, 0]
        dx = shifts_ref[f, p, 1]
        amount = jnp.where(dx > 0, LANES - dx, -dx)
        source = lane + dx

        def rolled(value):
            if value is None:
                return jnp.zeros((H, LANES), jnp.float32)
            return pltpu.roll(value, amount, 1)

        inner = jnp.where(source >= LANES, rolled(block(f, p + 1)), rolled(block(f, p)))
        padded_ref[s, pl.ds(MAXS, H), :] = jnp.where(source < 0, rolled(block(f, p - 1)), inner)
        out_ref[f, :, p * LANES : (p + 1) * LANES] = padded_ref[s, pl.ds(MAXS + dy, H), :].astype(jnp.bfloat16)

    def frames(g, carry):
        for h in range(2):
            for p in range(BLOCKS):
                shift(2 * g + h, p, h * BLOCKS + p)
        return carry

    lax.fori_loop(0, FRAMES // 2, frames, 0)


def register(movie, shifts):
    return pl.pallas_call(
        register_kernel,
        out_shape=jax.ShapeDtypeStruct((FRAMES, H, W), jnp.bfloat16),
        in_specs=[SMEM, VMEM],
        out_specs=VMEM,
        scratch_shapes=[pltpu.VMEM((2 * BLOCKS, H + 2 * MAXS, LANES), jnp.float32)],
        cost_estimate=pl.CostEstimate(flops=2_000_000_000, bytes_accessed=2_000_000, transcendentals=0),
        compiler_params=pltpu.CompilerParams(vmem_limit_bytes=8 << 20),
        name="register",
    )(shifts, movie)


def smooth_kernel(registered_ref, wide_ref, tall_ref, out_ref, filtered_ref, soft_ref):
    step = 2

    def chunk(c, carry):
        registered = registered_ref[pl.ds(c * step, step)].reshape(step * H, W)
        soft_ref[...] = dot32(registered, wide_ref[...]).astype(jnp.bfloat16)
        for k in range(step):
            low = dot32(tall_ref[...], soft_ref[k * H : (k + 1) * H, :])
            filtered = registered[k * H : (k + 1) * H].astype(jnp.float32) - low
            for p in range(BLOCKS):
                span = pl.ds(c * step + k, H, stride=FRAMES)
                filtered_ref[p, span, :] = filtered[:, p * LANES : (p + 1) * LANES]
        return carry

    lax.fori_loop(0, FRAMES // step, chunk, 0)
    lanes8 = iota((FRAMES, LANES), 1)
    near = lanes8 < 2 * TW
    even = lax.rem(lanes8 // TW, 2) == 0

    def tile_row(ty, carry):
        for q in range(4):
            for p in range(BLOCKS):
                v = []
                for r in range(4):
                    at = pl.multiple_of((ty * TH + 4 * q + r) * FRAMES, FRAMES)
                    v.append(filtered_ref[p, pl.ds(at, FRAMES), :])
                a0 = jnp.where(near, v[0], pltpu.roll(v[2], 64, 1))
                a2 = jnp.where(near, pltpu.roll(v[0], 64, 1), v[2])
                a1 = jnp.where(near, v[1], pltpu.roll(v[3], 64, 1))
                a3 = jnp.where(near, pltpu.roll(v[1], 64, 1), v[3])
                tiles = (
                    jnp.where(even, a0, pltpu.roll(a1, 32, 1)),
                    jnp.where(even, pltpu.roll(a0, 96, 1), a1),
                    jnp.where(even, a2, pltpu.roll(a3, 32, 1)),
                    jnp.where(even, pltpu.roll(a2, 96, 1), a3),
                )
                for m in range(4):
                    column = 4 * p + m
                    at = (16 * lax.rem(ty, 2) + column) * 4 + ty // 2
                    out_ref[at, :, q * LANES : (q + 1) * LANES] = tiles[m].astype(jnp.bfloat16)
        return carry

    lax.fori_loop(0, H // TH, tile_row, 0)


def smooth(registered):
    return pl.pallas_call(
        smooth_kernel,
        out_shape=jax.ShapeDtypeStruct((TILES, FRAMES, PIXELS), jnp.bfloat16),
        in_specs=[VMEM] * 3,
        out_specs=VMEM,
        scratch_shapes=[
            pltpu.VMEM((BLOCKS, H * FRAMES, LANES), jnp.float32),
            pltpu.VMEM((2 * H, W), jnp.bfloat16),
        ],
        cost_estimate=pl.CostEstimate(flops=4_000_000_000, bytes_accessed=3_000_000, transcendentals=0),
        compiler_params=pltpu.CompilerParams(vmem_limit_bytes=16 << 20),
        name="smooth",
    )(registered, smoothing_table(W), smoothing_table(H).T)


def pack_kernel(ids_ref, order_ref, footprint_ref, support_ref, start_ref, out_ref):
    footprints = footprint_ref[...] * support_ref[...].astype(jnp.bfloat16)
    parts = [part.astype(jnp.float32) for part in split3(start_ref[...])]
    row = iota((SLOTS, LANES), 0)
    lane = iota((SLOTS, LANES), 1)
    owners = jnp.zeros((SLOTS, LANES), jnp.float32)
    for i in range(SLOTS):
        owner = order_ref[ids_ref[0, i]].astype(jnp.float32)
        owners = jnp.where((row == i) & (lane == ID_LANE), owner, owners)
    for w in range(LINE):
        extra = owners
        for half in range(2):
            for k, part in enumerate(parts):
                group = 3 * half + k
                turned = pltpu.roll(part, (FRAMES * (group - w - LINE * half)) % LANES, 1)
                extra = jnp.where(lane // FRAMES == group, turned, extra)
        for to in range(w, PLANE, LINE):
            out_ref[to, :, :PIXELS] = footprints
            out_ref[to, :, PIXELS:] = extra.astype(jnp.bfloat16)


def pack(ids, order, footprint, support, start):
    return pl.pallas_call(
        pack_kernel,
        out_shape=jax.ShapeDtypeStruct((PLANE, SLOTS, MESSAGE), jnp.bfloat16),
        in_specs=[SMEM, SMEM, VMEM, VMEM, VMEM],
        out_specs=VMEM,
        cost_estimate=pl.CostEstimate(flops=200_000_000, bytes_accessed=200_000, transcendentals=0),
        name="pack",
    )(ids, order, footprint, support, start)


def project_kernel(
    where_ref, tiled_ref, here_ref, left_ref, far_ref, right_ref, out_ref, select_ref, terms_ref
):
    x, y = where_ref[0], where_ref[1]
    many = PLANE // 2
    rows = many * SLOTS
    width = NEURONS + LANES
    same = iota((rows, 2 * rows), 0) // SLOTS == lax.rem(iota((rows, 2 * rows), 1), rows) // SLOTS
    own_row = iota((many, SLOTS, LANES), 1) == 2 * x + y // 2
    back = lax.rem(LANES - 3 * FRAMES * lax.rem(y, 2), LANES)
    contract = (((1,), (1,)), ((), ()))
    neuron = iota((rows, NEURONS), 1)
    neuron_t = iota((NEURONS, rows), 0)
    diagonal = iota((rows, rows), 0) == iota((rows, rows), 1)
    out_ref[:, width:] = jnp.zeros((NEURONS, LANES), jnp.float32)
    for at in range(2 * PLANES):
        ky, first = at // 2, many * (at % 2)
        message = (here_ref, left_ref, far_ref, right_ref)[ky][first : first + many]
        source = lax.rem(y + PLANES - ky, PLANES)
        frames = [
            tiled_ref[PLANES * (LINE * source + k % LINE) + (first + k) // LINE] for k in range(many)
        ]
        prints = message[:, :, :PIXELS].reshape(rows, PIXELS)
        extra = message[:, :, PIXELS:].astype(jnp.float32).reshape(rows, LANES)
        found = lax.dot_general(
            prints, jnp.concatenate(frames + [prints], axis=0), contract, preferred_element_type=jnp.float32
        )
        found = jnp.where(same, found, 0.0)
        ids = extra[:, ID_LANE : ID_LANE + 1]
        select = jnp.where(neuron == ids.astype(jnp.int32), 1.0, 0.0).astype(jnp.bfloat16)
        ids_row = jnp.sum(jnp.where(diagonal, ids, 0.0), axis=0, keepdims=True).astype(jnp.int32)
        span = slice(at * rows, (at + 1) * rows)
        select_ref[:, span] = jnp.where(neuron_t == ids_row, 1.0, 0.0).astype(jnp.bfloat16)
        spread = place(found[:, rows:], select)
        for k, (one, two) in enumerate(zip(split3(spread), split3(found[:, :rows]), strict=True)):
            terms_ref[span, k * width : k * width + NEURONS] = one
            terms_ref[span, k * width + NEURONS : (k + 1) * width] = two
        piece = jnp.sum(jnp.where(own_row, extra.reshape(many, SLOTS, LANES), 0.0), axis=1)
        piece = pltpu.roll(piece, back, 1)
        piece = piece + (pltpu.roll(piece, LANES - FRAMES, 1) + pltpu.roll(piece, LANES - 2 * FRAMES, 1))
        for k in range(many // LINE):
            tile = pl.multiple_of(PLANE * (first // LINE + k) + LINE * source, LINE)
            out_ref[pl.ds(tile, LINE), width:] = piece[k * LINE : (k + 1) * LINE]
    sums = dot32(select_ref[...], terms_ref[...])
    out_ref[:, :width] = sums[:, :width] + (sums[:, width : 2 * width] + sums[:, 2 * width :])


def project(where, tiled, here, left, far, right):
    rows = TILES * SLOTS
    return pl.pallas_call(
        project_kernel,
        out_shape=jax.ShapeDtypeStruct((NEURONS, NEURONS + 2 * LANES), jnp.float32),
        in_specs=[SMEM] + [VMEM] * 5,
        out_specs=VMEM,
        scratch_shapes=[
            pltpu.VMEM((NEURONS, rows), jnp.bfloat16),
            pltpu.VMEM((rows, 3 * (NEURONS + LANES)), jnp.bfloat16),
        ],
        cost_estimate=pl.CostEstimate(flops=2_000_000_000, bytes_accessed=3_000_000, transcendentals=0),
        compiler_params=pltpu.CompilerParams(vmem_limit_bytes=16 << 20),
        name="project",
    )(where, tiled, here, left, far, right)


def solve_kernel(where_ref, mine_ref, other_ref, *refs):
    out_refs, current_ref, own_ref = refs[:PLANES], refs[PLANES], refs[PLANES + 1]
    y, core = where_ref[1], where_ref[2]
    sums = mine_ref[:, : NEURONS + LANES] + other_ref[:, : NEURONS + LANES]
    coupling = sums[:, :NEURONS]
    source = iota((LANES, LANES), 0)
    target = lax.rem(iota((LANES, LANES), 1), FRAMES)
    fold = jnp.where(lax.rem(source, FRAMES) == target, 1.0, 0.0)
    drive = place(sums[:, NEURONS:], fold.astype(jnp.bfloat16))
    copy = jnp.where(source == target, 1.0, 0.0).astype(jnp.bfloat16)
    here = mine_ref[:TILES, NEURONS + LANES :]
    there = other_ref[:TILES, NEURONS + LANES :]
    current_ref[pl.ds(0, TILES, stride=2), :] = place(jnp.where(core == 0, here, there), copy)
    current_ref[pl.ds(1, TILES, stride=2), :] = place(jnp.where(core == 0, there, here), copy)
    current = current_ref[...]
    bound = 1.0 + jnp.sum(coupling, axis=1, keepdims=True)
    for _ in range(ITERS):
        product = jnp.dot(coupling, current, preferred_element_type=jnp.float32, precision=HIGHEST)
        current = jnp.maximum(current - (product - drive) / bound, 0.0)
    current_ref[...] = current
    even = current_ref[pl.ds(0, TILES, stride=2), :]
    odd = current_ref[pl.ds(1, TILES, stride=2), :]
    own_ref[...] = jnp.where(core == 0, even, odd)
    for k in range(PLANES):
        for x in range(PLANE // LINE):
            at = pl.multiple_of(PLANE * x + LINE * lax.rem(y + k, PLANES), LINE)
            out_refs[k][x * LINE : (x + 1) * LINE, :] = own_ref[pl.ds(at, LINE), :]


def solve(where, mine, other):
    return pl.pallas_call(
        solve_kernel,
        out_shape=[jax.ShapeDtypeStruct((PLANE, LANES), jnp.float32)] * PLANES,
        in_specs=[SMEM, VMEM, VMEM],
        out_specs=[VMEM] * PLANES,
        scratch_shapes=[pltpu.VMEM((NEURONS, LANES), jnp.float32), pltpu.VMEM((TILES, LANES), jnp.float32)],
        cost_estimate=pl.CostEstimate(flops=2_000_000_000, bytes_accessed=1_000_000, transcendentals=0),
        compiler_params=pltpu.CompilerParams(vmem_limit_bytes=8 << 20),
        name="solve",
    )(where, mine, other)


def merge_kernel(where_ref, *refs):
    group = lax.rem(iota((PLANE, LANES), 1) // FRAMES, PLANES)
    merged = refs[0][...]
    for k in range(1, PLANES):
        merged = jnp.where(group == lax.rem(where_ref[1] + PLANES - k, PLANES), refs[k][...], merged)
    refs[PLANES][...] = merged


def merge(where, pieces):
    return pl.pallas_call(
        merge_kernel,
        out_shape=jax.ShapeDtypeStruct((PLANE, LANES), jnp.float32),
        in_specs=[SMEM] + [VMEM] * PLANES,
        out_specs=VMEM,
        cost_estimate=pl.CostEstimate(flops=100_000_000, bytes_accessed=100_000, transcendentals=0),
        compiler_params=pltpu.CompilerParams(vmem_limit_bytes=2 << 20),
        name="merge",
    )(where, *pieces)


def join_kernel(pieces_ref, out_ref):
    pieces = pieces_ref[...]
    rolled = [pieces] + [pltpu.roll(pieces, FRAMES * j, 1) for j in range(1, PLANES)]
    group = iota((LINE, LANES), 1) // FRAMES
    inside = lax.rem(group, LINE) == iota((LINE, LANES), 0)
    for b in range(TILES * FRAMES // LANES):
        first = LINE * (b // 2)
        total = jnp.zeros((LINE, LANES), jnp.float32)
        for j in range(PLANES):
            hit = inside & (lax.rem(group + PLANES - j, PLANES) == 2 * (b % 2) + group // LINE)
            total = jnp.where(hit, rolled[j][first : first + LINE], total)
        out_ref[:, b * LANES : (b + 1) * LANES] = jnp.sum(total, axis=0, keepdims=True)


def join(pieces):
    return pl.pallas_call(
        join_kernel,
        out_shape=jax.ShapeDtypeStruct((1, TILES * FRAMES), jnp.float32),
        in_specs=[VMEM],
        out_specs=VMEM,
        compiler_params=pltpu.CompilerParams(vmem_limit_bytes=2 << 20),
        name="join",
    )(pieces)


def store_kernel(arrived_ref, out_ref, sems):
    copies = [pltpu.make_async_copy(arrived_ref.at[:, x], out_ref.at[x], sems.at[x]) for x in range(PLANES)]
    for copy in copies:
        copy.start()
    for copy in copies:
        copy.wait()


def store(arrived):
    return pl.pallas_call(
        store_kernel,
        out_shape=jax.ShapeDtypeStruct((PLANES, PLANE, FRAMES, PIXELS), jnp.bfloat16),
        in_specs=[VMEM],
        out_specs=pl.BlockSpec(memory_space=pl.ANY),
        scratch_shapes=[pltpu.SemaphoreType.DMA((PLANES,))],
        cost_estimate=pl.CostEstimate(flops=500_000_000, bytes_accessed=2_000_000, transcendentals=0),
        compiler_params=pltpu.CompilerParams(vmem_limit_bytes=4 << 20),
        name="store",
    )(arrived.reshape(PLANE, PLANES, FRAMES, PIXELS))


def moved(array, axis, by):
    count = lax.axis_size(axis)
    return lax.ppermute(array, axis, [(i, (i + by) % count) for i in range(count)])


def local(movie, shifts, footprint, support, neuron_ids, owner_order, start_traces):
    where = jnp.stack([lax.axis_index(axis) for axis in ("ta_0", "ta_1", "row")]).astype(jnp.int32)
    packed = pack(neuron_ids[0], owner_order, footprint[0, 0], support[0, 0], start_traces.reshape(8, LANES))
    here = lax.all_to_all(packed, XZ, 0, 0, tiled=True)
    registered = register(movie[0], shifts[0])
    tiled = smooth(registered)
    arrived = lax.all_to_all(tiled, YZX, split_axis=0, concat_axis=0, tiled=True)
    left, far, right = [moved(here, "ta_1", by) for by in range(1, PLANES)]
    mine = project(where, tiled, here, left, far, right)
    other = moved(mine, "row", 1)
    pieces = solve(where, mine, other)
    pieces = [pieces[0]] + [moved(pieces[k], "ta_1", k) for k in range(1, PLANES)]
    pieces = merge(where, pieces)
    pieces = lax.all_to_all(pieces.reshape(PLANE, 1, LANES), XZ, 0, 0, tiled=True)
    tile_movie = store(arrived)
    traces = join(pieces.reshape(PLANE, LANES))
    return (tile_movie.reshape(1, 1, -1, PIXELS), traces)


def solution(mesh):
    finer = Mesh(mesh.devices.reshape(4, 4, 8, mesh.shape["row"]), TA_ROW)
    return jax.shard_map(
        local,
        mesh=finer,
        in_specs=(
            P("row", TA, None, None),
            P("row", TA, None, None),
            P("row", TA, None, None),
            P("row", TA, None, None),
            P("row", TA, None),
            P(),
            P(TA_ROW, None),
        ),
        out_specs=(P("row", TA, None, None), P(TA_ROW, None)),
        check_vma=False,
    )
```

```python
import jax
import jax.numpy as jnp
import numpy as np
from jax import lax
from jax.experimental import pallas as pl
from jax.experimental.pallas import tpu as pltpu
from jax.sharding import Mesh
from jax.sharding import PartitionSpec as P

TH = 16
TW = 32
MAXS = 8
ITERS = 2
TA = ("ta_0", "ta_1", "ta_2")
YZ = ("ta_1", "ta_2")
YZX = ("ta_1", "ta_2", "ta_0")
TA_ROW = ("ta_0", "ta_1", "ta_2", "row")

FRAMES = 8
H = 128
W = 512
LANES = 128
BLOCKS = W // LANES
SLOTS = 8
NEURONS = 256
TILES = 128
PIXELS = TH * TW
PLANE = 32
PLANES = 4
LINE = 8
MESSAGE = PIXELS + LANES
ID_LANE = 64
HIGHEST = lax.Precision.HIGHEST
VMEM = pl.BlockSpec(memory_space=pltpu.VMEM)
SMEM = pl.BlockSpec(memory_space=pltpu.SMEM)


def smoothing_table(length):
    places = np.arange(length, dtype=np.float32)
    spread = places[:, None] - places[None, :]
    kernel = np.exp(-spread * spread / np.float32(32.0)).astype(np.float32)
    return (kernel / np.sum(kernel, axis=0, keepdims=True, dtype=np.float32)).astype(jnp.bfloat16)


def iota(shape, dim):
    return lax.broadcasted_iota(jnp.int32, shape, dim)


def split3(value):
    high = value.astype(jnp.bfloat16)
    rest = value - high.astype(jnp.float32)
    mid = rest.astype(jnp.bfloat16)
    low = (rest - mid.astype(jnp.float32)).astype(jnp.bfloat16)
    return high, mid, low


def dot32(left, right):
    return jnp.dot(left, right, preferred_element_type=jnp.float32)


def place(value, exact):
    high, mid, low = split3(value)
    return dot32(high, exact) + (dot32(mid, exact) + dot32(low, exact))


def register_kernel(shifts_ref, movie_ref, out_ref, padded_ref):
    lane = iota((H, LANES), 1)
    for s in range(2 * BLOCKS):
        padded_ref[s, pl.ds(0, MAXS), :] = jnp.zeros((MAXS, LANES), jnp.float32)
        padded_ref[s, pl.ds(MAXS + H, MAXS), :] = jnp.zeros((MAXS, LANES), jnp.float32)

    def block(f, p):
        if p < 0 or p >= BLOCKS:
            return None
        return movie_ref[f, :, p * LANES : (p + 1) * LANES].astype(jnp.float32)

    def shift(f, p, s):
        dy = shifts_ref[f, p, 0]
        dx = shifts_ref[f, p, 1]
        amount = jnp.where(dx > 0, LANES - dx, -dx)
        source = lane + dx

        def rolled(value):
            if value is None:
                return jnp.zeros((H, LANES), jnp.float32)
            return pltpu.roll(value, amount, 1)

        inner = jnp.where(source >= LANES, rolled(block(f, p + 1)), rolled(block(f, p)))
        padded_ref[s, pl.ds(MAXS, H), :] = jnp.where(source < 0, rolled(block(f, p - 1)), inner)
        out_ref[f, :, p * LANES : (p + 1) * LANES] = padded_ref[s, pl.ds(MAXS + dy, H), :].astype(jnp.bfloat16)

    def frames(g, carry):
        for h in range(2):
            for p in range(BLOCKS):
                shift(2 * g + h, p, h * BLOCKS + p)
        return carry

    lax.fori_loop(0, FRAMES // 2, frames, 0)


def register(movie, shifts):
    return pl.pallas_call(
        register_kernel,
        out_shape=jax.ShapeDtypeStruct((FRAMES, H, W), jnp.bfloat16),
        in_specs=[SMEM, VMEM],
        out_specs=VMEM,
        scratch_shapes=[pltpu.VMEM((2 * BLOCKS, H + 2 * MAXS, LANES), jnp.float32)],
        cost_estimate=pl.CostEstimate(flops=2_000_000_000, bytes_accessed=2_000_000, transcendentals=0),
        compiler_params=pltpu.CompilerParams(vmem_limit_bytes=8 << 20),
        name="register",
    )(shifts, movie)


def smooth_kernel(registered_ref, wide_ref, tall_ref, out_ref, filtered_ref, soft_ref):
    step = 2

    def chunk(c, carry):
        registered = registered_ref[pl.ds(c * step, step)].reshape(step * H, W)
        soft_ref[...] = dot32(registered, wide_ref[...]).astype(jnp.bfloat16)
        for k in range(step):
            low = dot32(tall_ref[...], soft_ref[k * H : (k + 1) * H, :])
            filtered = registered[k * H : (k + 1) * H].astype(jnp.float32) - low
            for p in range(BLOCKS):
                span = pl.ds(c * step + k, H, stride=FRAMES)
                filtered_ref[p, span, :] = filtered[:, p * LANES : (p + 1) * LANES]
        return carry

    lax.fori_loop(0, FRAMES // step, chunk, 0)
    lanes8 = iota((FRAMES, LANES), 1)
    near = lanes8 < 2 * TW
    even = lax.rem(lanes8 // TW, 2) == 0

    def tile_row(ty, carry):
        for q in range(4):
            for p in range(BLOCKS):
                v = []
                for r in range(4):
                    at = pl.multiple_of((ty * TH + 4 * q + r) * FRAMES, FRAMES)
                    v.append(filtered_ref[p, pl.ds(at, FRAMES), :])
                a0 = jnp.where(near, v[0], pltpu.roll(v[2], 64, 1))
                a2 = jnp.where(near, pltpu.roll(v[0], 64, 1), v[2])
                a1 = jnp.where(near, v[1], pltpu.roll(v[3], 64, 1))
                a3 = jnp.where(near, pltpu.roll(v[1], 64, 1), v[3])
                tiles = (
                    jnp.where(even, a0, pltpu.roll(a1, 32, 1)),
                    jnp.where(even, pltpu.roll(a0, 96, 1), a1),
                    jnp.where(even, a2, pltpu.roll(a3, 32, 1)),
                    jnp.where(even, pltpu.roll(a2, 96, 1), a3),
                )
                for m in range(4):
                    column = 4 * p + m
                    at = (16 * lax.rem(ty, 2) + column) * 4 + ty // 2
                    out_ref[at, :, q * LANES : (q + 1) * LANES] = tiles[m].astype(jnp.bfloat16)
        return carry

    lax.fori_loop(0, H // TH, tile_row, 0)


def smooth(registered):
    return pl.pallas_call(
        smooth_kernel,
        out_shape=jax.ShapeDtypeStruct((TILES, FRAMES, PIXELS), jnp.bfloat16),
        in_specs=[VMEM] * 3,
        out_specs=VMEM,
        scratch_shapes=[
            pltpu.VMEM((BLOCKS, H * FRAMES, LANES), jnp.float32),
            pltpu.VMEM((2 * H, W), jnp.bfloat16),
        ],
        cost_estimate=pl.CostEstimate(flops=4_000_000_000, bytes_accessed=3_000_000, transcendentals=0),
        compiler_params=pltpu.CompilerParams(vmem_limit_bytes=16 << 20),
        name="smooth",
    )(registered, smoothing_table(W), smoothing_table(H).T)


def pack_kernel(ids_ref, order_ref, footprint_ref, support_ref, start_ref, out_ref):
    footprints = footprint_ref[...] * support_ref[...].astype(jnp.bfloat16)
    parts = [part.astype(jnp.float32) for part in split3(start_ref[...])]
    row = iota((SLOTS, LANES), 0)
    lane = iota((SLOTS, LANES), 1)
    owners = jnp.zeros((SLOTS, LANES), jnp.float32)
    for i in range(SLOTS):
        owner = order_ref[ids_ref[0, i]].astype(jnp.float32)
        owners = jnp.where((row == i) & (lane == ID_LANE), owner, owners)
    for w in range(PLANE // 2):
        extra = owners
        for k, part in enumerate(parts):
            extra = jnp.where(lane // FRAMES == k, pltpu.roll(part, (FRAMES * (k - w)) % LANES, 1), extra)
        for to in (w, w + PLANE // 2):
            out_ref[to, :, :PIXELS] = footprints
            out_ref[to, :, PIXELS:] = extra.astype(jnp.bfloat16)


def pack(ids, order, footprint, support, start):
    return pl.pallas_call(
        pack_kernel,
        out_shape=jax.ShapeDtypeStruct((PLANE, SLOTS, MESSAGE), jnp.bfloat16),
        in_specs=[SMEM, SMEM, VMEM, VMEM, VMEM],
        out_specs=VMEM,
        cost_estimate=pl.CostEstimate(flops=200_000_000, bytes_accessed=200_000, transcendentals=0),
        name="pack",
    )(ids, order, footprint, support, start)


def project_kernel(
    where_ref, tiled_ref, here_ref, left_ref, far_ref, right_ref, out_ref, select_ref, terms_ref
):
    x, y = where_ref[0], where_ref[1]
    many = PLANE // 2
    rows = many * SLOTS
    width = NEURONS + LANES
    same = iota((rows, 2 * rows), 0) // SLOTS == lax.rem(iota((rows, 2 * rows), 1), rows) // SLOTS
    own_row = iota((many, SLOTS, LANES), 1) == 2 * x + y // 2
    contract = (((1,), (1,)), ((), ()))
    neuron = iota((rows, NEURONS), 1)
    neuron_t = iota((NEURONS, rows), 0)
    diagonal = iota((rows, rows), 0) == iota((rows, rows), 1)
    out_ref[:, width:] = jnp.zeros((NEURONS, LANES), jnp.float32)
    for at in range(2 * PLANES):
        kx, first = at // 2, many * (at % 2)
        message = (here_ref, left_ref, far_ref, right_ref)[kx][first : first + many]
        source = lax.rem(x + PLANES - kx, PLANES)
        tile = pl.multiple_of(PLANE * source + first, many)
        frames = [tiled_ref[PLANES * (first + k) + source] for k in range(many)]
        prints = message[:, :, :PIXELS].reshape(rows, PIXELS)
        extra = message[:, :, PIXELS:].astype(jnp.float32).reshape(rows, LANES)
        found = lax.dot_general(
            prints, jnp.concatenate(frames + [prints], axis=0), contract, preferred_element_type=jnp.float32
        )
        found = jnp.where(same, found, 0.0)
        ids = extra[:, ID_LANE : ID_LANE + 1]
        select = jnp.where(neuron == ids.astype(jnp.int32), 1.0, 0.0).astype(jnp.bfloat16)
        ids_row = jnp.sum(jnp.where(diagonal, ids, 0.0), axis=0, keepdims=True).astype(jnp.int32)
        span = slice(at * rows, (at + 1) * rows)
        select_ref[:, span] = jnp.where(neuron_t == ids_row, 1.0, 0.0).astype(jnp.bfloat16)
        spread = place(found[:, rows:], select)
        for k, (one, two) in enumerate(zip(split3(spread), split3(found[:, :rows]), strict=True)):
            terms_ref[span, k * width : k * width + NEURONS] = one
            terms_ref[span, k * width + NEURONS : (k + 1) * width] = two
        piece = jnp.sum(jnp.where(own_row, extra.reshape(many, SLOTS, LANES), 0.0), axis=1)
        piece = piece + (pltpu.roll(piece, LANES - FRAMES, 1) + pltpu.roll(piece, LANES - 2 * FRAMES, 1))
        out_ref[pl.ds(tile, many), width:] = piece
    sums = dot32(select_ref[...], terms_ref[...])
    out_ref[:, :width] = sums[:, :width] + (sums[:, width : 2 * width] + sums[:, 2 * width :])


def project(where, tiled, here, left, far, right):
    rows = TILES * SLOTS
    return pl.pallas_call(
        project_kernel,
        out_shape=jax.ShapeDtypeStruct((NEURONS, NEURONS + 2 * LANES), jnp.float32),
        in_specs=[SMEM] + [VMEM] * 5,
        out_specs=VMEM,
        scratch_shapes=[
            pltpu.VMEM((NEURONS, rows), jnp.bfloat16),
            pltpu.VMEM((rows, 3 * (NEURONS + LANES)), jnp.bfloat16),
        ],
        cost_estimate=pl.CostEstimate(flops=2_000_000_000, bytes_accessed=3_000_000, transcendentals=0),
        compiler_params=pltpu.CompilerParams(vmem_limit_bytes=16 << 20),
        name="project",
    )(where, tiled, here, left, far, right)


def solve_kernel(where_ref, mine_ref, other_ref, *refs):
    out_refs, current_ref, own_ref = refs[:PLANES], refs[PLANES], refs[PLANES + 1]
    x, core = where_ref[0], where_ref[2]
    sums = mine_ref[:, : NEURONS + LANES] + other_ref[:, : NEURONS + LANES]
    coupling = sums[:, :NEURONS]
    source = iota((LANES, LANES), 0)
    target = lax.rem(iota((LANES, LANES), 1), FRAMES)
    fold = jnp.where(lax.rem(source, FRAMES) == target, 1.0, 0.0)
    drive = place(sums[:, NEURONS:], fold.astype(jnp.bfloat16))
    copy = jnp.where(source == target, 1.0, 0.0).astype(jnp.bfloat16)
    here = mine_ref[:TILES, NEURONS + LANES :]
    there = other_ref[:TILES, NEURONS + LANES :]
    current_ref[pl.ds(0, TILES, stride=2), :] = place(jnp.where(core == 0, here, there), copy)
    current_ref[pl.ds(1, TILES, stride=2), :] = place(jnp.where(core == 0, there, here), copy)
    current = current_ref[...]
    bound = 1.0 + jnp.sum(coupling, axis=1, keepdims=True)
    for _ in range(ITERS):
        product = jnp.dot(coupling, current, preferred_element_type=jnp.float32, precision=HIGHEST)
        current = jnp.maximum(current - (product - drive) / bound, 0.0)
    current_ref[...] = current
    even = current_ref[pl.ds(0, TILES, stride=2), :]
    odd = current_ref[pl.ds(1, TILES, stride=2), :]
    own_ref[...] = jnp.where(core == 0, even, odd)
    for k in range(PLANES):
        at = pl.multiple_of(PLANE * lax.rem(x + k, PLANES), PLANE)
        out_refs[k][...] = own_ref[pl.ds(at, PLANE), :]


def solve(where, mine, other):
    return pl.pallas_call(
        solve_kernel,
        out_shape=[jax.ShapeDtypeStruct((PLANE, LANES), jnp.float32)] * PLANES,
        in_specs=[SMEM, VMEM, VMEM],
        out_specs=[VMEM] * PLANES,
        scratch_shapes=[pltpu.VMEM((NEURONS, LANES), jnp.float32), pltpu.VMEM((TILES, LANES), jnp.float32)],
        cost_estimate=pl.CostEstimate(flops=2_000_000_000, bytes_accessed=1_000_000, transcendentals=0),
        compiler_params=pltpu.CompilerParams(vmem_limit_bytes=8 << 20),
        name="solve",
    )(where, mine, other)


def merge_kernel(where_ref, *refs):
    out_refs, merged_ref = refs[PLANES : 2 * PLANES], refs[2 * PLANES]
    group = lax.rem(iota((PLANE, LANES), 1) // FRAMES, PLANES)
    merged = refs[0][...]
    for k in range(1, PLANES):
        merged = jnp.where(group == lax.rem(where_ref[0] + PLANES - k, PLANES), refs[k][...], merged)
    merged_ref[...] = merged
    for k in range(PLANES):
        at = pl.multiple_of(LINE * lax.rem(where_ref[1] + k, PLANES), LINE)
        out_refs[k][...] = merged_ref[pl.ds(at, LINE), :]


def merge(where, pieces):
    return pl.pallas_call(
        merge_kernel,
        out_shape=[jax.ShapeDtypeStruct((LINE, LANES), jnp.float32)] * PLANES,
        in_specs=[SMEM] + [VMEM] * PLANES,
        out_specs=[VMEM] * PLANES,
        scratch_shapes=[pltpu.VMEM((PLANE, LANES), jnp.float32)],
        cost_estimate=pl.CostEstimate(flops=100_000_000, bytes_accessed=100_000, transcendentals=0),
        compiler_params=pltpu.CompilerParams(vmem_limit_bytes=2 << 20),
        name="merge",
    )(where, *pieces)


def gather_kernel(where_ref, *refs):
    group = iota((LINE, LANES), 1) // FRAMES // PLANES
    merged = refs[0][...]
    for k in range(1, PLANES):
        merged = jnp.where(group == lax.rem(where_ref[1] + PLANES - k, PLANES), refs[k][...], merged)
    refs[PLANES][...] = merged


def gather(where, pieces):
    return pl.pallas_call(
        gather_kernel,
        out_shape=jax.ShapeDtypeStruct((LINE, LANES), jnp.float32),
        in_specs=[SMEM] + [VMEM] * PLANES,
        out_specs=VMEM,
        cost_estimate=pl.CostEstimate(flops=100_000_000, bytes_accessed=100_000, transcendentals=0),
        compiler_params=pltpu.CompilerParams(vmem_limit_bytes=2 << 20),
        name="gather",
    )(where, *pieces)


def join_kernel(pieces_ref, out_ref):
    pieces = pieces_ref[...]
    places = LANES // FRAMES
    rolled = [pieces] + [pltpu.roll(pieces, FRAMES * j, 1) for j in range(1, places)]
    group = iota((LINE, LANES), 1) // FRAMES
    inside = lax.rem(group, LINE) == iota((LINE, LANES), 0)
    for b in range(TILES * FRAMES // LANES):
        wanted = PLANES * (2 * (b % 2) + group // LINE) + b // 2
        shift = lax.rem(group - wanted + places, places)
        total = jnp.zeros((LINE, LANES), jnp.float32)
        for j in range(places):
            total = jnp.where(inside & (shift == j), rolled[j], total)
        out_ref[:, b * LANES : (b + 1) * LANES] = jnp.sum(total, axis=0, keepdims=True)


def join(pieces):
    return pl.pallas_call(
        join_kernel,
        out_shape=jax.ShapeDtypeStruct((1, TILES * FRAMES), jnp.float32),
        in_specs=[VMEM],
        out_specs=VMEM,
        compiler_params=pltpu.CompilerParams(vmem_limit_bytes=2 << 20),
        name="join",
    )(pieces)


def store_kernel(arrived_ref, out_ref, sems):
    copies = [pltpu.make_async_copy(arrived_ref.at[:, x], out_ref.at[x], sems.at[x]) for x in range(PLANES)]
    for copy in copies:
        copy.start()
    for copy in copies:
        copy.wait()


def store(arrived):
    return pl.pallas_call(
        store_kernel,
        out_shape=jax.ShapeDtypeStruct((PLANES, PLANE, FRAMES, PIXELS), jnp.bfloat16),
        in_specs=[VMEM],
        out_specs=pl.BlockSpec(memory_space=pl.ANY),
        scratch_shapes=[pltpu.SemaphoreType.DMA((PLANES,))],
        cost_estimate=pl.CostEstimate(flops=500_000_000, bytes_accessed=2_000_000, transcendentals=0),
        compiler_params=pltpu.CompilerParams(vmem_limit_bytes=4 << 20),
        name="store",
    )(arrived.reshape(PLANE, PLANES, FRAMES, PIXELS))


def moved(array, axis, by):
    count = lax.axis_size(axis)
    return lax.ppermute(array, axis, [(i, (i + by) % count) for i in range(count)])


def local(movie, shifts, footprint, support, neuron_ids, owner_order, start_traces):
    where = jnp.stack([lax.axis_index(axis) for axis in ("ta_0", "ta_1", "row")]).astype(jnp.int32)
    packed = pack(neuron_ids[0], owner_order, footprint[0, 0], support[0, 0], start_traces.reshape(8, LANES))
    here = lax.all_to_all(packed, YZ, 0, 0, tiled=True)
    registered = register(movie[0], shifts[0])
    tiled = smooth(registered)
    arrived = lax.all_to_all(tiled, YZX, split_axis=0, concat_axis=0, tiled=True)
    left, far, right = [moved(here, "ta_0", by) for by in range(1, PLANES)]
    mine = project(where, tiled, here, left, far, right)
    other = moved(mine, "row", 1)
    pieces = solve(where, mine, other)
    pieces = [pieces[0]] + [moved(pieces[k], "ta_0", k) for k in range(1, PLANES)]
    pieces = merge(where, pieces)
    pieces = [pieces[0]] + [moved(pieces[k], "ta_1", k) for k in range(1, PLANES)]
    pieces = gather(where, pieces)
    pieces = lax.all_to_all(pieces.reshape(LINE, 1, LANES), "ta_2", 0, 0, tiled=True)
    tile_movie = store(arrived)
    traces = join(pieces.reshape(LINE, LANES))
    return (tile_movie.reshape(1, 1, -1, PIXELS), traces)


def solution(mesh):
    finer = Mesh(mesh.devices.reshape(4, 4, 8, mesh.shape["row"]), TA_ROW)
    return jax.shard_map(
        local,
        mesh=finer,
        in_specs=(
            P("row", TA, None, None),
            P("row", TA, None, None),
            P("row", TA, None, None),
            P("row", TA, None, None),
            P("row", TA, None),
            P(),
            P(TA_ROW, None),
        ),
        out_specs=(P("row", TA, None, None), P(TA_ROW, None)),
        check_vma=False,
    )
```

```python
import jax
import jax.numpy as jnp
import numpy as np
from jax import lax
from jax.experimental import pallas as pl
from jax.experimental.pallas import tpu as pltpu
from jax.sharding import PartitionSpec as P

TH = 16
TW = 32
MAXS = 8
ITERS = 2
TA = "ta"
TA_ROW = ("ta", "row")

FRAMES = 8
H = 128
W = 512
LANES = 128
BLOCKS = W // LANES
SLOTS = 8
NEURONS = 256
TILES = 128
PIXELS = TH * TW
PLANE = 32
PLANES = 4
LINE = 8
MESSAGE = PIXELS + LANES
ID_LANE = 64
HIGHEST = lax.Precision.HIGHEST
VMEM = pl.BlockSpec(memory_space=pltpu.VMEM)
SMEM = pl.BlockSpec(memory_space=pltpu.SMEM)


def smoothing_table(length):
    places = np.arange(length, dtype=np.float32)
    spread = places[:, None] - places[None, :]
    kernel = np.exp(-spread * spread / np.float32(32.0)).astype(np.float32)
    return (kernel / np.sum(kernel, axis=0, keepdims=True, dtype=np.float32)).astype(jnp.bfloat16)


def far_end(r):
    return (r // LINE + 2) % 4 * LINE + (r % LINE + 4) % LINE


NEAR_PLANES = [[PLANE * x + r for r in range(PLANE)] for x in range(PLANES)]
FAR_PLANES = [[PLANE * x + far_end(r) for r in range(PLANE)] for x in range(PLANES)]
FAR_ALL = [[PLANE * ((r + 2) % PLANES) + far_end(r // PLANES) for r in range(TILES)]]


def iota(shape, dim):
    return lax.broadcasted_iota(jnp.int32, shape, dim)


def split3(value):
    high = value.astype(jnp.bfloat16)
    rest = value - high.astype(jnp.float32)
    mid = rest.astype(jnp.bfloat16)
    low = (rest - mid.astype(jnp.float32)).astype(jnp.bfloat16)
    return high, mid, low


def dot32(left, right):
    return jnp.dot(left, right, preferred_element_type=jnp.float32)


def place(value, exact):
    high, mid, low = split3(value)
    return dot32(high, exact) + (dot32(mid, exact) + dot32(low, exact))


def register_kernel(shifts_ref, movie_ref, out_ref, padded_ref):
    lane = iota((H, LANES), 1)
    for s in range(2 * BLOCKS):
        padded_ref[s, pl.ds(0, MAXS), :] = jnp.zeros((MAXS, LANES), jnp.float32)
        padded_ref[s, pl.ds(MAXS + H, MAXS), :] = jnp.zeros((MAXS, LANES), jnp.float32)

    def block(f, p):
        if p < 0 or p >= BLOCKS:
            return None
        return movie_ref[f, :, p * LANES : (p + 1) * LANES].astype(jnp.float32)

    def shift(f, p, s):
        dy = shifts_ref[f, p, 0]
        dx = shifts_ref[f, p, 1]
        amount = jnp.where(dx > 0, LANES - dx, -dx)
        source = lane + dx

        def rolled(value):
            if value is None:
                return jnp.zeros((H, LANES), jnp.float32)
            return pltpu.roll(value, amount, 1)

        inner = jnp.where(source >= LANES, rolled(block(f, p + 1)), rolled(block(f, p)))
        padded_ref[s, pl.ds(MAXS, H), :] = jnp.where(source < 0, rolled(block(f, p - 1)), inner)
        out_ref[f, :, p * LANES : (p + 1) * LANES] = padded_ref[s, pl.ds(MAXS + dy, H), :].astype(jnp.bfloat16)

    def frames(g, carry):
        for h in range(2):
            for p in range(BLOCKS):
                shift(2 * g + h, p, h * BLOCKS + p)
        return carry

    lax.fori_loop(0, FRAMES // 2, frames, 0)


def register(movie, shifts):
    return pl.pallas_call(
        register_kernel,
        out_shape=jax.ShapeDtypeStruct((FRAMES, H, W), jnp.bfloat16),
        in_specs=[SMEM, VMEM],
        out_specs=VMEM,
        scratch_shapes=[pltpu.VMEM((2 * BLOCKS, H + 2 * MAXS, LANES), jnp.float32)],
        cost_estimate=pl.CostEstimate(flops=2_000_000_000, bytes_accessed=2_000_000, transcendentals=0),
        compiler_params=pltpu.CompilerParams(vmem_limit_bytes=8 << 20),
        name="register",
    )(shifts, movie)


def smooth_kernel(registered_ref, wide_ref, tall_ref, out_ref, filtered_ref, soft_ref):
    step = 2

    def chunk(c, carry):
        registered = registered_ref[pl.ds(c * step, step)].reshape(step * H, W)
        soft_ref[...] = dot32(registered, wide_ref[...]).astype(jnp.bfloat16)
        for k in range(step):
            low = dot32(tall_ref[...], soft_ref[k * H : (k + 1) * H, :])
            filtered = registered[k * H : (k + 1) * H].astype(jnp.float32) - low
            for p in range(BLOCKS):
                span = pl.ds(c * step + k, H, stride=FRAMES)
                filtered_ref[p, span, :] = filtered[:, p * LANES : (p + 1) * LANES]
        return carry

    lax.fori_loop(0, FRAMES // step, chunk, 0)
    lanes8 = iota((FRAMES, LANES), 1)
    near = lanes8 < 2 * TW
    even = lax.rem(lanes8 // TW, 2) == 0

    def tile_row(ty, carry):
        for q in range(4):
            for p in range(BLOCKS):
                v = []
                for r in range(4):
                    at = pl.multiple_of((ty * TH + 4 * q + r) * FRAMES, FRAMES)
                    v.append(filtered_ref[p, pl.ds(at, FRAMES), :])
                a0 = jnp.where(near, v[0], pltpu.roll(v[2], 64, 1))
                a2 = jnp.where(near, pltpu.roll(v[0], 64, 1), v[2])
                a1 = jnp.where(near, v[1], pltpu.roll(v[3], 64, 1))
                a3 = jnp.where(near, pltpu.roll(v[1], 64, 1), v[3])
                tiles = (
                    jnp.where(even, a0, pltpu.roll(a1, 32, 1)),
                    jnp.where(even, pltpu.roll(a0, 96, 1), a1),
                    jnp.where(even, a2, pltpu.roll(a3, 32, 1)),
                    jnp.where(even, pltpu.roll(a2, 96, 1), a3),
                )
                for m in range(4):
                    column = 4 * p + m
                    yz = LINE * (2 - 2 * lax.rem(ty, 2) + column // LINE) + (column + 4) % LINE
                    at = PLANES * yz + lax.rem(ty // 2 + 2, PLANES)
                    out_ref[at, :, q * LANES : (q + 1) * LANES] = tiles[m].astype(jnp.bfloat16)
        return carry

    lax.fori_loop(0, H // TH, tile_row, 0)


def smooth(registered):
    return pl.pallas_call(
        smooth_kernel,
        out_shape=jax.ShapeDtypeStruct((TILES, FRAMES, PIXELS), jnp.bfloat16),
        in_specs=[VMEM] * 3,
        out_specs=VMEM,
        scratch_shapes=[
            pltpu.VMEM((BLOCKS, H * FRAMES, LANES), jnp.float32),
            pltpu.VMEM((2 * H, W), jnp.bfloat16),
        ],
        cost_estimate=pl.CostEstimate(flops=4_000_000_000, bytes_accessed=3_000_000, transcendentals=0),
        compiler_params=pltpu.CompilerParams(vmem_limit_bytes=16 << 20),
        name="smooth",
    )(registered, smoothing_table(W), smoothing_table(H).T)


def pack_kernel(ids_ref, order_ref, footprint_ref, support_ref, start_ref, out_ref):
    footprints = footprint_ref[...] * support_ref[...].astype(jnp.bfloat16)
    parts = [part.astype(jnp.float32) for part in split3(start_ref[...])]
    row = iota((SLOTS, LANES), 0)
    lane = iota((SLOTS, LANES), 1)
    owners = jnp.zeros((SLOTS, LANES), jnp.float32)
    for i in range(SLOTS):
        owner = order_ref[ids_ref[0, i]].astype(jnp.float32)
        owners = jnp.where((row == i) & (lane == ID_LANE), owner, owners)
    for w in range(PLANE // 2):
        extra = owners
        for k, part in enumerate(parts):
            extra = jnp.where(lane // FRAMES == k, pltpu.roll(part, (FRAMES * (k - w)) % LANES, 1), extra)
        for to in (far_end(w), far_end(w + PLANE // 2)):
            out_ref[to, :, :PIXELS] = footprints
            out_ref[to, :, PIXELS:] = extra.astype(jnp.bfloat16)


def pack(ids, order, footprint, support, start):
    return pl.pallas_call(
        pack_kernel,
        out_shape=jax.ShapeDtypeStruct((PLANE, SLOTS, MESSAGE), jnp.bfloat16),
        in_specs=[SMEM, SMEM, VMEM, VMEM, VMEM],
        out_specs=VMEM,
        cost_estimate=pl.CostEstimate(flops=200_000_000, bytes_accessed=200_000, transcendentals=0),
        name="pack",
    )(ids, order, footprint, support, start)


def project_kernel(
    where_ref, tiled_ref, here_ref, left_ref, far_ref, right_ref, out_ref, select_ref, terms_ref
):
    x, y = where_ref[0], where_ref[1]
    many = PLANE // 2
    rows = many * SLOTS
    width = NEURONS + LANES
    same = iota((rows, 2 * rows), 0) // SLOTS == lax.rem(iota((rows, 2 * rows), 1), rows) // SLOTS
    own_row = iota((many, SLOTS, LANES), 1) == 2 * x + y // 2
    contract = (((1,), (1,)), ((), ()))
    neuron = iota((rows, NEURONS), 1)
    neuron_t = iota((NEURONS, rows), 0)
    diagonal = iota((rows, rows), 0) == iota((rows, rows), 1)
    out_ref[:, width:] = jnp.zeros((NEURONS, LANES), jnp.float32)
    for at in range(2 * PLANES):
        kx, first = at // 2, many * (at % 2)
        message = (here_ref, left_ref, far_ref, right_ref)[kx][first : first + many]
        source = lax.rem(x + PLANES - kx, PLANES)
        frames = [tiled_ref[PLANES * (first + k) + lax.rem(source + 2, PLANES)] for k in range(many)]
        prints = message[:, :, :PIXELS].reshape(rows, PIXELS)
        extra = message[:, :, PIXELS:].astype(jnp.float32).reshape(rows, LANES)
        found = lax.dot_general(
            prints, jnp.concatenate(frames + [prints], axis=0), contract, preferred_element_type=jnp.float32
        )
        found = jnp.where(same, found, 0.0)
        ids = extra[:, ID_LANE : ID_LANE + 1]
        select = jnp.where(neuron == ids.astype(jnp.int32), 1.0, 0.0).astype(jnp.bfloat16)
        ids_row = jnp.sum(jnp.where(diagonal, ids, 0.0), axis=0, keepdims=True).astype(jnp.int32)
        span = slice(at * rows, (at + 1) * rows)
        select_ref[:, span] = jnp.where(neuron_t == ids_row, 1.0, 0.0).astype(jnp.bfloat16)
        spread = place(found[:, rows:], select)
        for k, (one, two) in enumerate(zip(split3(spread), split3(found[:, :rows]), strict=True)):
            terms_ref[span, k * width : k * width + NEURONS] = one
            terms_ref[span, k * width + NEURONS : (k + 1) * width] = two
        piece = jnp.sum(jnp.where(own_row, extra.reshape(many, SLOTS, LANES), 0.0), axis=1)
        piece = piece + (pltpu.roll(piece, LANES - FRAMES, 1) + pltpu.roll(piece, LANES - 2 * FRAMES, 1))
        for k in range(0, many, LINE):
            tile = pl.multiple_of(PLANE * source + far_end(first + k) // LINE * LINE, LINE)
            out_ref[pl.ds(tile, LINE), width:] = pltpu.roll(piece[k : k + LINE], LINE // 2, 0)
    sums = dot32(select_ref[...], terms_ref[...])
    out_ref[:, :width] = sums[:, :width] + (sums[:, width : 2 * width] + sums[:, 2 * width :])


def project(where, tiled, here, left, far, right):
    rows = TILES * SLOTS
    return pl.pallas_call(
        project_kernel,
        out_shape=jax.ShapeDtypeStruct((NEURONS, NEURONS + 2 * LANES), jnp.float32),
        in_specs=[SMEM] + [VMEM] * 5,
        out_specs=VMEM,
        scratch_shapes=[
            pltpu.VMEM((NEURONS, rows), jnp.bfloat16),
            pltpu.VMEM((rows, 3 * (NEURONS + LANES)), jnp.bfloat16),
        ],
        cost_estimate=pl.CostEstimate(flops=2_000_000_000, bytes_accessed=3_000_000, transcendentals=0),
        compiler_params=pltpu.CompilerParams(vmem_limit_bytes=16 << 20),
        name="project",
    )(where, tiled, here, left, far, right)


def solve_kernel(where_ref, mine_ref, other_ref, *refs):
    out_refs, current_ref, own_ref = refs[:PLANES], refs[PLANES], refs[PLANES + 1]
    x, core = where_ref[0], where_ref[2]
    sums = mine_ref[:, : NEURONS + LANES] + other_ref[:, : NEURONS + LANES]
    coupling = sums[:, :NEURONS]
    source = iota((LANES, LANES), 0)
    target = lax.rem(iota((LANES, LANES), 1), FRAMES)
    fold = jnp.where(lax.rem(source, FRAMES) == target, 1.0, 0.0)
    drive = place(sums[:, NEURONS:], fold.astype(jnp.bfloat16))
    copy = jnp.where(source == target, 1.0, 0.0).astype(jnp.bfloat16)
    here = mine_ref[:TILES, NEURONS + LANES :]
    there = other_ref[:TILES, NEURONS + LANES :]
    current_ref[pl.ds(0, TILES, stride=2), :] = place(jnp.where(core == 0, here, there), copy)
    current_ref[pl.ds(1, TILES, stride=2), :] = place(jnp.where(core == 0, there, here), copy)
    current = current_ref[...]
    bound = 1.0 + jnp.sum(coupling, axis=1, keepdims=True)
    for _ in range(ITERS):
        product = jnp.dot(coupling, current, preferred_element_type=jnp.float32, precision=HIGHEST)
        current = jnp.maximum(current - (product - drive) / bound, 0.0)
    current_ref[...] = current
    even = current_ref[pl.ds(0, TILES, stride=2), :]
    odd = current_ref[pl.ds(1, TILES, stride=2), :]
    own_ref[...] = jnp.where(core == 0, even, odd)
    for k in range(PLANES):
        at = pl.multiple_of(PLANE * lax.rem(x + k, PLANES), PLANE)
        out_refs[k][...] = own_ref[pl.ds(at, PLANE), :]


def solve(where, mine, other):
    return pl.pallas_call(
        solve_kernel,
        out_shape=[jax.ShapeDtypeStruct((PLANE, LANES), jnp.float32)] * PLANES,
        in_specs=[SMEM, VMEM, VMEM],
        out_specs=[VMEM] * PLANES,
        scratch_shapes=[pltpu.VMEM((NEURONS, LANES), jnp.float32), pltpu.VMEM((TILES, LANES), jnp.float32)],
        cost_estimate=pl.CostEstimate(flops=2_000_000_000, bytes_accessed=1_000_000, transcendentals=0),
        compiler_params=pltpu.CompilerParams(vmem_limit_bytes=8 << 20),
        name="solve",
    )(where, mine, other)


def merge_kernel(where_ref, *refs):
    group = lax.rem(iota((PLANE, LANES), 1) // FRAMES, PLANES)
    merged = refs[0][...]
    for k in range(1, PLANES):
        merged = jnp.where(group == lax.rem(where_ref[0] + PLANES - k, PLANES), refs[k][...], merged)
    refs[PLANES][...] = merged


def merge(where, pieces):
    return pl.pallas_call(
        merge_kernel,
        out_shape=jax.ShapeDtypeStruct((PLANE, LANES), jnp.float32),
        in_specs=[SMEM] + [VMEM] * PLANES,
        out_specs=VMEM,
        cost_estimate=pl.CostEstimate(flops=100_000_000, bytes_accessed=100_000, transcendentals=0),
        compiler_params=pltpu.CompilerParams(vmem_limit_bytes=2 << 20),
        name="merge",
    )(where, *pieces)


def join_kernel(pieces_ref, out_ref):
    near = LANES // FRAMES
    pieces = pieces_ref[...]
    rolled = [pieces] + [pltpu.roll(pieces, FRAMES * j, 1) for j in range(1, PLANES)]
    group = iota((near, LANES), 1) // FRAMES
    inside = group == iota((near, LANES), 0)
    for b in range(TILES // near):
        xs, first = b // 2, near * (b % 2)
        total = jnp.zeros((near, LANES), jnp.float32)
        for j in range(PLANES):
            hit = inside & (lax.rem(group + PLANES - j, PLANES) == xs)
            total = jnp.where(hit, rolled[j][first : first + near], total)
        out_ref[:, b * LANES : (b + 1) * LANES] = jnp.sum(total, axis=0, keepdims=True)


def join(pieces):
    return pl.pallas_call(
        join_kernel,
        out_shape=jax.ShapeDtypeStruct((1, TILES * FRAMES), jnp.float32),
        in_specs=[VMEM],
        out_specs=VMEM,
        compiler_params=pltpu.CompilerParams(vmem_limit_bytes=2 << 20),
        name="join",
    )(pieces)


def store_kernel(arrived_ref, out_ref, sems):
    copies = []
    for x in range(PLANES):
        for y in range(2):
            for z in range(2):
                source = arrived_ref.at[y, :, z, :, (x + 2) % PLANES]
                target = out_ref.at[x, 1 - y, :, 1 - z]
                copies.append(pltpu.make_async_copy(source, target, sems.at[len(copies)]))
    for copy in copies:
        copy.start()
    for copy in copies:
        copy.wait()


def store(arrived):
    return pl.pallas_call(
        store_kernel,
        out_shape=jax.ShapeDtypeStruct((PLANES, 2, 2, 2, 4, FRAMES, PIXELS), jnp.bfloat16),
        in_specs=[VMEM],
        out_specs=pl.BlockSpec(memory_space=pl.ANY),
        scratch_shapes=[pltpu.SemaphoreType.DMA((4 * PLANES,))],
        cost_estimate=pl.CostEstimate(flops=500_000_000, bytes_accessed=2_000_000, transcendentals=0),
        compiler_params=pltpu.CompilerParams(vmem_limit_bytes=4 << 20),
        name="store",
    )(arrived.reshape(2, 2, 2, 4, PLANES, FRAMES, PIXELS))


def moved(array, by):
    return lax.ppermute(array, TA, [(t, (t + PLANE * by) % TILES) for t in range(TILES)])


def exchanged(array, ranks):
    return lax.all_to_all(array, TA, 0, 0, tiled=True, axis_index_groups=ranks)


def local(movie, shifts, footprint, support, neuron_ids, owner_order, start_traces):
    at = lax.axis_index(TA)
    where = jnp.stack([at // PLANE, at % PLANE // LINE, lax.axis_index("row")]).astype(jnp.int32)
    packed = pack(neuron_ids[0], owner_order, footprint[0, 0], support[0, 0], start_traces.reshape(8, LANES))
    here = exchanged(packed, FAR_PLANES)
    registered = register(movie[0], shifts[0])
    tiled = smooth(registered)
    arrived = exchanged(tiled, FAR_ALL)
    left, far, right = [moved(here, by) for by in range(1, PLANES)]
    mine = project(where, tiled, here, left, far, right)
    other = lax.ppermute(mine, "row", [(0, 1), (1, 0)])
    pieces = solve(where, mine, other)
    pieces = [pieces[0]] + [moved(pieces[k], k) for k in range(1, PLANES)]
    pieces = merge(where, pieces)
    pieces = exchanged(pieces.reshape(PLANE, 1, LANES), NEAR_PLANES)
    tile_movie = store(arrived)
    traces = join(pieces.reshape(PLANE, LANES))
    return (tile_movie.reshape(1, 1, -1, PIXELS), traces)


def solution(mesh):
    return jax.shard_map(
        local,
        mesh=mesh,
        in_specs=(
            P("row", TA, None, None),
            P("row", TA, None, None),
            P("row", TA, None, None),
            P("row", TA, None, None),
            P("row", TA, None),
            P(),
            P(TA_ROW, None),
        ),
        out_specs=(P("row", TA, None, None), P(TA_ROW, None)),
        check_vma=False,
    )
```

```python
import jax
import jax.numpy as jnp
import numpy as np
from jax import lax
from jax.experimental import pallas as pl
from jax.experimental.pallas import tpu as pltpu
from jax.sharding import PartitionSpec as P

TH = 16
TW = 32
MAXS = 8
ITERS = 2
TA = "ta"
TA_ROW = ("ta", "row")

FRAMES = 8
H = 128
W = 512
LANES = 128
BLOCKS = W // LANES
SLOTS = 8
NEURONS = 256
TILES = 128
PIXELS = TH * TW
PLANE = 32
PLANES = 4
LINE = 8
MESSAGE = PIXELS + LANES
ID_LANE = 64
HIGHEST = lax.Precision.HIGHEST
VMEM = pl.BlockSpec(memory_space=pltpu.VMEM)
SMEM = pl.BlockSpec(memory_space=pltpu.SMEM)


def smoothing_table(length):
    places = np.arange(length, dtype=np.float32)
    spread = places[:, None] - places[None, :]
    kernel = np.exp(-spread * spread / np.float32(32.0)).astype(np.float32)
    return (kernel / np.sum(kernel, axis=0, keepdims=True, dtype=np.float32)).astype(jnp.bfloat16)


def far_end(r):
    return (r // LINE + 2) % 4 * LINE + (r % LINE + 4) % LINE


FAR_PLANES = [[PLANE * x + far_end(r) for r in range(PLANE)] for x in range(PLANES)]
FAR_ALL = [[PLANE * ((r + 2) % PLANES) + far_end(r // PLANES) for r in range(TILES)]]


def iota(shape, dim):
    return lax.broadcasted_iota(jnp.int32, shape, dim)


def split3(value):
    high = value.astype(jnp.bfloat16)
    rest = value - high.astype(jnp.float32)
    mid = rest.astype(jnp.bfloat16)
    low = (rest - mid.astype(jnp.float32)).astype(jnp.bfloat16)
    return high, mid, low


def dot32(left, right):
    return jnp.dot(left, right, preferred_element_type=jnp.float32)


def place(value, exact):
    high, mid, low = split3(value)
    return dot32(high, exact) + (dot32(mid, exact) + dot32(low, exact))


def register_kernel(shifts_ref, movie_ref, out_ref, padded_ref):
    lane = iota((H, LANES), 1)
    for s in range(2 * BLOCKS):
        padded_ref[s, pl.ds(0, MAXS), :] = jnp.zeros((MAXS, LANES), jnp.float32)
        padded_ref[s, pl.ds(MAXS + H, MAXS), :] = jnp.zeros((MAXS, LANES), jnp.float32)

    def block(f, p):
        if p < 0 or p >= BLOCKS:
            return None
        return movie_ref[f, :, p * LANES : (p + 1) * LANES].astype(jnp.float32)

    def shift(f, p, s):
        dy = shifts_ref[f, p, 0]
        dx = shifts_ref[f, p, 1]
        amount = jnp.where(dx > 0, LANES - dx, -dx)
        source = lane + dx

        def rolled(value):
            if value is None:
                return jnp.zeros((H, LANES), jnp.float32)
            return pltpu.roll(value, amount, 1)

        inner = jnp.where(source >= LANES, rolled(block(f, p + 1)), rolled(block(f, p)))
        padded_ref[s, pl.ds(MAXS, H), :] = jnp.where(source < 0, rolled(block(f, p - 1)), inner)
        out_ref[f, :, p * LANES : (p + 1) * LANES] = padded_ref[s, pl.ds(MAXS + dy, H), :].astype(jnp.bfloat16)

    def frames(g, carry):
        for h in range(2):
            for p in range(BLOCKS):
                shift(2 * g + h, p, h * BLOCKS + p)
        return carry

    lax.fori_loop(0, FRAMES // 2, frames, 0)


def register(movie, shifts):
    return pl.pallas_call(
        register_kernel,
        out_shape=jax.ShapeDtypeStruct((FRAMES, H, W), jnp.bfloat16),
        in_specs=[SMEM, VMEM],
        out_specs=VMEM,
        scratch_shapes=[pltpu.VMEM((2 * BLOCKS, H + 2 * MAXS, LANES), jnp.float32)],
        cost_estimate=pl.CostEstimate(flops=2_000_000_000, bytes_accessed=2_000_000, transcendentals=0),
        compiler_params=pltpu.CompilerParams(vmem_limit_bytes=8 << 20),
        name="register",
    )(shifts, movie)


def smooth_kernel(registered_ref, wide_ref, tall_ref, out_ref, filtered_ref, soft_ref):
    step = 2

    def chunk(c, carry):
        registered = registered_ref[pl.ds(c * step, step)].reshape(step * H, W)
        soft_ref[...] = dot32(registered, wide_ref[...]).astype(jnp.bfloat16)
        for k in range(step):
            low = dot32(tall_ref[...], soft_ref[k * H : (k + 1) * H, :])
            filtered = registered[k * H : (k + 1) * H].astype(jnp.float32) - low
            for p in range(BLOCKS):
                span = pl.ds(c * step + k, H, stride=FRAMES)
                filtered_ref[p, span, :] = filtered[:, p * LANES : (p + 1) * LANES]
        return carry

    lax.fori_loop(0, FRAMES // step, chunk, 0)
    lanes8 = iota((FRAMES, LANES), 1)
    near = lanes8 < 2 * TW
    even = lax.rem(lanes8 // TW, 2) == 0

    def tile_row(ty, carry):
        for q in range(4):
            for p in range(BLOCKS):
                v = []
                for r in range(4):
                    at = pl.multiple_of((ty * TH + 4 * q + r) * FRAMES, FRAMES)
                    v.append(filtered_ref[p, pl.ds(at, FRAMES), :])
                a0 = jnp.where(near, v[0], pltpu.roll(v[2], 64, 1))
                a2 = jnp.where(near, pltpu.roll(v[0], 64, 1), v[2])
                a1 = jnp.where(near, v[1], pltpu.roll(v[3], 64, 1))
                a3 = jnp.where(near, pltpu.roll(v[1], 64, 1), v[3])
                tiles = (
                    jnp.where(even, a0, pltpu.roll(a1, 32, 1)),
                    jnp.where(even, pltpu.roll(a0, 96, 1), a1),
                    jnp.where(even, a2, pltpu.roll(a3, 32, 1)),
                    jnp.where(even, pltpu.roll(a2, 96, 1), a3),
                )
                for m in range(4):
                    column = 4 * p + m
                    yz = LINE * (2 - 2 * lax.rem(ty, 2) + column // LINE) + (column + 4) % LINE
                    at = PLANES * yz + lax.rem(ty // 2 + 2, PLANES)
                    out_ref[at, :, q * LANES : (q + 1) * LANES] = tiles[m].astype(jnp.bfloat16)
        return carry

    lax.fori_loop(0, H // TH, tile_row, 0)


def smooth(registered):
    return pl.pallas_call(
        smooth_kernel,
        out_shape=jax.ShapeDtypeStruct((TILES, FRAMES, PIXELS), jnp.bfloat16),
        in_specs=[VMEM] * 3,
        out_specs=VMEM,
        scratch_shapes=[
            pltpu.VMEM((BLOCKS, H * FRAMES, LANES), jnp.float32),
            pltpu.VMEM((2 * H, W), jnp.bfloat16),
        ],
        cost_estimate=pl.CostEstimate(flops=4_000_000_000, bytes_accessed=3_000_000, transcendentals=0),
        compiler_params=pltpu.CompilerParams(vmem_limit_bytes=16 << 20),
        name="smooth",
    )(registered, smoothing_table(W), smoothing_table(H).T)


def pack_kernel(ids_ref, order_ref, footprint_ref, support_ref, start_ref, out_ref):
    footprints = footprint_ref[...] * support_ref[...].astype(jnp.bfloat16)
    parts = [part.astype(jnp.float32) for part in split3(start_ref[...])]
    row = iota((SLOTS, LANES), 0)
    lane = iota((SLOTS, LANES), 1)
    owners = jnp.zeros((SLOTS, LANES), jnp.float32)
    for i in range(SLOTS):
        owner = order_ref[ids_ref[0, i]].astype(jnp.float32)
        owners = jnp.where((row == i) & (lane == ID_LANE), owner, owners)
    for w in range(PLANE // 2):
        extra = owners
        for k, part in enumerate(parts):
            extra = jnp.where(lane // FRAMES == k, pltpu.roll(part, (FRAMES * (k - w)) % LANES, 1), extra)
        for to in (far_end(w), far_end(w + PLANE // 2)):
            out_ref[to, :, :PIXELS] = footprints
            out_ref[to, :, PIXELS:] = extra.astype(jnp.bfloat16)


def pack(ids, order, footprint, support, start):
    return pl.pallas_call(
        pack_kernel,
        out_shape=jax.ShapeDtypeStruct((PLANE, SLOTS, MESSAGE), jnp.bfloat16),
        in_specs=[SMEM, SMEM, VMEM, VMEM, VMEM],
        out_specs=VMEM,
        cost_estimate=pl.CostEstimate(flops=200_000_000, bytes_accessed=200_000, transcendentals=0),
        name="pack",
    )(ids, order, footprint, support, start)


def project_kernel(
    where_ref, tiled_ref, here_ref, left_ref, far_ref, right_ref, out_ref, select_ref, terms_ref
):
    x, y = where_ref[0], where_ref[1]
    many = PLANE // 2
    rows = many * SLOTS
    width = NEURONS + LANES
    same = iota((rows, 2 * rows), 0) // SLOTS == lax.rem(iota((rows, 2 * rows), 1), rows) // SLOTS
    own_row = iota((many, SLOTS, LANES), 1) == 2 * x + y // 2
    contract = (((1,), (1,)), ((), ()))
    neuron = iota((rows, NEURONS), 1)
    neuron_t = iota((NEURONS, rows), 0)
    diagonal = iota((rows, rows), 0) == iota((rows, rows), 1)
    out_ref[:, width:] = jnp.zeros((NEURONS, LANES), jnp.float32)
    for at in range(2 * PLANES):
        kx, first = at // 2, many * (at % 2)
        message = (here_ref, left_ref, far_ref, right_ref)[kx][first : first + many]
        source = lax.rem(x + PLANES - kx, PLANES)
        frames = [tiled_ref[PLANES * (first + k) + lax.rem(source + 2, PLANES)] for k in range(many)]
        prints = message[:, :, :PIXELS].reshape(rows, PIXELS)
        extra = message[:, :, PIXELS:].astype(jnp.float32).reshape(rows, LANES)
        found = lax.dot_general(
            prints, jnp.concatenate(frames + [prints], axis=0), contract, preferred_element_type=jnp.float32
        )
        found = jnp.where(same, found, 0.0)
        ids = extra[:, ID_LANE : ID_LANE + 1]
        select = jnp.where(neuron == ids.astype(jnp.int32), 1.0, 0.0).astype(jnp.bfloat16)
        ids_row = jnp.sum(jnp.where(diagonal, ids, 0.0), axis=0, keepdims=True).astype(jnp.int32)
        span = slice(at * rows, (at + 1) * rows)
        select_ref[:, span] = jnp.where(neuron_t == ids_row, 1.0, 0.0).astype(jnp.bfloat16)
        spread = place(found[:, rows:], select)
        for k, (one, two) in enumerate(zip(split3(spread), split3(found[:, :rows]), strict=True)):
            terms_ref[span, k * width : k * width + NEURONS] = one
            terms_ref[span, k * width + NEURONS : (k + 1) * width] = two
        piece = jnp.sum(jnp.where(own_row, extra.reshape(many, SLOTS, LANES), 0.0), axis=1)
        piece = piece + (pltpu.roll(piece, LANES - FRAMES, 1) + pltpu.roll(piece, LANES - 2 * FRAMES, 1))
        for k in range(0, many, LINE):
            tile = pl.multiple_of(PLANE * source + far_end(first + k) // LINE * LINE, LINE)
            out_ref[pl.ds(tile, LINE), width:] = pltpu.roll(piece[k : k + LINE], LINE // 2, 0)
    sums = dot32(select_ref[...], terms_ref[...])
    out_ref[:, :width] = sums[:, :width] + (sums[:, width : 2 * width] + sums[:, 2 * width :])


def project(where, tiled, here, left, far, right):
    rows = TILES * SLOTS
    return pl.pallas_call(
        project_kernel,
        out_shape=jax.ShapeDtypeStruct((NEURONS, NEURONS + 2 * LANES), jnp.float32),
        in_specs=[SMEM] + [VMEM] * 5,
        out_specs=VMEM,
        scratch_shapes=[
            pltpu.VMEM((NEURONS, rows), jnp.bfloat16),
            pltpu.VMEM((rows, 3 * (NEURONS + LANES)), jnp.bfloat16),
        ],
        cost_estimate=pl.CostEstimate(flops=2_000_000_000, bytes_accessed=3_000_000, transcendentals=0),
        compiler_params=pltpu.CompilerParams(vmem_limit_bytes=16 << 20),
        name="project",
    )(where, tiled, here, left, far, right)


def solve_kernel(where_ref, mine_ref, other_ref, *refs):
    out_refs, current_ref, own_ref = refs[:PLANES], refs[PLANES], refs[PLANES + 1]
    x, core = where_ref[0], where_ref[2]
    sums = mine_ref[:, : NEURONS + LANES] + other_ref[:, : NEURONS + LANES]
    coupling = sums[:, :NEURONS]
    source = iota((LANES, LANES), 0)
    target = lax.rem(iota((LANES, LANES), 1), FRAMES)
    fold = jnp.where(lax.rem(source, FRAMES) == target, 1.0, 0.0)
    drive = place(sums[:, NEURONS:], fold.astype(jnp.bfloat16))
    copy = jnp.where(source == target, 1.0, 0.0).astype(jnp.bfloat16)
    here = mine_ref[:TILES, NEURONS + LANES :]
    there = other_ref[:TILES, NEURONS + LANES :]
    current_ref[pl.ds(0, TILES, stride=2), :] = place(jnp.where(core == 0, here, there), copy)
    current_ref[pl.ds(1, TILES, stride=2), :] = place(jnp.where(core == 0, there, here), copy)
    current = current_ref[...]
    bound = 1.0 + jnp.sum(coupling, axis=1, keepdims=True)
    for _ in range(ITERS):
        product = jnp.dot(coupling, current, preferred_element_type=jnp.float32, precision=HIGHEST)
        current = jnp.maximum(current - (product - drive) / bound, 0.0)
    current_ref[...] = current
    even = current_ref[pl.ds(0, TILES, stride=2), :]
    odd = current_ref[pl.ds(1, TILES, stride=2), :]
    own_ref[...] = jnp.where(core == 0, even, odd)
    for k in range(PLANES):
        at = pl.multiple_of(PLANE * lax.rem(x + k, PLANES), PLANE)
        out_refs[k][...] = own_ref[pl.ds(at, PLANE), :]


def solve(where, mine, other):
    return pl.pallas_call(
        solve_kernel,
        out_shape=[jax.ShapeDtypeStruct((PLANE, LANES), jnp.float32)] * PLANES,
        in_specs=[SMEM, VMEM, VMEM],
        out_specs=[VMEM] * PLANES,
        scratch_shapes=[pltpu.VMEM((NEURONS, LANES), jnp.float32), pltpu.VMEM((TILES, LANES), jnp.float32)],
        cost_estimate=pl.CostEstimate(flops=2_000_000_000, bytes_accessed=1_000_000, transcendentals=0),
        compiler_params=pltpu.CompilerParams(vmem_limit_bytes=8 << 20),
        name="solve",
    )(where, mine, other)


def ranked(rows):
    groups = [far_end(r) // LINE * LINE for r in range(0, PLANE, LINE)]
    return jnp.concatenate([pltpu.roll(rows[g : g + LINE], LINE // 2, 0) for g in groups], axis=0)


def merge_kernel(where_ref, *refs):
    group = lax.rem(iota((PLANE, LANES), 1) // FRAMES, PLANES)
    merged = refs[0][...]
    for k in range(1, PLANES):
        merged = jnp.where(group == lax.rem(where_ref[0] + PLANES - k, PLANES), refs[k][...], merged)
    refs[PLANES][...] = ranked(merged)


def merge(where, pieces):
    return pl.pallas_call(
        merge_kernel,
        out_shape=jax.ShapeDtypeStruct((PLANE, LANES), jnp.float32),
        in_specs=[SMEM] + [VMEM] * PLANES,
        out_specs=VMEM,
        cost_estimate=pl.CostEstimate(flops=100_000_000, bytes_accessed=100_000, transcendentals=0),
        compiler_params=pltpu.CompilerParams(vmem_limit_bytes=2 << 20),
        name="merge",
    )(where, *pieces)


def join_kernel(pieces_ref, out_ref):
    near = LANES // FRAMES
    pieces = ranked(pieces_ref[...])
    rolled = [pieces] + [pltpu.roll(pieces, FRAMES * j, 1) for j in range(1, PLANES)]
    group = iota((near, LANES), 1) // FRAMES
    inside = group == iota((near, LANES), 0)
    for b in range(TILES // near):
        xs, first = b // 2, near * (b % 2)
        total = jnp.zeros((near, LANES), jnp.float32)
        for j in range(PLANES):
            hit = inside & (lax.rem(group + PLANES - j, PLANES) == xs)
            total = jnp.where(hit, rolled[j][first : first + near], total)
        out_ref[:, b * LANES : (b + 1) * LANES] = jnp.sum(total, axis=0, keepdims=True)


def join(pieces):
    return pl.pallas_call(
        join_kernel,
        out_shape=jax.ShapeDtypeStruct((1, TILES * FRAMES), jnp.float32),
        in_specs=[VMEM],
        out_specs=VMEM,
        compiler_params=pltpu.CompilerParams(vmem_limit_bytes=2 << 20),
        name="join",
    )(pieces)


def store_kernel(arrived_ref, out_ref, sems):
    copies = []
    for x in range(PLANES):
        for y in range(2):
            for z in range(2):
                source = arrived_ref.at[y, :, z, :, (x + 2) % PLANES]
                target = out_ref.at[x, 1 - y, :, 1 - z]
                copies.append(pltpu.make_async_copy(source, target, sems.at[len(copies)]))
    for copy in copies:
        copy.start()
    for copy in copies:
        copy.wait()


def store(arrived):
    return pl.pallas_call(
        store_kernel,
        out_shape=jax.ShapeDtypeStruct((PLANES, 2, 2, 2, 4, FRAMES, PIXELS), jnp.bfloat16),
        in_specs=[VMEM],
        out_specs=pl.BlockSpec(memory_space=pl.ANY),
        scratch_shapes=[pltpu.SemaphoreType.DMA((4 * PLANES,))],
        cost_estimate=pl.CostEstimate(flops=500_000_000, bytes_accessed=2_000_000, transcendentals=0),
        compiler_params=pltpu.CompilerParams(vmem_limit_bytes=4 << 20),
        name="store",
    )(arrived.reshape(2, 2, 2, 4, PLANES, FRAMES, PIXELS))


def moved(array, by):
    return lax.ppermute(array, TA, [(t, (t + PLANE * by) % TILES) for t in range(TILES)])


def exchanged(array, ranks):
    return lax.all_to_all(array, TA, 0, 0, tiled=True, axis_index_groups=ranks)


def local(movie, shifts, footprint, support, neuron_ids, owner_order, start_traces):
    at = lax.axis_index(TA)
    where = jnp.stack([at // PLANE, at % PLANE // LINE, lax.axis_index("row")]).astype(jnp.int32)
    packed = pack(neuron_ids[0], owner_order, footprint[0, 0], support[0, 0], start_traces.reshape(8, LANES))
    here = exchanged(packed, FAR_PLANES)
    registered = register(movie[0], shifts[0])
    tiled = smooth(registered)
    arrived = exchanged(tiled, FAR_ALL)
    left, far, right = [moved(here, by) for by in range(1, PLANES)]
    mine = project(where, tiled, here, left, far, right)
    other = lax.ppermute(mine, "row", [(0, 1), (1, 0)])
    pieces = solve(where, mine, other)
    pieces = [pieces[0]] + [moved(pieces[k], k) for k in range(1, PLANES)]
    pieces = merge(where, pieces)
    pieces = exchanged(pieces.reshape(PLANE, 1, LANES), FAR_PLANES)
    tile_movie = store(arrived)
    traces = join(pieces.reshape(PLANE, LANES))
    return (tile_movie.reshape(1, 1, -1, PIXELS), traces)


def solution(mesh):
    return jax.shard_map(
        local,
        mesh=mesh,
        in_specs=(
            P("row", TA, None, None),
            P("row", TA, None, None),
            P("row", TA, None, None),
            P("row", TA, None, None),
            P("row", TA, None),
            P(),
            P(TA_ROW, None),
        ),
        out_specs=(P("row", TA, None, None), P(TA_ROW, None)),
        check_vma=False,
    )
```

```python
import jax
import jax.numpy as jnp
import numpy as np
from jax import lax
from jax.experimental import pallas as pl
from jax.experimental.pallas import tpu as pltpu
from jax.sharding import PartitionSpec as P

TH = 16
TW = 32
MAXS = 8
ITERS = 2
TA = "ta"
TA_ROW = ("ta", "row")

FRAMES = 8
H = 128
W = 512
LANES = 128
BLOCKS = W // LANES
SLOTS = 8
NEURONS = 256
TILES = 128
PIXELS = TH * TW
PLANE = 32
PLANES = 4
LINE = 8
MESSAGE = PIXELS + LANES
ID_LANE = 64
HIGHEST = lax.Precision.HIGHEST
VMEM = pl.BlockSpec(memory_space=pltpu.VMEM)
SMEM = pl.BlockSpec(memory_space=pltpu.SMEM)


def smoothing_table(length):
    places = np.arange(length, dtype=np.float32)
    spread = places[:, None] - places[None, :]
    kernel = np.exp(-spread * spread / np.float32(32.0)).astype(np.float32)
    return (kernel / np.sum(kernel, axis=0, keepdims=True, dtype=np.float32)).astype(jnp.bfloat16)


def far_end(r):
    return (r // LINE + 2) % 4 * LINE + (r % LINE + 4) % LINE


FAR_PLANES = [[PLANE * x + far_end(r) for r in range(PLANE)] for x in range(PLANES)]
FAR_ALL = [[PLANE * (r % PLANES) + far_end(r // PLANES) for r in range(TILES)]]


def iota(shape, dim):
    return lax.broadcasted_iota(jnp.int32, shape, dim)


def split3(value):
    high = value.astype(jnp.bfloat16)
    rest = value - high.astype(jnp.float32)
    mid = rest.astype(jnp.bfloat16)
    low = (rest - mid.astype(jnp.float32)).astype(jnp.bfloat16)
    return high, mid, low


def dot32(left, right):
    return jnp.dot(left, right, preferred_element_type=jnp.float32)


def place(value, exact):
    high, mid, low = split3(value)
    return dot32(high, exact) + (dot32(mid, exact) + dot32(low, exact))


def register_kernel(shifts_ref, movie_ref, out_ref, padded_ref):
    lane = iota((H, LANES), 1)
    for s in range(2 * BLOCKS):
        padded_ref[s, pl.ds(0, MAXS), :] = jnp.zeros((MAXS, LANES), jnp.float32)
        padded_ref[s, pl.ds(MAXS + H, MAXS), :] = jnp.zeros((MAXS, LANES), jnp.float32)

    def block(f, p):
        if p < 0 or p >= BLOCKS:
            return None
        return movie_ref[f, :, p * LANES : (p + 1) * LANES].astype(jnp.float32)

    def shift(f, p, s):
        dy = shifts_ref[f, p, 0]
        dx = shifts_ref[f, p, 1]
        amount = jnp.where(dx > 0, LANES - dx, -dx)
        source = lane + dx

        def rolled(value):
            if value is None:
                return jnp.zeros((H, LANES), jnp.float32)
            return pltpu.roll(value, amount, 1)

        inner = jnp.where(source >= LANES, rolled(block(f, p + 1)), rolled(block(f, p)))
        padded_ref[s, pl.ds(MAXS, H), :] = jnp.where(source < 0, rolled(block(f, p - 1)), inner)
        out_ref[f, :, p * LANES : (p + 1) * LANES] = padded_ref[s, pl.ds(MAXS + dy, H), :].astype(jnp.bfloat16)

    def frames(g, carry):
        for h in range(2):
            for p in range(BLOCKS):
                shift(2 * g + h, p, h * BLOCKS + p)
        return carry

    lax.fori_loop(0, FRAMES // 2, frames, 0)


def register(movie, shifts):
    return pl.pallas_call(
        register_kernel,
        out_shape=jax.ShapeDtypeStruct((FRAMES, H, W), jnp.bfloat16),
        in_specs=[SMEM, VMEM],
        out_specs=VMEM,
        scratch_shapes=[pltpu.VMEM((2 * BLOCKS, H + 2 * MAXS, LANES), jnp.float32)],
        cost_estimate=pl.CostEstimate(flops=2_000_000_000, bytes_accessed=2_000_000, transcendentals=0),
        compiler_params=pltpu.CompilerParams(vmem_limit_bytes=8 << 20),
        name="register",
    )(shifts, movie)


def smooth_kernel(registered_ref, wide_ref, tall_ref, out_ref, filtered_ref, soft_ref):
    step = 2

    def chunk(c, carry):
        registered = registered_ref[pl.ds(c * step, step)].reshape(step * H, W)
        soft_ref[...] = dot32(registered, wide_ref[...]).astype(jnp.bfloat16)
        for k in range(step):
            low = dot32(tall_ref[...], soft_ref[k * H : (k + 1) * H, :])
            filtered = registered[k * H : (k + 1) * H].astype(jnp.float32) - low
            for p in range(BLOCKS):
                span = pl.ds(c * step + k, H, stride=FRAMES)
                filtered_ref[p, span, :] = filtered[:, p * LANES : (p + 1) * LANES]
        return carry

    lax.fori_loop(0, FRAMES // step, chunk, 0)
    lanes8 = iota((FRAMES, LANES), 1)
    near = lanes8 < 2 * TW
    even = lax.rem(lanes8 // TW, 2) == 0

    def tile_row(ty, carry):
        for q in range(4):
            for p in range(BLOCKS):
                v = []
                for r in range(4):
                    at = pl.multiple_of((ty * TH + 4 * q + r) * FRAMES, FRAMES)
                    v.append(filtered_ref[p, pl.ds(at, FRAMES), :])
                a0 = jnp.where(near, v[0], pltpu.roll(v[2], 64, 1))
                a2 = jnp.where(near, pltpu.roll(v[0], 64, 1), v[2])
                a1 = jnp.where(near, v[1], pltpu.roll(v[3], 64, 1))
                a3 = jnp.where(near, pltpu.roll(v[1], 64, 1), v[3])
                tiles = (
                    jnp.where(even, a0, pltpu.roll(a1, 32, 1)),
                    jnp.where(even, pltpu.roll(a0, 96, 1), a1),
                    jnp.where(even, a2, pltpu.roll(a3, 32, 1)),
                    jnp.where(even, pltpu.roll(a2, 96, 1), a3),
                )
                for m in range(4):
                    column = 4 * p + m
                    yz = LINE * (2 - 2 * lax.rem(ty, 2) + column // LINE) + (column + 4) % LINE
                    at = PLANES * yz + ty // 2
                    out_ref[at, :, q * LANES : (q + 1) * LANES] = tiles[m].astype(jnp.bfloat16)
        return carry

    lax.fori_loop(0, H // TH, tile_row, 0)


def smooth(registered):
    return pl.pallas_call(
        smooth_kernel,
        out_shape=jax.ShapeDtypeStruct((TILES, FRAMES, PIXELS), jnp.bfloat16),
        in_specs=[VMEM] * 3,
        out_specs=VMEM,
        scratch_shapes=[
            pltpu.VMEM((BLOCKS, H * FRAMES, LANES), jnp.float32),
            pltpu.VMEM((2 * H, W), jnp.bfloat16),
        ],
        cost_estimate=pl.CostEstimate(flops=4_000_000_000, bytes_accessed=3_000_000, transcendentals=0),
        compiler_params=pltpu.CompilerParams(vmem_limit_bytes=16 << 20),
        name="smooth",
    )(registered, smoothing_table(W), smoothing_table(H).T)


def pack_kernel(ids_ref, order_ref, footprint_ref, support_ref, start_ref, out_ref):
    footprints = footprint_ref[...] * support_ref[...].astype(jnp.bfloat16)
    parts = [part.astype(jnp.float32) for part in split3(start_ref[...])]
    row = iota((SLOTS, LANES), 0)
    lane = iota((SLOTS, LANES), 1)
    owners = jnp.zeros((SLOTS, LANES), jnp.float32)
    for i in range(SLOTS):
        owner = order_ref[ids_ref[0, i]].astype(jnp.float32)
        owners = jnp.where((row == i) & (lane == ID_LANE), owner, owners)
    for w in range(PLANE // 2):
        extra = owners
        for k, part in enumerate(parts):
            extra = jnp.where(lane // FRAMES == k, pltpu.roll(part, (FRAMES * (k - w)) % LANES, 1), extra)
        for to in (far_end(w), far_end(w + PLANE // 2)):
            out_ref[to, :, :PIXELS] = footprints
            out_ref[to, :, PIXELS:] = extra.astype(jnp.bfloat16)


def pack(ids, order, footprint, support, start):
    return pl.pallas_call(
        pack_kernel,
        out_shape=jax.ShapeDtypeStruct((PLANE, SLOTS, MESSAGE), jnp.bfloat16),
        in_specs=[SMEM, SMEM, VMEM, VMEM, VMEM],
        out_specs=VMEM,
        cost_estimate=pl.CostEstimate(flops=200_000_000, bytes_accessed=200_000, transcendentals=0),
        name="pack",
    )(ids, order, footprint, support, start)


def project_kernel(
    where_ref, tiled_ref, here_ref, left_ref, far_ref, right_ref, out_ref, select_ref, terms_ref
):
    x, y = where_ref[0], where_ref[1]
    many = PLANE // 2
    rows = many * SLOTS
    width = NEURONS + LANES
    same = iota((rows, 2 * rows), 0) // SLOTS == lax.rem(iota((rows, 2 * rows), 1), rows) // SLOTS
    own_row = iota((many, SLOTS, LANES), 1) == 2 * x + y // 2
    contract = (((1,), (1,)), ((), ()))
    neuron = iota((rows, NEURONS), 1)
    neuron_t = iota((NEURONS, rows), 0)
    diagonal = iota((rows, rows), 0) == iota((rows, rows), 1)
    out_ref[:, width:] = jnp.zeros((NEURONS, LANES), jnp.float32)
    for at in range(2 * PLANES):
        kx, first = at // 2, many * (at % 2)
        message = (here_ref, left_ref, far_ref, right_ref)[kx][first : first + many]
        source = lax.rem(x + PLANES - kx, PLANES)
        frames = [tiled_ref[PLANES * (first + k) + source] for k in range(many)]
        prints = message[:, :, :PIXELS].reshape(rows, PIXELS)
        extra = message[:, :, PIXELS:].astype(jnp.float32).reshape(rows, LANES)
        found = lax.dot_general(
            prints, jnp.concatenate(frames + [prints], axis=0), contract, preferred_element_type=jnp.float32
        )
        found = jnp.where(same, found, 0.0)
        ids = extra[:, ID_LANE : ID_LANE + 1]
        select = jnp.where(neuron == ids.astype(jnp.int32), 1.0, 0.0).astype(jnp.bfloat16)
        ids_row = jnp.sum(jnp.where(diagonal, ids, 0.0), axis=0, keepdims=True).astype(jnp.int32)
        span = slice(at * rows, (at + 1) * rows)
        select_ref[:, span] = jnp.where(neuron_t == ids_row, 1.0, 0.0).astype(jnp.bfloat16)
        spread = place(found[:, rows:], select)
        for k, (one, two) in enumerate(zip(split3(spread), split3(found[:, :rows]), strict=True)):
            terms_ref[span, k * width : k * width + NEURONS] = one
            terms_ref[span, k * width + NEURONS : (k + 1) * width] = two
        piece = jnp.sum(jnp.where(own_row, extra.reshape(many, SLOTS, LANES), 0.0), axis=1)
        piece = piece + (pltpu.roll(piece, LANES - FRAMES, 1) + pltpu.roll(piece, LANES - 2 * FRAMES, 1))
        for k in range(0, many, LINE):
            tile = pl.multiple_of(PLANE * source + far_end(first + k) // LINE * LINE, LINE)
            out_ref[pl.ds(tile, LINE), width:] = pltpu.roll(piece[k : k + LINE], LINE // 2, 0)
    sums = dot32(select_ref[...], terms_ref[...])
    out_ref[:, :width] = sums[:, :width] + (sums[:, width : 2 * width] + sums[:, 2 * width :])


def project(where, tiled, here, left, far, right):
    rows = TILES * SLOTS
    return pl.pallas_call(
        project_kernel,
        out_shape=jax.ShapeDtypeStruct((NEURONS, NEURONS + 2 * LANES), jnp.float32),
        in_specs=[SMEM] + [VMEM] * 5,
        out_specs=VMEM,
        scratch_shapes=[
            pltpu.VMEM((NEURONS, rows), jnp.bfloat16),
            pltpu.VMEM((rows, 3 * (NEURONS + LANES)), jnp.bfloat16),
        ],
        cost_estimate=pl.CostEstimate(flops=2_000_000_000, bytes_accessed=3_000_000, transcendentals=0),
        compiler_params=pltpu.CompilerParams(vmem_limit_bytes=16 << 20),
        name="project",
    )(where, tiled, here, left, far, right)


def solve_kernel(where_ref, mine_ref, other_ref, *refs):
    out_refs, current_ref, own_ref = refs[:PLANES], refs[PLANES], refs[PLANES + 1]
    x, core = where_ref[0], where_ref[2]
    sums = mine_ref[:, : NEURONS + LANES] + other_ref[:, : NEURONS + LANES]
    coupling = sums[:, :NEURONS]
    source = iota((LANES, LANES), 0)
    target = lax.rem(iota((LANES, LANES), 1), FRAMES)
    fold = jnp.where(lax.rem(source, FRAMES) == target, 1.0, 0.0)
    drive = place(sums[:, NEURONS:], fold.astype(jnp.bfloat16))
    copy = jnp.where(source == target, 1.0, 0.0).astype(jnp.bfloat16)
    here = mine_ref[:TILES, NEURONS + LANES :]
    there = other_ref[:TILES, NEURONS + LANES :]
    current_ref[pl.ds(0, TILES, stride=2), :] = place(jnp.where(core == 0, here, there), copy)
    current_ref[pl.ds(1, TILES, stride=2), :] = place(jnp.where(core == 0, there, here), copy)
    current = current_ref[...]
    bound = 1.0 + jnp.sum(coupling, axis=1, keepdims=True)
    for _ in range(ITERS):
        product = jnp.dot(coupling, current, preferred_element_type=jnp.float32, precision=HIGHEST)
        current = jnp.maximum(current - (product - drive) / bound, 0.0)
    current_ref[...] = current
    even = current_ref[pl.ds(0, TILES, stride=2), :]
    odd = current_ref[pl.ds(1, TILES, stride=2), :]
    own_ref[...] = jnp.where(core == 0, even, odd)
    for k in range(PLANES):
        at = pl.multiple_of(PLANE * lax.rem(x + k, PLANES), PLANE)
        out_refs[k][...] = own_ref[pl.ds(at, PLANE), :]


def solve(where, mine, other):
    return pl.pallas_call(
        solve_kernel,
        out_shape=[jax.ShapeDtypeStruct((PLANE, LANES), jnp.float32)] * PLANES,
        in_specs=[SMEM, VMEM, VMEM],
        out_specs=[VMEM] * PLANES,
        scratch_shapes=[pltpu.VMEM((NEURONS, LANES), jnp.float32), pltpu.VMEM((TILES, LANES), jnp.float32)],
        cost_estimate=pl.CostEstimate(flops=2_000_000_000, bytes_accessed=1_000_000, transcendentals=0),
        compiler_params=pltpu.CompilerParams(vmem_limit_bytes=8 << 20),
        name="solve",
    )(where, mine, other)


def ranked(rows):
    groups = [far_end(r) // LINE * LINE for r in range(0, PLANE, LINE)]
    return jnp.concatenate([pltpu.roll(rows[g : g + LINE], LINE // 2, 0) for g in groups], axis=0)


def merge_kernel(where_ref, *refs):
    group = lax.rem(iota((PLANE, LANES), 1) // FRAMES, PLANES)
    merged = refs[0][...]
    for k in range(1, PLANES):
        merged = jnp.where(group == lax.rem(where_ref[0] + PLANES - k, PLANES), refs[k][...], merged)
    refs[PLANES][...] = ranked(merged)


def merge(where, pieces):
    return pl.pallas_call(
        merge_kernel,
        out_shape=jax.ShapeDtypeStruct((PLANE, LANES), jnp.float32),
        in_specs=[SMEM] + [VMEM] * PLANES,
        out_specs=VMEM,
        cost_estimate=pl.CostEstimate(flops=100_000_000, bytes_accessed=100_000, transcendentals=0),
        compiler_params=pltpu.CompilerParams(vmem_limit_bytes=2 << 20),
        name="merge",
    )(where, *pieces)


def join_kernel(pieces_ref, out_ref):
    near = LANES // FRAMES
    pieces = ranked(pieces_ref[...])
    rolled = [pieces] + [pltpu.roll(pieces, FRAMES * j, 1) for j in range(1, PLANES)]
    group = iota((near, LANES), 1) // FRAMES
    inside = group == iota((near, LANES), 0)
    for b in range(TILES // near):
        xs, first = b // 2, near * (b % 2)
        total = jnp.zeros((near, LANES), jnp.float32)
        for j in range(PLANES):
            hit = inside & (lax.rem(group + PLANES - j, PLANES) == xs)
            total = jnp.where(hit, rolled[j][first : first + near], total)
        out_ref[:, b * LANES : (b + 1) * LANES] = jnp.sum(total, axis=0, keepdims=True)


def join(pieces):
    return pl.pallas_call(
        join_kernel,
        out_shape=jax.ShapeDtypeStruct((1, TILES * FRAMES), jnp.float32),
        in_specs=[VMEM],
        out_specs=VMEM,
        compiler_params=pltpu.CompilerParams(vmem_limit_bytes=2 << 20),
        name="join",
    )(pieces)


def store_kernel(arrived_ref, out_ref, sems):
    copies = []
    for x in range(PLANES):
        for y in range(2):
            for z in range(2):
                source = arrived_ref.at[y, :, z, :, x]
                target = out_ref.at[x, 1 - y, :, 1 - z]
                copies.append(pltpu.make_async_copy(source, target, sems.at[len(copies)]))
    for copy in copies:
        copy.start()
    for copy in copies:
        copy.wait()


def store(arrived):
    return pl.pallas_call(
        store_kernel,
        out_shape=jax.ShapeDtypeStruct((PLANES, 2, 2, 2, 4, FRAMES, PIXELS), jnp.bfloat16),
        in_specs=[VMEM],
        out_specs=pl.BlockSpec(memory_space=pl.ANY),
        scratch_shapes=[pltpu.SemaphoreType.DMA((4 * PLANES,))],
        cost_estimate=pl.CostEstimate(flops=500_000_000, bytes_accessed=2_000_000, transcendentals=0),
        compiler_params=pltpu.CompilerParams(vmem_limit_bytes=4 << 20),
        name="store",
    )(arrived.reshape(2, 2, 2, 4, PLANES, FRAMES, PIXELS))


def moved(array, by):
    return lax.ppermute(array, TA, [(t, (t + PLANE * by) % TILES) for t in range(TILES)])


def exchanged(array, ranks):
    return lax.all_to_all(array, TA, 0, 0, tiled=True, axis_index_groups=ranks)


def local(movie, shifts, footprint, support, neuron_ids, owner_order, start_traces):
    at = lax.axis_index(TA)
    where = jnp.stack([at // PLANE, at % PLANE // LINE, lax.axis_index("row")]).astype(jnp.int32)
    packed = pack(neuron_ids[0], owner_order, footprint[0, 0], support[0, 0], start_traces.reshape(8, LANES))
    here = exchanged(packed, FAR_PLANES)
    registered = register(movie[0], shifts[0])
    tiled = smooth(registered)
    arrived = exchanged(tiled, FAR_ALL)
    left, far, right = [moved(here, by) for by in range(1, PLANES)]
    mine = project(where, tiled, here, left, far, right)
    other = lax.ppermute(mine, "row", [(0, 1), (1, 0)])
    pieces = solve(where, mine, other)
    pieces = [pieces[0]] + [moved(pieces[k], k) for k in range(1, PLANES)]
    pieces = merge(where, pieces)
    pieces = exchanged(pieces.reshape(PLANE, 1, LANES), FAR_PLANES)
    tile_movie = store(arrived)
    traces = join(pieces.reshape(PLANE, LANES))
    return (tile_movie.reshape(1, 1, -1, PIXELS), traces)


def solution(mesh):
    return jax.shard_map(
        local,
        mesh=mesh,
        in_specs=(
            P("row", TA, None, None),
            P("row", TA, None, None),
            P("row", TA, None, None),
            P("row", TA, None, None),
            P("row", TA, None),
            P(),
            P(TA_ROW, None),
        ),
        out_specs=(P("row", TA, None, None), P(TA_ROW, None)),
        check_vma=False,
    )
```
